32 devices in a mesh: scan: 8 (over z, y), grp: 4 (over x, core).
Axes of the slice: x: 2, y: 2, z: 4, core: 2. Of those that a mesh axis runs over, the one named last changes fastest.
Arguments:
- samples: float32 [128, 64, 6, 128], P('scan', 'grp'), may hold values from -6 to 6
- point_count: int32 [128], P('scan'), may hold values from 4096 to 8192
- corr_scan: int32 [128, 64], P('scan', 'grp'), may hold values from 0 to 127, as said below
- corr_tile: int32 [128, 64], P('scan', 'grp'), may hold values from 0 to 63
- corr_src: int32 [128, 64, 128], P('scan', 'grp'), may hold values from 0 to 2047
Outputs:
- hessian: float32 [128, 6, 6, 128], P('scan', None, None, 'grp')
- gradient: float32 [128, 6], P(('scan', 'grp'))
The draws below stay inside these ranges and needn't reach their ends.
Inputs may be any that keep to these rules, and one draw needn't show every extreme that they name: Never the scan of the entry's own row. A named tile is held by the device with scan index corr_scan // 16 and grp index corr_tile // 16; the 256 entries of one device name at most 16 tiles held by any one device, and in every draw some device is named exactly 16 times by every device.
All inputs are finite; a program needn't handle non-finite values.
Results may differ from the reference program's by a relative error of at most 0.00021.
Values sent between devices are 32-bit elements; how exact they have to be, the bound alone decides.
No kernel may reach another device: no remote copies, remote signals or barrier semaphores. Data moves between devices by JAX's collectives and lax.ppermute only.
A program may use at most 64 MiB of HBM per device.

```python
import jax
import jax.numpy as jnp
from jax import lax

SCAN_LOC = 16
TILES_G = 16
CT = 16
SCANS = 128
TILES = 64
N_SCAN = 8
N_GRP = 4
DEVICES = 32


def pair_plan(key):
    half_count = DEVICES // 2
    slot_cap = 2 * SCAN_LOC * CT // DEVICES
    request_count = SCAN_LOC * CT
    hub_device = jax.random.randint(jax.random.fold_in(key, 1), (), 0, DEVICES)

    def one_device(device):
        dev_key = jax.random.fold_in(key, device + 100)

        def one_round(round_idx):
            round_key = jax.random.fold_in(dev_key, round_idx)
            shuffled = jax.random.permutation(round_key, DEVICES - 1) + 1
            offsets = jnp.concatenate([jnp.zeros((1,), jnp.int32), shuffled[:half_count - 1].astype(jnp.int32)])
            return (hub_device + offsets) % DEVICES
        destination = jax.vmap(one_round)(jnp.arange(slot_cap)).reshape(request_count)
        own_index = device // N_GRP
        dest_index = destination // N_GRP
        dest_group = destination % N_GRP
        local_scan = jnp.arange(request_count) // CT
        chosen = jax.random.randint(jax.random.fold_in(dev_key, 5000), (request_count,), 0, SCAN_LOC)
        clashes = (dest_index == own_index) & (chosen == local_scan)
        chosen = jnp.where(clashes, (chosen + 1) % SCAN_LOC, chosen)
        target_scan = dest_index * SCAN_LOC + chosen
        tile_ids = dest_group * TILES_G + jax.random.randint(jax.random.fold_in(dev_key, 6000), (request_count,), 0, TILES_G)
        return (target_scan.astype(jnp.int32), tile_ids.astype(jnp.int32))
    targets, tile_ids = jax.vmap(one_device)(jnp.arange(DEVICES))
    grid_shape = (N_SCAN, N_GRP, SCAN_LOC, CT)
    targets = targets.reshape(grid_shape).transpose(0, 2, 1, 3).reshape(N_SCAN * SCAN_LOC, N_GRP * CT)
    tile_ids = tile_ids.reshape(grid_shape).transpose(0, 2, 1, 3).reshape(N_SCAN * SCAN_LOC, N_GRP * CT)
    return (targets, tile_ids)


def draw_corr_scan(key, part):
    return pair_plan(key)[0]


def draw_corr_tile(key, part):
    return pair_plan(key)[1]


def set_ends(result, stream_key, smallest, top_value):
    longest = result.shape.index(max(result.shape))
    spots = []
    for shift in (0, 1):
        where = [jax.random.randint(jax.random.fold_in(stream_key, axis), (), 0, length) for axis, length in enumerate(result.shape)]
        where[longest] = (where[longest] + shift) % result.shape[longest]
        spots.append(tuple(where))
    return result.at[spots[0]].set(smallest).at[spots[1]].set(top_value)


def steps_of(own_key, extent, pieces, low, high):
    level, own = 1.0, jax.random.fold_in(own_key, 6)
    for dim, blocks in pieces:
        draws = jnp.exp(jax.random.uniform(jax.random.fold_in(own, dim), (blocks,), jnp.float32, low / len(pieces), high / len(pieces)))
        level = level * jnp.repeat(draws, extent[dim] // blocks).reshape([-1 if axis == dim else 1 for axis in range(len(extent))])
    return level


def scatter_about(key, shape, scale, limit, split=(), held_as=jnp.bfloat16):
    array = scale * jax.random.normal(key, shape, jnp.float32)
    if split:
        array = array * steps_of(key, shape, split, -0.22, 0.18)
    return jnp.clip(array, -limit, limit).astype(held_as)


def setup_inputs(seed: int = 0) -> dict:
    seeds = jax.random.split(jax.random.key(seed), 6)
    samples = scatter_about(seeds[0], (SCANS, TILES, 6, 128), 1.0, 6.0, ((0, 8), (1, 4)), jnp.float32)
    point_count = set_ends(jax.random.randint(seeds[1], (SCANS,), TILES_G * N_GRP * 64, TILES_G * N_GRP * 128 + 1), jax.random.fold_in(seeds[1], 1), TILES_G * N_GRP * 64, TILES_G * N_GRP * 128).astype(jnp.int32)
    corr_scan = draw_corr_scan(jax.random.fold_in(seeds[5], 71), 0)
    corr_tile = draw_corr_tile(jax.random.fold_in(seeds[5], 71), 0)
    corr_src = set_ends(jax.random.randint(seeds[4], (SCANS, N_GRP * CT, 128), 0, TILES_G * 128), jax.random.fold_in(seeds[4], 1), 0, (TILES_G * 128) - 1).astype(jnp.int32)
    return {"samples": samples, "point_count": point_count, "corr_scan": corr_scan, "corr_tile": corr_tile, "corr_src": corr_src}


def pair_blocks(pos_x, pos_y, pos_z, source_mask, tile_data):
    diff_x = pos_x - tile_data[:, 0, :]
    diff_y = pos_y - tile_data[:, 1, :]
    diff_z = pos_z - tile_data[:, 2, :]
    normal_x = tile_data[:, 3, :]
    normal_y = tile_data[:, 4, :]
    normal_z = tile_data[:, 5, :]
    residual = normal_x * diff_x + normal_y * diff_y + normal_z * diff_z
    weight = source_mask / (1.0 + residual * residual)
    jacobian = jnp.stack([pos_y * normal_z - pos_z * normal_y, pos_z * normal_x - pos_x * normal_z, pos_x * normal_y - pos_y * normal_x, normal_x, normal_y, normal_z], axis=1)
    blocks = jnp.einsum("nik,njk->nij", jacobian * weight[:, None, :], jacobian, precision=lax.Precision.HIGHEST)
    vectors = jnp.einsum("nik,nk->ni", jacobian, weight * residual, precision=lax.Precision.HIGHEST)
    return blocks.reshape(-1, 36), vectors


def reference(samples, point_count, corr_scan, corr_tile, corr_src):
    scan_count = samples.shape[0]
    tile_count = samples.shape[1]
    column_count = corr_scan.shape[1]
    per_group = column_count // N_GRP
    group_points = (tile_count // N_GRP) * 128
    groups = (jnp.arange(column_count) // per_group).astype(jnp.int32)
    point_ids = groups[None, :, None] * group_points + corr_src
    flat_samples = samples.reshape(scan_count, tile_count * 768)
    offsets = ((point_ids // 128) * 768 + point_ids % 128).reshape(scan_count, column_count * 128)
    coords = [jnp.take_along_axis(flat_samples, offsets + axis_id * 128, axis=1).reshape(-1, 128) for axis_id in range(3)]
    source_mask = (point_ids < point_count[:, None, None]).astype(jnp.float32).reshape(-1, 128)
    target_scan = corr_scan.reshape(-1)
    target_tile = corr_tile.reshape(-1)
    tile_data = samples[target_scan, target_tile]
    row_ids = jnp.arange(128).astype(jnp.int32)
    target_mask = ((target_tile[:, None] * 128 + row_ids[None, :]) < point_count[target_scan][:, None]).astype(jnp.float32)
    tile_data = jnp.concatenate([tile_data[:, 0:3, :], tile_data[:, 3:6, :] * target_mask[:, None, :]], axis=1)
    blocks, vectors = pair_blocks(coords[0], coords[1], coords[2], source_mask, tile_data)
    source_scan = (jnp.arange(scan_count * column_count) // column_count).astype(jnp.int32)
    pairwise = jnp.zeros((scan_count, scan_count, 36), jnp.float32)
    pairwise = pairwise.at[source_scan, source_scan].add(blocks)
    pairwise = pairwise.at[target_scan, target_scan].add(blocks)
    pairwise = pairwise.at[source_scan, target_scan].add(-blocks)
    pairwise = pairwise.at[target_scan, source_scan].add(-blocks)
    hessian = pairwise.reshape(scan_count, scan_count, 6, 6).transpose(0, 2, 3, 1)
    gradient = jnp.zeros((scan_count, 6), jnp.float32)
    gradient = gradient.at[source_scan].add(vectors).at[target_scan].add(-vectors)
    return hessian, gradient
```

```python
import jax
import jax.numpy as jnp
from jax import lax
from jax.experimental import pallas as pl
from jax.experimental.pallas import tpu as pltpu
from jax.sharding import PartitionSpec as P

LANES = 128
COORDS = 3
FIELDS = 6
PAIRS = [(i, j) for i in range(FIELDS) for j in range(i, FIELDS)]
MAT = len(PAIRS)
VALUES = MAT + FIELDS
ROW_FLAG = VALUES
ROW_MATE = VALUES + 1
WIDTH = 32
BOTH_LANES = (((1,), (1,)), ((), ()))
AXES = ("scan", "grp")


def div(x, n):
    if n & (n - 1) == 0:
        return lax.shift_right_logical(x, jnp.int32(n.bit_length() - 1))
    return x // n


def mod(x, n):
    if n & (n - 1) == 0:
        return x & (n - 1)
    return x % n


def iota(shape, dim):
    return lax.broadcasted_iota(jnp.int32, shape, dim)


def pieces(x, count):
    parts = []
    for _ in range(count - 1):
        part = x.astype(jnp.bfloat16)
        parts.append(part)
        x = x - part.astype(jnp.float32)
    parts.append(x.astype(jnp.bfloat16))
    return parts


def dot(a, b, dims=(((1,), (0,)), ((), ()))):
    return lax.dot_general(a, b, dims, preferred_element_type=jnp.float32)


def sizes(samples_shape, entries_shape, devices):
    scan_local, _, tiles, _ = samples_shape
    per_scan = entries_shape[1]
    entries = scan_local * per_scan
    cap = 2 * entries // devices
    return scan_local, tiles, per_scan, entries, cap, (COORDS + 1) * cap + 1


def send_kernel(devices, groups, group_ref, count_ref, samples_ref, scan_ref, tile_ref, src_ref, out_ref, data_ref):
    scan_local, tiles, per_scan, entries, cap, block = sizes(samples_ref.shape, scan_ref.shape, devices)
    group_points = tiles * LANES

    def one_scan(s, carry):
        first = group_ref[0] * group_points
        limit = count_ref[s] - first
        for h in range(per_scan // 8):
            ids = src_ref[s, pl.ds(h * 8, 8), :]
            lane = mod(ids, LANES)
            tile = div(ids, LANES)
            found = [jnp.zeros((8, LANES), jnp.float32) for _ in range(COORDS)]
            for t in range(tiles):
                here = tile == t
                for a in range(COORDS):
                    row = jnp.broadcast_to(samples_ref[s, a, t : t + 1, :], (8, LANES))
                    found[a] = jnp.where(here, jnp.take_along_axis(row, lane, axis=1), found[a])
            at = pl.multiple_of(s * per_scan + h * 8, 8)
            for a in range(COORDS):
                data_ref[a, pl.ds(at, 8), :] = found[a]
            data_ref[COORDS, pl.ds(at, 8), :] = (ids < limit).astype(jnp.float32)
        return carry

    lax.fori_loop(0, scan_local, one_scan, 0)

    scans = scan_ref[...]
    tile_ids = tile_ref[...]
    device = div(scans, scan_local) * groups + div(tile_ids, tiles)
    stacked = jnp.concatenate(
        [device.astype(jnp.float32), mod(scans, scan_local).astype(jnp.float32), mod(tile_ids, tiles).astype(jnp.float32)],
        axis=0,
    ).astype(jnp.bfloat16)
    spread = (mod(iota((per_scan, entries), 1), per_scan) == iota((per_scan, entries), 0)).astype(jnp.float32)
    wide = dot(stacked, spread.astype(jnp.bfloat16))
    own = div(iota((scan_local, entries), 1), per_scan) == iota((scan_local, entries), 0)
    device_row, mate_row, tile_row = [
        jnp.sum(jnp.where(own, wide[f * scan_local : (f + 1) * scan_local], 0.0), axis=0, keepdims=True)
        for f in range(3)
    ]
    rank_parts = []
    columns = []
    for h in range(entries // LANES):
        across = device_row[:, h * LANES : (h + 1) * LANES]
        columns.append(jnp.broadcast_to(across, (LANES, LANES)).T)
        total = jnp.zeros((1, LANES), jnp.float32)
        for g in range(h + 1):
            same = columns[g] == across
            if g == h:
                same = same & (iota((LANES, LANES), 0) < iota((LANES, LANES), 1))
            total = total + jnp.sum(same.astype(jnp.float32), axis=0, keepdims=True)
        rank_parts.append(total)
    rank_row = jnp.concatenate(rank_parts, axis=1)
    slot_row = (device_row * cap + rank_row).astype(jnp.int32)
    place = (iota((devices * cap, entries), 0) == slot_row).astype(jnp.float32).astype(jnp.bfloat16)
    for a in range(COORDS + 1):
        values = data_ref[a]
        if a < COORDS:
            parts = [dot(place, part) for part in pieces(values, 3)]
            moved = (parts[0] + parts[1]) + parts[2]
        else:
            moved = dot(place, values.astype(jnp.bfloat16))
        for d in range(devices):
            out_ref[pl.ds(d * block + a * cap, cap), :] = moved[d * cap : (d + 1) * cap]
    owner_row = (div(iota((1, entries), 1), per_scan) + 1).astype(jnp.float32)
    field = div(iota((LANES, entries), 0), cap)
    picked = jnp.where(field == 0, owner_row, jnp.where(field == 1, mate_row, tile_row))
    picked = jnp.where(
        (mod(iota((LANES, entries), 0), cap).astype(jnp.float32) == rank_row) & (field < 3), picked, 0.0
    ).astype(jnp.bfloat16)
    towards = (iota((devices, entries), 0).astype(jnp.float32) == device_row).astype(jnp.float32).astype(jnp.bfloat16)
    notes = dot(towards, picked, BOTH_LANES)
    for d in range(devices):
        out_ref[pl.ds(d * block + (COORDS + 1) * cap, 1), :] = notes[d : d + 1]


def pair_kernel(devices, group_ref, count_ref, samples_ref, recv_ref, flat_ref, pack_ref, point_ref, mate_ref, note_ref, wide_ref):
    scan_local, _, tiles, _ = samples_ref.shape
    slots = flat_ref.shape[1]
    cap = slots // devices
    block = (COORDS + 1) * cap + 1
    for d in range(devices):
        note_ref[pl.ds(d, 1), :] = recv_ref[pl.ds(d * block + (COORDS + 1) * cap, 1), :]
    notes = note_ref[...].astype(jnp.bfloat16)
    mine = div(iota((devices, slots), 1), cap) == iota((devices, slots), 0)
    rows = []
    for f in range(3):
        spread = (iota((LANES, slots), 0) == mod(iota((LANES, slots), 1), cap) + f * cap).astype(jnp.float32)
        rows.append(
            jnp.sum(jnp.where(mine, dot(notes, spread.astype(jnp.bfloat16)), 0.0), axis=0, keepdims=True)
        )
    flag_row, mate_row, tile_row = rows
    code_row = (mate_row * tiles + tile_row).astype(jnp.int32)
    table = scan_local * tiles
    chosen = (iota((table, slots), 0) == code_row).astype(jnp.float32).astype(jnp.bfloat16)
    base = group_ref[0] * tiles
    point_ids = (base + iota((tiles, LANES), 0)) * LANES + iota((tiles, LANES), 1)
    for a in range(FIELDS):
        values = []
        for b in range(scan_local):
            value = samples_ref[b, a]
            if a >= COORDS:
                value = jnp.where(point_ids < count_ref[b], value, 0.0)
            values.append(value)
        values = jnp.concatenate(values, axis=0)
        turned = jnp.concatenate([values[h : h + LANES].T for h in range(0, table, LANES)], axis=1)
        parts = [dot(part, chosen) for part in pieces(turned, 3)]
        mate_ref[a] = (parts[0] + parts[1]) + parts[2]
    per_chunk = LANES // cap
    for c in range(slots // LANES):
        for a in range(COORDS + 1):
            stack = [
                recv_ref[pl.ds(d * block + a * cap, cap), :] for d in range(c * per_chunk, (c + 1) * per_chunk)
            ]
            point_ref[a, :, c * LANES : (c + 1) * LANES] = jnp.concatenate(stack, axis=0).T
    for c in range(slots // LANES):
        lanes = slice(c * LANES, (c + 1) * LANES)

        def step(k, sums):
            at = pl.ds(pl.multiple_of(k * 8, 8), 8)
            px, py, pz, mask = [point_ref[a, at, lanes] for a in range(COORDS + 1)]
            qx, qy, qz, nx, ny, nz = [mate_ref[a, at, lanes] for a in range(FIELDS)]
            residual = nx * (px - qx) + ny * (py - qy) + nz * (pz - qz)
            weight = mask / (1.0 + residual * residual)
            jac = [py * nz - pz * ny, pz * nx - px * nz, px * ny - py * nx, nx, ny, nz]
            scaled = [weight * j for j in jac]
            terms = [scaled[i] * jac[j] for i, j in PAIRS] + [residual * s for s in scaled]
            return tuple(s + t for s, t in zip(sums, terms))

        zero = jnp.zeros((8, LANES), jnp.float32)
        sums = lax.fori_loop(0, LANES // 8, step, (zero,) * VALUES)
        lines = [jnp.sum(s, axis=0, keepdims=True) for s in sums]
        lines += [flag_row[:, lanes], mate_row[:, lanes]]
        lines += [jnp.zeros((1, LANES), jnp.float32)] * (WIDTH - len(lines))
        flat = jnp.concatenate(lines, axis=0)
        flat_ref[:, lanes] = flat
        tall = jnp.concatenate([flat, jnp.zeros((LANES - WIDTH, LANES), jnp.float32)], axis=0)
        wide_ref[pl.ds(c * LANES, LANES), :] = tall.T
    per_row = LANES // WIDTH
    packed = wide_ref[pl.ds(0, slots // per_row, stride=per_row), :]
    for k in range(1, per_row):
        packed = packed + pltpu.roll(wide_ref[pl.ds(k, slots // per_row, stride=per_row), :], k * WIDTH, 1)
    pack_ref[...] = packed


def layout(scan_local, groups, scan_total):
    columns = scan_total // groups
    pack = max(1, LANES // columns)
    per_block = -(-(MAT + 1) // pack)
    return columns, pack, per_block


def join_kernel(devices, groups, scan_local, place_ref, flat_ref, back_ref, out_ref):
    slots = flat_ref.shape[1]
    cap = slots // devices
    per_row = LANES // WIDTH
    stride = slots // per_row
    scan_total = scan_local * (devices // groups)
    columns, pack, per_block = layout(scan_local, groups, scan_total)
    turned = back_ref[...].T
    every = jnp.concatenate([turned[k * WIDTH : (k + 1) * WIDTH] for k in range(per_row)] + [flat_ref[...]], axis=1)
    total = 2 * slots
    at = iota((1, total), 1)
    mine = at < slots
    slot = jnp.where(mine, mod(at, stride) * per_row + div(at, stride), at - slots)
    peer = div(div(slot, cap), groups) * scan_local
    flag = every[ROW_FLAG : ROW_FLAG + 1].astype(jnp.int32) - 1
    mate = every[ROW_MATE : ROW_MATE + 1].astype(jnp.int32)
    row = jnp.where(mine, flag, mate)
    other = peer + jnp.where(mine, mate, flag)
    own = place_ref[0] * scan_local + row
    row_hot = iota((scan_local, total), 0) == row
    column = iota((scan_total, total), 0)
    mix = ((column == own).astype(jnp.float32) - (column == other).astype(jnp.float32)).astype(jnp.bfloat16)
    high = every.astype(jnp.bfloat16).astype(jnp.float32)
    hess = None
    for part in (high, every - high):
        spread = jnp.concatenate(
            [jnp.where(row_hot, part[q : q + 1], 0.0).astype(jnp.bfloat16) for q in range(MAT)], axis=0
        )
        piece = dot(spread, mix, BOTH_LANES)
        hess = piece if hess is None else hess + piece
    signed = jnp.where(mine, every, -every)
    lane = iota((scan_local, LANES), 1)
    home = MAT // per_block
    grad = jnp.zeros((scan_local, LANES), jnp.float32)
    for q in range(FIELDS):
        value = jnp.sum(jnp.where(row_hot, signed[MAT + q : MAT + q + 1], 0.0), axis=1, keepdims=True)
        grad = jnp.where(lane == home * columns + q, value, grad)
    rows = per_block * scan_local
    for c in range(groups):
        side, shift = divmod(c * columns, LANES)
        for r in range(per_block):
            tile = jnp.zeros((scan_local, LANES), jnp.float32)
            for k in range(pack):
                q = k * per_block + r
                if q < MAT:
                    value = hess[q * scan_local : (q + 1) * scan_local, side * LANES : (side + 1) * LANES]
                    turn = (k * columns - shift) % LANES
                    if turn:
                        value = pltpu.roll(value, turn, 1)
                elif q == MAT:
                    value = grad
                else:
                    continue
                if pack > 1:
                    value = jnp.where(div(lane, columns) == k, value, tile)
                tile = value
            out_ref[c, r * scan_local : (r + 1) * scan_local, :] = tile


def close_kernel(groups, group_ref, parts_ref, hess_ref, grad_ref, hold_ref):
    scan_local, columns = hess_ref.shape[1:]
    per_block = parts_ref.shape[1] // scan_local
    whole = parts_ref[0]
    for g in range(1, groups):
        whole = whole + parts_ref[g]
    for q in range(MAT + 1):
        k, r = divmod(q, per_block)
        tile = whole[r * scan_local : (r + 1) * scan_local, k * columns : (k + 1) * columns]
        if q < MAT:
            i, j = PAIRS[q]
            hess_ref[i * FIELDS + j] = tile
            if i != j:
                hess_ref[j * FIELDS + i] = tile
        else:
            hold_ref[:, 0:columns] = tile
    part = scan_local // groups
    grad_ref[...] = hold_ref[pl.ds(group_ref[0] * part, part), 0:FIELDS]


def call(kernel, out_shape, smem, vmem, scratch=()):
    return pl.pallas_call(
        kernel,
        out_shape=out_shape,
        in_specs=[pl.BlockSpec(memory_space=pltpu.SMEM)] * smem + [pl.BlockSpec(memory_space=pltpu.VMEM)] * vmem,
        scratch_shapes=list(scratch),
    )


def f32(*shape):
    return jax.ShapeDtypeStruct(shape, jnp.float32)


def exchange(x, axes):
    count, width = x.shape
    moved = lax.all_to_all(x.reshape(count, 1, width), axes, split_axis=0, concat_axis=0, tiled=True)
    return moved.reshape(count, width)


def local(samples, point_count, corr_scan, corr_tile, corr_src):
    devices = lax.axis_size(AXES)
    groups = lax.axis_size("grp")
    samples = samples.transpose(0, 2, 1, 3)
    scan_local, tiles, per_scan, entries, cap, block = sizes(samples.shape, corr_scan.shape, devices)
    slots = devices * cap
    scan_total = scan_local * (devices // groups)
    columns, pack, per_block = layout(scan_local, groups, scan_total)
    group = lax.axis_index("grp").astype(jnp.int32).reshape(1)
    scan = lax.axis_index("scan").astype(jnp.int32).reshape(1)
    bind = lambda kernel, *args: lambda *refs: kernel(*args, *refs)
    sent = call(
        bind(send_kernel, devices, groups),
        f32(devices * block, LANES),
        2,
        4,
        [pltpu.VMEM((COORDS + 1, entries, LANES), jnp.float32)],
    )(group, point_count, samples, corr_scan, corr_tile, corr_src)
    received = exchange(sent, AXES)
    flat, packed = call(
        bind(pair_kernel, devices),
        (f32(WIDTH, slots), f32(slots * WIDTH // LANES, LANES)),
        2,
        2,
        [
            pltpu.VMEM((COORDS + 1, LANES, slots), jnp.float32),
            pltpu.VMEM((FIELDS, LANES, slots), jnp.float32),
            pltpu.VMEM((devices, LANES), jnp.float32),
            pltpu.VMEM((slots, LANES), jnp.float32),
        ],
    )(group, point_count, samples, received)
    back = exchange(packed, AXES)
    shares = call(
        bind(join_kernel, devices, groups, scan_local), f32(groups, per_block * scan_local, LANES), 1, 2
    )(scan, flat, back)
    shares = lax.all_to_all(shares, "grp", split_axis=0, concat_axis=0, tiled=True)
    hess, grad = call(
        bind(close_kernel, groups),
        (f32(FIELDS * FIELDS, scan_local, columns), f32(scan_local // groups, FIELDS)),
        1,
        1,
        [pltpu.VMEM((scan_local, LANES), jnp.float32)],
    )(group, shares)
    return hess.reshape(FIELDS, FIELDS, scan_local, columns).transpose(2, 0, 1, 3), grad


def solution(mesh):
    placed = (
        P("scan", "grp", None, None),
        P("scan"),
        P("scan", "grp"),
        P("scan", "grp"),
        P("scan", "grp", None),
    )
    return jax.shard_map(
        local,
        mesh=mesh,
        in_specs=placed,
        out_specs=(P("scan", None, None, "grp"), P(AXES, None)),
        check_vma=False,
    )
```

```python
import jax
import jax.numpy as jnp
from jax import lax
from jax.experimental import pallas as pl
from jax.experimental.pallas import tpu as pltpu
from jax.sharding import PartitionSpec as P

LANES = 128
COORDS = 3
FIELDS = 6
PAIRS = [(i, j) for i in range(FIELDS) for j in range(i, FIELDS)]
MAT = len(PAIRS)
ROW_FLAG = MAT
ROW_MATE = MAT + 1
HEAD = MAT + 3
WIDTH = 32
BOTH_LANES = (((1,), (1,)), ((), ()))
AXES = ("scan", "grp")


def div(x, n):
    if n & (n - 1) == 0:
        return lax.shift_right_logical(x, jnp.int32(n.bit_length() - 1))
    return x // n


def mod(x, n):
    if n & (n - 1) == 0:
        return x & (n - 1)
    return x % n


def iota(shape, dim):
    return lax.broadcasted_iota(jnp.int32, shape, dim)


def pieces(x, count):
    parts = []
    for _ in range(count - 1):
        part = x.astype(jnp.bfloat16)
        parts.append(part)
        x = x - part.astype(jnp.float32)
    parts.append(x.astype(jnp.bfloat16))
    return parts


def dot(a, b, dims=(((1,), (0,)), ((), ()))):
    return lax.dot_general(a, b, dims, preferred_element_type=jnp.float32)


def sizes(samples_shape, entries_shape, devices):
    scan_local, _, tiles, _ = samples_shape
    per_scan = entries_shape[1]
    entries = scan_local * per_scan
    cap = 2 * entries // devices
    return scan_local, tiles, per_scan, entries, cap, (COORDS + 1) * cap + 1


def send_kernel(devices, groups, group_ref, count_ref, samples_ref, scan_ref, tile_ref, src_ref, out_ref, data_ref):
    scan_local, tiles, per_scan, entries, cap, block = sizes(samples_ref.shape, scan_ref.shape, devices)
    group_points = tiles * LANES

    def one_scan(s, carry):
        first = group_ref[0] * group_points
        limit = count_ref[s] - first
        for h in range(per_scan // 8):
            ids = src_ref[s, pl.ds(h * 8, 8), :]
            lane = mod(ids, LANES)
            tile = div(ids, LANES)
            found = [jnp.zeros((8, LANES), jnp.float32) for _ in range(COORDS)]
            for t in range(tiles):
                here = tile == t
                for a in range(COORDS):
                    row = jnp.broadcast_to(samples_ref[s, a, t : t + 1, :], (8, LANES))
                    found[a] = jnp.where(here, jnp.take_along_axis(row, lane, axis=1), found[a])
            at = pl.multiple_of(s * per_scan + h * 8, 8)
            for a in range(COORDS):
                data_ref[a, pl.ds(at, 8), :] = found[a]
            data_ref[COORDS, pl.ds(at, 8), :] = (ids < limit).astype(jnp.float32)
        return carry

    lax.fori_loop(0, scan_local, one_scan, 0)

    scans = scan_ref[...]
    tile_ids = tile_ref[...]
    device = div(scans, scan_local) * groups + div(tile_ids, tiles)
    stacked = jnp.concatenate(
        [device.astype(jnp.float32), mod(scans, scan_local).astype(jnp.float32), mod(tile_ids, tiles).astype(jnp.float32)],
        axis=0,
    ).astype(jnp.bfloat16)
    spread = (mod(iota((per_scan, entries), 1), per_scan) == iota((per_scan, entries), 0)).astype(jnp.float32)
    wide = dot(stacked, spread.astype(jnp.bfloat16))
    own = div(iota((scan_local, entries), 1), per_scan) == iota((scan_local, entries), 0)
    device_row, mate_row, tile_row = [
        jnp.sum(jnp.where(own, wide[f * scan_local : (f + 1) * scan_local], 0.0), axis=0, keepdims=True)
        for f in range(3)
    ]
    rank_parts = []
    columns = []
    for h in range(entries // LANES):
        across = device_row[:, h * LANES : (h + 1) * LANES]
        columns.append(jnp.broadcast_to(across, (LANES, LANES)).T)
        total = jnp.zeros((1, LANES), jnp.float32)
        for g in range(h + 1):
            same = columns[g] == across
            if g == h:
                same = same & (iota((LANES, LANES), 0) < iota((LANES, LANES), 1))
            total = total + jnp.sum(same.astype(jnp.float32), axis=0, keepdims=True)
        rank_parts.append(total)
    rank_row = jnp.concatenate(rank_parts, axis=1)
    slot_row = (device_row * cap + rank_row).astype(jnp.int32)
    place = (iota((devices * cap, entries), 0) == slot_row).astype(jnp.float32).astype(jnp.bfloat16)
    for a in range(COORDS + 1):
        values = data_ref[a]
        if a < COORDS:
            parts = [dot(place, part) for part in pieces(values, 3)]
            moved = (parts[0] + parts[1]) + parts[2]
        else:
            moved = dot(place, values.astype(jnp.bfloat16))
        for d in range(devices):
            out_ref[pl.ds(d * block + a * cap, cap), :] = moved[d * cap : (d + 1) * cap]
    owner_row = (div(iota((1, entries), 1), per_scan) + 1).astype(jnp.float32)
    field = div(iota((LANES, entries), 0), cap)
    picked = jnp.where(field == 0, owner_row, jnp.where(field == 1, mate_row, tile_row))
    picked = jnp.where(
        (mod(iota((LANES, entries), 0), cap).astype(jnp.float32) == rank_row) & (field < 3), picked, 0.0
    ).astype(jnp.bfloat16)
    towards = (iota((devices, entries), 0).astype(jnp.float32) == device_row).astype(jnp.float32).astype(jnp.bfloat16)
    notes = dot(towards, picked, BOTH_LANES)
    for d in range(devices):
        out_ref[pl.ds(d * block + (COORDS + 1) * cap, 1), :] = notes[d : d + 1]


def turn(x, amount):
    amount = amount % LANES
    return pltpu.roll(x, amount, 1) if amount else x


def back_layout(scan_local, groups, cap):
    span = groups * cap
    return span, HEAD * span // LANES, WIDTH * scan_local // LANES


def partner(index, k, groups):
    return index ^ k if groups & (groups - 1) == 0 else (index + k) % groups


def pair_kernel(devices, groups, group_ref, count_ref, samples_ref, recv_ref, flat_ref, back_ref, point_ref, mate_ref, note_ref):
    scan_local, _, tiles, _ = samples_ref.shape
    slots = flat_ref.shape[1]
    cap = slots // devices
    block = (COORDS + 1) * cap + 1
    for d in range(devices):
        note_ref[pl.ds(d, 1), :] = recv_ref[pl.ds(d * block + (COORDS + 1) * cap, 1), :]
    notes = note_ref[...].astype(jnp.bfloat16)
    mine = div(iota((devices, slots), 1), cap) == iota((devices, slots), 0)
    rows = []
    for f in range(3):
        spread = (iota((LANES, slots), 0) == mod(iota((LANES, slots), 1), cap) + f * cap).astype(jnp.float32)
        rows.append(
            jnp.sum(jnp.where(mine, dot(notes, spread.astype(jnp.bfloat16)), 0.0), axis=0, keepdims=True)
        )
    flag_row, mate_row, tile_row = rows
    code_row = (mate_row * tiles + tile_row).astype(jnp.int32)
    table = scan_local * tiles
    chosen = (iota((table, slots), 0) == code_row).astype(jnp.float32).astype(jnp.bfloat16)
    base = group_ref[0] * tiles
    point_ids = (base + iota((tiles, LANES), 0)) * LANES + iota((tiles, LANES), 1)
    for a in range(FIELDS):
        values = []
        for b in range(scan_local):
            value = samples_ref[b, a]
            if a >= COORDS:
                value = jnp.where(point_ids < count_ref[b], value, 0.0)
            values.append(value)
        values = jnp.concatenate(values, axis=0)
        turned = jnp.concatenate([values[h : h + LANES].T for h in range(0, table, LANES)], axis=1)
        parts = [dot(part, chosen) for part in pieces(turned, 3)]
        mate_ref[a] = (parts[0] + parts[1]) + parts[2]
    per_chunk = LANES // cap
    for c in range(slots // LANES):
        for a in range(COORDS + 1):
            stack = [
                recv_ref[pl.ds(d * block + a * cap, cap), :] for d in range(c * per_chunk, (c + 1) * per_chunk)
            ]
            point_ref[a, :, c * LANES : (c + 1) * LANES] = jnp.concatenate(stack, axis=0).T
    for c in range(slots // LANES):
        lanes = slice(c * LANES, (c + 1) * LANES)

        def step(k, sums):
            at = pl.ds(pl.multiple_of(k * 8, 8), 8)
            px, py, pz, mask = [point_ref[a, at, lanes] for a in range(COORDS + 1)]
            qx, qy, qz, nx, ny, nz = [mate_ref[a, at, lanes] for a in range(FIELDS)]
            residual = nx * (px - qx) + ny * (py - qy) + nz * (pz - qz)
            weight = mask / (1.0 + residual * residual)
            jac = [py * nz - pz * ny, pz * nx - px * nz, px * ny - py * nx, nx, ny, nz]
            scaled = [weight * j for j in jac]
            terms = [scaled[i] * jac[j] for i, j in PAIRS] + [residual * s for s in scaled]
            return tuple(s + t for s, t in zip(sums, terms))

        zero = jnp.zeros((8, LANES), jnp.float32)
        sums = lax.fori_loop(0, LANES // 8, step, (zero,) * (MAT + FIELDS))
        lines = [jnp.sum(s, axis=0, keepdims=True) for s in sums]
        blank = jnp.zeros((1, LANES), jnp.float32)
        lines[MAT:MAT] = [flag_row[:, lanes], mate_row[:, lanes], blank]
        lines += [blank] * (WIDTH - len(lines))
        flat_ref[:, lanes] = jnp.concatenate(lines, axis=0)
    scans = devices // groups
    span, slot_rows, sum_rows = back_layout(scan_local, groups, cap)
    source = div(div(iota((1, slots), 1), cap), groups) * scan_local + flag_row.astype(jnp.int32) - 1
    source = jnp.where(flag_row > 0.0, source, -1)
    source_hot = (iota((scans * scan_local, slots), 0) == source).astype(jnp.float32).astype(jnp.bfloat16)
    parts = [dot(part, source_hot, BOTH_LANES) for part in pieces(flat_ref[...], 3)]
    sums = (parts[0] + parts[1]) + parts[2]
    slot_lane = div(iota((slot_rows, LANES), 1), span)
    sum_lane = div(iota((sum_rows, LANES), 1), scan_local)
    for scan in range(scans):
        c, start = divmod(scan * span, LANES)
        body = None
        for i in range(LANES // span):
            piece = flat_ref[i * slot_rows : (i + 1) * slot_rows, c * LANES : (c + 1) * LANES]
            piece = turn(piece, i * span - start)
            body = piece if i == 0 else jnp.where(slot_lane == i, piece, body)
        c, start = divmod(scan * scan_local, LANES)
        tail = None
        for i in range(WIDTH // sum_rows):
            piece = turn(sums[i * sum_rows : (i + 1) * sum_rows, c * LANES : (c + 1) * LANES], i * scan_local - start)
            tail = piece if i == 0 else jnp.where(sum_lane == i, piece, tail)
        for c in range(groups):
            at = (scan * groups + c) * (slot_rows + sum_rows)
            back_ref[at : at + slot_rows, :] = body
            back_ref[at + slot_rows : at + slot_rows + sum_rows, :] = tail


def layout(scan_local, groups, scan_total):
    columns = scan_total // groups
    pack = max(1, LANES // columns)
    per_block = -(-(MAT + 1) // pack)
    return columns, pack, per_block


def block_rows(every, row_hot, count):
    high = every.astype(jnp.bfloat16).astype(jnp.float32)
    for part in (high, every - high):
        yield jnp.concatenate(
            [jnp.where(row_hot, part[q : q + 1], 0.0).astype(jnp.bfloat16) for q in range(count)], axis=0
        )


def held_kernel(devices, groups, scan_local, place_ref, flat_ref, *refs):
    out_refs, stage_ref = refs[:-1], refs[-1]
    slots = flat_ref.shape[1]
    cap = slots // devices
    scan_total = scan_local * (devices // groups)
    columns, pack, per_block = layout(scan_local, groups, scan_total)
    every = flat_ref[...]
    row = every[ROW_MATE : ROW_MATE + 1].astype(jnp.int32)
    other = div(div(iota((1, slots), 1), cap), groups) * scan_local + every[ROW_FLAG : ROW_FLAG + 1].astype(jnp.int32) - 1
    own = place_ref[0] * scan_local + row
    row_hot = iota((scan_local, slots), 0) == row
    column = iota((scan_total, slots), 0)
    mix = ((column == own).astype(jnp.float32) - (column == other).astype(jnp.float32)).astype(jnp.bfloat16)
    hess = sum(dot(rows, mix, BOTH_LANES) for rows in block_rows(every, row_hot, MAT))
    lane = iota((scan_local, LANES), 1)
    home = MAT // per_block
    grad = jnp.zeros((scan_local, LANES), jnp.float32)
    for q in range(FIELDS):
        value = jnp.sum(jnp.where(row_hot, every[HEAD + q : HEAD + q + 1], 0.0), axis=1, keepdims=True)
        grad = jnp.where(lane == home * columns + q, -value, grad)
    for c in range(groups):
        side, shift = divmod(c * columns, LANES)
        for r in range(per_block):
            tile = jnp.zeros((scan_local, LANES), jnp.float32)
            for k in range(pack):
                q = k * per_block + r
                if q < MAT:
                    value = hess[q * scan_local : (q + 1) * scan_local, side * LANES : (side + 1) * LANES]
                    value = turn(value, k * columns - shift)
                elif q == MAT:
                    value = grad
                else:
                    continue
                tile = jnp.where(div(lane, columns) == k, value, tile) if pack > 1 else value
            stage_ref[c, r * scan_local : (r + 1) * scan_local, :] = tile
    for k, out_ref in enumerate(out_refs):
        out_ref[...] = stage_ref[partner(place_ref[1], k, groups)]


def close_kernel(devices, groups, cap, place_ref, back_ref, *refs):
    part_refs, (hess_ref, grad_ref, every_ref, hold_ref) = refs[:groups], refs[groups:]
    scan_local, columns = hess_ref.shape[1:]
    per_block = part_refs[0].shape[0] // scan_local
    span, slot_rows, sum_rows = back_layout(scan_local, groups, cap)
    block = slot_rows + sum_rows
    senders = devices // groups
    first = place_ref[1] * (senders * block)
    lane_block = div(iota((slot_rows, LANES), 1), span)
    per_chunk = LANES // span
    for chunk in range(senders // per_chunk):
        found = [back_ref[pl.ds(first + (chunk * per_chunk + u) * block, slot_rows), :] for u in range(per_chunk)]
        for i in range(LANES // span):
            tile = None
            for u in range(per_chunk):
                piece = turn(found[u], (u - i) * span)
                tile = piece if u == 0 else jnp.where(lane_block == u, piece, tile)
            every_ref[i * slot_rows : (i + 1) * slot_rows, chunk * LANES : (chunk + 1) * LANES] = tile
    every = every_ref[...]
    total = every.shape[1]
    row = every[ROW_FLAG : ROW_FLAG + 1].astype(jnp.int32) - 1
    mate = every[ROW_MATE : ROW_MATE + 1].astype(jnp.int32)
    column = div(div(iota((1, total), 1), span), groups) * scan_local + mate
    row_hot = iota((scan_local, total), 0) == row
    mix = (iota((columns, total), 0) == column).astype(jnp.float32).astype(jnp.bfloat16)
    cross = sum(dot(rows, mix, BOTH_LANES) for rows in block_rows(every, row_hot, MAT))
    sums = back_ref[slot_rows:block, :]
    for d in range(1, devices):
        sums = sums + back_ref[d * block + slot_rows : (d + 1) * block, :]
    line = iota((scan_local, LANES), 0)
    lane = iota((scan_local, LANES), 1)

    def by_row(q):
        i, r = divmod(q, sum_rows)
        return jnp.sum(jnp.where(lane == line + i * scan_local, sums[r : r + 1], 0.0), axis=1, keepdims=True)

    whole = part_refs[0][...]
    for part_ref in part_refs[1:]:
        whole = whole + part_ref[...]
    offset = place_ref[0] * scan_local - place_ref[1] * columns
    diagonal = iota((scan_local, columns), 1) == iota((scan_local, columns), 0) + offset
    for q in range(MAT):
        k, r = divmod(q, per_block)
        tile = whole[r * scan_local : (r + 1) * scan_local, k * columns : (k + 1) * columns]
        tile = tile - cross[q * scan_local : (q + 1) * scan_local]
        tile = tile + jnp.where(diagonal, by_row(q), 0.0)
        i, j = PAIRS[q]
        hess_ref[i * FIELDS + j] = tile
        if i != j:
            hess_ref[j * FIELDS + i] = tile
    k, r = divmod(MAT, per_block)
    grad = turn(whole[r * scan_local : (r + 1) * scan_local], -k * columns)
    for q in range(FIELDS):
        grad = grad + jnp.where(lane == q, by_row(HEAD + q), 0.0)
    hold_ref[...] = grad
    part = scan_local // groups
    grad_ref[...] = hold_ref[pl.ds(place_ref[1] * part, part), 0:FIELDS]


def call(kernel, out_shape, smem, vmem, scratch=()):
    return pl.pallas_call(
        kernel,
        out_shape=out_shape,
        in_specs=[pl.BlockSpec(memory_space=pltpu.SMEM)] * smem + [pl.BlockSpec(memory_space=pltpu.VMEM)] * vmem,
        scratch_shapes=list(scratch),
    )


def f32(*shape):
    return jax.ShapeDtypeStruct(shape, jnp.float32)


def exchange(x, axes):
    count, width = x.shape
    moved = lax.all_to_all(x.reshape(count, 1, width), axes, split_axis=0, concat_axis=0, tiled=True)
    return moved.reshape(count, width)


def local(samples, point_count, corr_scan, corr_tile, corr_src):
    devices = lax.axis_size(AXES)
    groups = lax.axis_size("grp")
    samples = samples.transpose(0, 2, 1, 3)
    scan_local, tiles, per_scan, entries, cap, block = sizes(samples.shape, corr_scan.shape, devices)
    slots = devices * cap
    scan_total = scan_local * (devices // groups)
    columns, pack, per_block = layout(scan_local, groups, scan_total)
    group = lax.axis_index("grp").astype(jnp.int32)
    place = jnp.stack([lax.axis_index("scan").astype(jnp.int32), group])
    group = group.reshape(1)
    _, slot_rows, sum_rows = back_layout(scan_local, groups, cap)

    def bind(kernel, *args):
        return lambda *refs: kernel(*args, *refs)

    sent = call(
        bind(send_kernel, devices, groups),
        f32(devices * block, LANES),
        2,
        4,
        [pltpu.VMEM((COORDS + 1, entries, LANES), jnp.float32)],
    )(group, point_count, samples, corr_scan, corr_tile, corr_src)
    received = exchange(sent, AXES)
    flat, back = call(
        bind(pair_kernel, devices, groups),
        (f32(WIDTH, slots), f32(devices * (slot_rows + sum_rows), LANES)),
        2,
        2,
        [
            pltpu.VMEM((COORDS + 1, LANES, slots), jnp.float32),
            pltpu.VMEM((FIELDS, LANES, slots), jnp.float32),
            pltpu.VMEM((devices, LANES), jnp.float32),
        ],
    )(group, point_count, samples, received)
    back = exchange(back, AXES)
    share = f32(per_block * scan_local, LANES)
    shares = call(
        bind(held_kernel, devices, groups, scan_local),
        (share,) * groups,
        1,
        1,
        [pltpu.VMEM((groups,) + share.shape, jnp.float32)],
    )(place, flat)
    shares = [shares[0]] + [
        lax.ppermute(shares[k], "grp", [(g, partner(g, k, groups)) for g in range(groups)]) for k in range(1, groups)
    ]
    hess, grad = call(
        bind(close_kernel, devices, groups, cap),
        (f32(FIELDS * FIELDS, scan_local, columns), f32(scan_local // groups, FIELDS)),
        1,
        1 + groups,
        [
            pltpu.VMEM((HEAD, (devices // groups) * groups * cap), jnp.float32),
            pltpu.VMEM((scan_local, LANES), jnp.float32),
        ],
    )(place, back, *shares)
    return hess.reshape(FIELDS, FIELDS, scan_local, columns).transpose(2, 0, 1, 3), grad


def solution(mesh):
    placed = (
        P("scan", "grp", None, None),
        P("scan"),
        P("scan", "grp"),
        P("scan", "grp"),
        P("scan", "grp", None),
    )
    return jax.shard_map(
        local,
        mesh=mesh,
        in_specs=placed,
        out_specs=(P("scan", None, None, "grp"), P(AXES, None)),
        check_vma=False,
    )
```

```python
import jax
import jax.numpy as jnp
from jax import lax
from jax.experimental import pallas as pl
from jax.experimental.pallas import tpu as pltpu
from jax.sharding import PartitionSpec as P

LANES = 128
COORDS = 3
FIELDS = 6
PAIRS = [(i, j) for i in range(FIELDS) for j in range(i, FIELDS)]
MAT = len(PAIRS)
ROW_FLAG = MAT
ROW_MATE = MAT + 1
HEAD = MAT + 3
WIDTH = 32
BOTH_LANES = (((1,), (1,)), ((), ()))
AXES = ("scan", "grp")


def div(x, n):
    if n & (n - 1) == 0:
        return lax.shift_right_logical(x, jnp.int32(n.bit_length() - 1))
    return x // n


def mod(x, n):
    if n & (n - 1) == 0:
        return x & (n - 1)
    return x % n


def iota(shape, dim):
    return lax.broadcasted_iota(jnp.int32, shape, dim)


def pieces(x, count):
    parts = []
    for _ in range(count - 1):
        part = x.astype(jnp.bfloat16)
        parts.append(part)
        x = x - part.astype(jnp.float32)
    parts.append(x.astype(jnp.bfloat16))
    return parts


def dot(a, b, dims=(((1,), (0,)), ((), ()))):
    return lax.dot_general(a, b, dims, preferred_element_type=jnp.float32)


def sizes(samples_shape, entries_shape, devices):
    scan_local, _, tiles, _ = samples_shape
    per_scan = entries_shape[1]
    entries = scan_local * per_scan
    cap = 2 * entries // devices
    return scan_local, tiles, per_scan, entries, cap, (COORDS + 1) * cap + 1


def send_kernel(devices, groups, group_ref, count_ref, samples_ref, scan_ref, tile_ref, src_ref, out_ref, data_ref):
    scan_local, tiles, per_scan, entries, cap, block = sizes(samples_ref.shape, scan_ref.shape, devices)
    group_points = tiles * LANES

    def one_scan(s, carry):
        first = group_ref[0] * group_points
        limit = count_ref[s] - first
        for h in range(per_scan // 8):
            ids = src_ref[s, pl.ds(h * 8, 8), :]
            lane = mod(ids, LANES)
            tile = div(ids, LANES)
            found = [jnp.zeros((8, LANES), jnp.float32) for _ in range(COORDS)]
            for t in range(tiles):
                here = tile == t
                for a in range(COORDS):
                    row = jnp.broadcast_to(samples_ref[s, a, t : t + 1, :], (8, LANES))
                    found[a] = jnp.where(here, jnp.take_along_axis(row, lane, axis=1), found[a])
            at = pl.multiple_of(s * per_scan + h * 8, 8)
            for a in range(COORDS):
                data_ref[a, pl.ds(at, 8), :] = found[a]
            data_ref[COORDS, pl.ds(at, 8), :] = (ids < limit).astype(jnp.float32)
        return carry

    lax.fori_loop(0, scan_local, one_scan, 0)

    scans = scan_ref[...]
    tile_ids = tile_ref[...]
    device = div(scans, scan_local) * groups + div(tile_ids, tiles)
    stacked = jnp.concatenate(
        [device.astype(jnp.float32), mod(scans, scan_local).astype(jnp.float32), mod(tile_ids, tiles).astype(jnp.float32)],
        axis=0,
    ).astype(jnp.bfloat16)
    spread = (mod(iota((per_scan, entries), 1), per_scan) == iota((per_scan, entries), 0)).astype(jnp.float32)
    wide = dot(stacked, spread.astype(jnp.bfloat16))
    own = div(iota((scan_local, entries), 1), per_scan) == iota((scan_local, entries), 0)
    device_row, mate_row, tile_row = [
        jnp.sum(jnp.where(own, wide[f * scan_local : (f + 1) * scan_local], 0.0), axis=0, keepdims=True)
        for f in range(3)
    ]
    rank_parts = []
    columns = []
    for h in range(entries // LANES):
        across = device_row[:, h * LANES : (h + 1) * LANES]
        columns.append(jnp.broadcast_to(across, (LANES, LANES)).T)
        total = jnp.zeros((1, LANES), jnp.float32)
        for g in range(h + 1):
            same = columns[g] == across
            if g == h:
                same = same & (iota((LANES, LANES), 0) < iota((LANES, LANES), 1))
            total = total + jnp.sum(same.astype(jnp.float32), axis=0, keepdims=True)
        rank_parts.append(total)
    rank_row = jnp.concatenate(rank_parts, axis=1)
    slot_row = (device_row * cap + rank_row).astype(jnp.int32)
    place = (iota((devices * cap, entries), 0) == slot_row).astype(jnp.float32).astype(jnp.bfloat16)
    for a in range(COORDS + 1):
        values = data_ref[a]
        if a < COORDS:
            parts = [dot(place, part) for part in pieces(values, 3)]
            moved = (parts[0] + parts[1]) + parts[2]
        else:
            moved = dot(place, values.astype(jnp.bfloat16))
        for d in range(devices):
            out_ref[pl.ds(d * block + a * cap, cap), :] = moved[d * cap : (d + 1) * cap]
    owner_row = (div(iota((1, entries), 1), per_scan) + 1).astype(jnp.float32)
    field = div(iota((LANES, entries), 0), cap)
    picked = jnp.where(field == 0, owner_row, jnp.where(field == 1, mate_row, tile_row))
    picked = jnp.where(
        (mod(iota((LANES, entries), 0), cap).astype(jnp.float32) == rank_row) & (field < 3), picked, 0.0
    ).astype(jnp.bfloat16)
    towards = (iota((devices, entries), 0).astype(jnp.float32) == device_row).astype(jnp.float32).astype(jnp.bfloat16)
    notes = dot(towards, picked, BOTH_LANES)
    for d in range(devices):
        out_ref[pl.ds(d * block + (COORDS + 1) * cap, 1), :] = notes[d : d + 1]


def turn(x, amount):
    amount = amount % LANES
    return pltpu.roll(x, amount, 1) if amount else x


def back_layout(scan_local, groups, cap):
    span = groups * cap
    return span, HEAD * span // LANES, WIDTH * scan_local // LANES


def partner(index, k, groups):
    return index ^ k if groups & (groups - 1) == 0 else (index + k) % groups


def pair_kernel(devices, groups, group_ref, count_ref, samples_ref, recv_ref, flat_ref, back_ref, point_ref, mate_ref, note_ref):
    scan_local, _, tiles, _ = samples_ref.shape
    slots = flat_ref.shape[1]
    cap = slots // devices
    block = (COORDS + 1) * cap + 1
    for d in range(devices):
        note_ref[pl.ds(d, 1), :] = recv_ref[pl.ds(d * block + (COORDS + 1) * cap, 1), :]
    notes = note_ref[...].astype(jnp.bfloat16)
    mine = div(iota((devices, slots), 1), cap) == iota((devices, slots), 0)
    rows = []
    for f in range(3):
        spread = (iota((LANES, slots), 0) == mod(iota((LANES, slots), 1), cap) + f * cap).astype(jnp.float32)
        rows.append(
            jnp.sum(jnp.where(mine, dot(notes, spread.astype(jnp.bfloat16)), 0.0), axis=0, keepdims=True)
        )
    flag_row, mate_row, tile_row = rows
    code_row = (mate_row * tiles + tile_row).astype(jnp.int32)
    table = scan_local * tiles
    chosen = (iota((table, slots), 0) == code_row).astype(jnp.float32).astype(jnp.bfloat16)
    base = group_ref[0] * tiles
    point_ids = (base + iota((tiles, LANES), 0)) * LANES + iota((tiles, LANES), 1)
    for a in range(FIELDS):
        values = []
        for b in range(scan_local):
            value = samples_ref[b, a]
            if a >= COORDS:
                value = jnp.where(point_ids < count_ref[b], value, 0.0)
            values.append(value)
        values = jnp.concatenate(values, axis=0)
        turned = jnp.concatenate([values[h : h + LANES].T for h in range(0, table, LANES)], axis=1)
        parts = [dot(part, chosen) for part in pieces(turned, 3)]
        mate_ref[a] = (parts[0] + parts[1]) + parts[2]
    per_chunk = LANES // cap
    for c in range(slots // LANES):
        for a in range(COORDS + 1):
            stack = [
                recv_ref[pl.ds(d * block + a * cap, cap), :] for d in range(c * per_chunk, (c + 1) * per_chunk)
            ]
            point_ref[a, :, c * LANES : (c + 1) * LANES] = jnp.concatenate(stack, axis=0).T
    for c in range(slots // LANES):
        lanes = slice(c * LANES, (c + 1) * LANES)

        def step(k, sums):
            at = pl.ds(pl.multiple_of(k * 8, 8), 8)
            px, py, pz, mask = [point_ref[a, at, lanes] for a in range(COORDS + 1)]
            qx, qy, qz, nx, ny, nz = [mate_ref[a, at, lanes] for a in range(FIELDS)]
            residual = nx * (px - qx) + ny * (py - qy) + nz * (pz - qz)
            weight = mask / (1.0 + residual * residual)
            jac = [py * nz - pz * ny, pz * nx - px * nz, px * ny - py * nx, nx, ny, nz]
            scaled = [weight * j for j in jac]
            terms = [scaled[i] * jac[j] for i, j in PAIRS] + [residual * s for s in scaled]
            return tuple(s + t for s, t in zip(sums, terms))

        zero = jnp.zeros((8, LANES), jnp.float32)
        sums = lax.fori_loop(0, LANES // 8, step, (zero,) * (MAT + FIELDS))
        lines = [jnp.sum(s, axis=0, keepdims=True) for s in sums]
        blank = jnp.zeros((1, LANES), jnp.float32)
        lines[MAT:MAT] = [flag_row[:, lanes], mate_row[:, lanes], blank]
        lines += [blank] * (WIDTH - len(lines))
        flat_ref[:, lanes] = jnp.concatenate(lines, axis=0)
    scans = devices // groups
    span, slot_rows, sum_rows = back_layout(scan_local, groups, cap)
    source = div(div(iota((1, slots), 1), cap), groups) * scan_local + flag_row.astype(jnp.int32) - 1
    source = jnp.where(flag_row > 0.0, source, -1)
    source_hot = (iota((scans * scan_local, slots), 0) == source).astype(jnp.float32).astype(jnp.bfloat16)
    parts = [dot(part, source_hot, BOTH_LANES) for part in pieces(flat_ref[...], 3)]
    sums = (parts[0] + parts[1]) + parts[2]
    slot_lane = div(iota((slot_rows, LANES), 1), span)
    sum_lane = div(iota((sum_rows, LANES), 1), scan_local)
    for scan in range(scans):
        c, start = divmod(scan * span, LANES)
        body = None
        for i in range(LANES // span):
            piece = flat_ref[i * slot_rows : (i + 1) * slot_rows, c * LANES : (c + 1) * LANES]
            piece = turn(piece, i * span - start)
            body = piece if i == 0 else jnp.where(slot_lane == i, piece, body)
        c, start = divmod(scan * scan_local, LANES)
        tail = None
        for i in range(WIDTH // sum_rows):
            piece = turn(sums[i * sum_rows : (i + 1) * sum_rows, c * LANES : (c + 1) * LANES], i * scan_local - start)
            tail = piece if i == 0 else jnp.where(sum_lane == i, piece, tail)
        for c in range(groups):
            at = (scan * groups + c) * (slot_rows + sum_rows)
            back_ref[at : at + slot_rows, :] = body
            back_ref[at + slot_rows : at + slot_rows + sum_rows, :] = tail


def layout(scan_local, groups, scan_total):
    columns = scan_total // groups
    pack = max(1, LANES // columns)
    per_block = -(-(MAT + 1) // pack)
    return columns, pack, per_block


def block_rows(every, row_hot, count):
    high = every.astype(jnp.bfloat16).astype(jnp.float32)
    for part in (high, every - high):
        yield jnp.concatenate(
            [jnp.where(row_hot, part[q : q + 1], 0.0).astype(jnp.bfloat16) for q in range(count)], axis=0
        )


def held_kernel(devices, groups, scan_local, place_ref, flat_ref, *refs):
    out_refs, stage_ref = refs[:-1], refs[-1]
    slots = flat_ref.shape[1]
    cap = slots // devices
    scan_total = scan_local * (devices // groups)
    columns, pack, per_block = layout(scan_local, groups, scan_total)
    every = flat_ref[...]
    row = every[ROW_MATE : ROW_MATE + 1].astype(jnp.int32)
    other = div(div(iota((1, slots), 1), cap), groups) * scan_local + every[ROW_FLAG : ROW_FLAG + 1].astype(jnp.int32) - 1
    own = place_ref[0] * scan_local + row
    row_hot = iota((scan_local, slots), 0) == row
    column = iota((scan_total, slots), 0)
    mix = ((column == own).astype(jnp.float32) - (column == other).astype(jnp.float32)).astype(jnp.bfloat16)
    hess = sum(dot(rows, mix, BOTH_LANES) for rows in block_rows(every, row_hot, MAT))
    lane = iota((scan_local, LANES), 1)
    home = MAT // per_block
    grad = jnp.zeros((scan_local, LANES), jnp.float32)
    for q in range(FIELDS):
        value = jnp.sum(jnp.where(row_hot, every[HEAD + q : HEAD + q + 1], 0.0), axis=1, keepdims=True)
        grad = jnp.where(lane == home * columns + q, -value, grad)
    for c in range(groups):
        side, shift = divmod(c * columns, LANES)
        for r in range(per_block):
            tile = jnp.zeros((scan_local, LANES), jnp.float32)
            for k in range(pack):
                q = k * per_block + r
                if q < MAT:
                    value = hess[q * scan_local : (q + 1) * scan_local, side * LANES : (side + 1) * LANES]
                    value = turn(value, k * columns - shift)
                elif q == MAT:
                    value = grad
                else:
                    continue
                tile = jnp.where(div(lane, columns) == k, value, tile) if pack > 1 else value
            stage_ref[c, r * scan_local : (r + 1) * scan_local, :] = tile
    for k, out_ref in enumerate(out_refs):
        out_ref[...] = stage_ref[partner(place_ref[1], k, groups)]


def close_kernel(devices, groups, cap, place_ref, back_ref, *refs):
    part_refs, (hess_ref, grad_ref, every_ref, hold_ref) = refs[:groups], refs[groups:]
    scan_local, columns = hess_ref.shape[1:]
    per_block = part_refs[0].shape[0] // scan_local
    span, slot_rows, sum_rows = back_layout(scan_local, groups, cap)
    block = slot_rows + sum_rows
    senders = devices // groups
    first = place_ref[1] * (senders * block)
    lane_block = div(iota((slot_rows, LANES), 1), span)
    per_chunk = LANES // span
    for chunk in range(senders // per_chunk):
        found = [back_ref[pl.ds(first + (chunk * per_chunk + u) * block, slot_rows), :] for u in range(per_chunk)]
        for i in range(LANES // span):
            tile = None
            for u in range(per_chunk):
                piece = turn(found[u], (u - i) * span)
                tile = piece if u == 0 else jnp.where(lane_block == u, piece, tile)
            every_ref[i * slot_rows : (i + 1) * slot_rows, chunk * LANES : (chunk + 1) * LANES] = tile
    every = every_ref[...]
    total = every.shape[1]
    row = every[ROW_FLAG : ROW_FLAG + 1].astype(jnp.int32) - 1
    mate = every[ROW_MATE : ROW_MATE + 1].astype(jnp.int32)
    column = div(div(iota((1, total), 1), span), groups) * scan_local + mate
    row_hot = iota((scan_local, total), 0) == row
    mix = (iota((columns, total), 0) == column).astype(jnp.float32).astype(jnp.bfloat16)
    cross = sum(dot(rows, mix, BOTH_LANES) for rows in block_rows(every, row_hot, MAT))
    sums = back_ref[slot_rows:block, :]
    for d in range(1, devices):
        sums = sums + back_ref[d * block + slot_rows : (d + 1) * block, :]
    line = iota((scan_local, LANES), 0)
    lane = iota((scan_local, LANES), 1)

    def by_row(q):
        i, r = divmod(q, sum_rows)
        return jnp.sum(jnp.where(lane == line + i * scan_local, sums[r : r + 1], 0.0), axis=1, keepdims=True)

    whole = part_refs[0][...]
    for part_ref in part_refs[1:]:
        whole = whole + part_ref[...]
    offset = place_ref[0] * scan_local - place_ref[1] * columns
    diagonal = iota((scan_local, columns), 1) == iota((scan_local, columns), 0) + offset
    for q in range(MAT):
        k, r = divmod(q, per_block)
        tile = whole[r * scan_local : (r + 1) * scan_local, k * columns : (k + 1) * columns]
        tile = tile - cross[q * scan_local : (q + 1) * scan_local]
        tile = tile + jnp.where(diagonal, by_row(q), 0.0)
        i, j = PAIRS[q]
        hess_ref[i * FIELDS + j] = tile
        if i != j:
            hess_ref[j * FIELDS + i] = tile
    k, r = divmod(MAT, per_block)
    grad = turn(whole[r * scan_local : (r + 1) * scan_local], -k * columns)
    for q in range(FIELDS):
        grad = grad + jnp.where(lane == q, by_row(HEAD + q), 0.0)
    hold_ref[...] = grad
    part = scan_local // groups
    grad_ref[...] = hold_ref[pl.ds(place_ref[1] * part, part), 0:FIELDS]


def call(kernel, out_shape, smem, vmem, scratch=()):
    body = pl.pallas_call(
        kernel,
        out_shape=out_shape,
        in_specs=[pl.BlockSpec(memory_space=pltpu.SMEM)] * smem + [pl.BlockSpec(memory_space=pltpu.VMEM)] * vmem,
        scratch_shapes=list(scratch),
    )

    def run(*args):
        args = args[:smem] + tuple(pltpu.with_memory_space_constraint(x, pltpu.VMEM) for x in args[smem:])
        return body(*args)

    return run


def f32(*shape):
    return jax.ShapeDtypeStruct(shape, jnp.float32)


def near(*shape):
    return pltpu.VMEM(shape, jnp.float32)


def exchange(x, axes):
    count, width = x.shape
    moved = lax.all_to_all(x.reshape(count, 1, width), axes, split_axis=0, concat_axis=0, tiled=True)
    return moved.reshape(count, width)


def local(samples, point_count, corr_scan, corr_tile, corr_src):
    devices = lax.axis_size(AXES)
    groups = lax.axis_size("grp")
    samples = samples.transpose(0, 2, 1, 3)
    scan_local, tiles, per_scan, entries, cap, block = sizes(samples.shape, corr_scan.shape, devices)
    slots = devices * cap
    scan_total = scan_local * (devices // groups)
    columns, pack, per_block = layout(scan_local, groups, scan_total)
    group = lax.axis_index("grp").astype(jnp.int32)
    place = jnp.stack([lax.axis_index("scan").astype(jnp.int32), group])
    group = group.reshape(1)
    _, slot_rows, sum_rows = back_layout(scan_local, groups, cap)

    def bind(kernel, *args):
        return lambda *refs: kernel(*args, *refs)

    sent = call(
        bind(send_kernel, devices, groups),
        near(devices * block, LANES),
        2,
        4,
        [pltpu.VMEM((COORDS + 1, entries, LANES), jnp.float32)],
    )(group, point_count, samples, corr_scan, corr_tile, corr_src)
    received = exchange(sent, AXES)
    flat, back = call(
        bind(pair_kernel, devices, groups),
        (near(WIDTH, slots), near(devices * (slot_rows + sum_rows), LANES)),
        2,
        2,
        [
            pltpu.VMEM((COORDS + 1, LANES, slots), jnp.float32),
            pltpu.VMEM((FIELDS, LANES, slots), jnp.float32),
            pltpu.VMEM((devices, LANES), jnp.float32),
        ],
    )(group, point_count, samples, received)
    back = exchange(back, AXES)
    share = near(per_block * scan_local, LANES)
    shares = call(
        bind(held_kernel, devices, groups, scan_local),
        (share,) * groups,
        1,
        1,
        [pltpu.VMEM((groups,) + share.shape, jnp.float32)],
    )(place, flat)
    shares = [shares[0]] + [
        lax.ppermute(shares[k], "grp", [(g, partner(g, k, groups)) for g in range(groups)]) for k in range(1, groups)
    ]
    hess, grad = call(
        bind(close_kernel, devices, groups, cap),
        (f32(FIELDS * FIELDS, scan_local, columns), f32(scan_local // groups, FIELDS)),
        1,
        1 + groups,
        [
            pltpu.VMEM((HEAD, (devices // groups) * groups * cap), jnp.float32),
            pltpu.VMEM((scan_local, LANES), jnp.float32),
        ],
    )(place, back, *shares)
    return hess.reshape(FIELDS, FIELDS, scan_local, columns).transpose(2, 0, 1, 3), grad


def solution(mesh):
    placed = (
        P("scan", "grp", None, None),
        P("scan"),
        P("scan", "grp"),
        P("scan", "grp"),
        P("scan", "grp", None),
    )
    return jax.shard_map(
        local,
        mesh=mesh,
        in_specs=placed,
        out_specs=(P("scan", None, None, "grp"), P(AXES, None)),
        check_vma=False,
    )
```

```python
import jax
import jax.numpy as jnp
from jax import lax
from jax.experimental import pallas as pl
from jax.experimental.pallas import tpu as pltpu
from jax.sharding import PartitionSpec as P

LANES = 128
COORDS = 3
FIELDS = 6
PAIRS = [(i, j) for i in range(FIELDS) for j in range(i, FIELDS)]
MAT = len(PAIRS)
ROW_FLAG = MAT
ROW_MATE = MAT + 1
HEAD = MAT + 3
WIDTH = 32
BOTH_LANES = (((1,), (1,)), ((), ()))
AXES = ("scan", "grp")


def div(x, n):
    if n & (n - 1) == 0:
        return lax.shift_right_logical(x, jnp.int32(n.bit_length() - 1))
    return x // n


def mod(x, n):
    if n & (n - 1) == 0:
        return x & (n - 1)
    return x % n


def iota(shape, dim):
    return lax.broadcasted_iota(jnp.int32, shape, dim)


def pieces(x, count):
    parts = []
    for _ in range(count - 1):
        part = x.astype(jnp.bfloat16)
        parts.append(part)
        x = x - part.astype(jnp.float32)
    parts.append(x.astype(jnp.bfloat16))
    return parts


def dot(a, b, dims=(((1,), (0,)), ((), ()))):
    return lax.dot_general(a, b, dims, preferred_element_type=jnp.float32)


def sizes(samples_shape, entries_shape, devices):
    scan_local, _, tiles, _ = samples_shape
    per_scan = entries_shape[1]
    entries = scan_local * per_scan
    cap = 2 * entries // devices
    return scan_local, tiles, per_scan, entries, cap, (COORDS + 1) * cap + 1


def send_kernel(
    devices,
    groups,
    group_ref,
    count_ref,
    samples_hbm,
    scan_hbm,
    tile_hbm,
    src_hbm,
    out_ref,
    samples_ref,
    scan_ref,
    tile_ref,
    src_ref,
    data_ref,
    sems,
):
    scan_local, tiles, per_scan, entries, cap, block = sizes(samples_ref.shape, scan_ref.shape, devices)
    group_points = tiles * LANES
    pairs = ((scan_hbm, scan_ref), (tile_hbm, tile_ref), (src_hbm, src_ref), (samples_hbm, samples_ref))
    loads = [pltpu.make_async_copy(far, here, sems.at[k]) for k, (far, here) in enumerate(pairs)]
    for load in loads:
        load.start()
    for load in loads[:2]:
        load.wait()

    scans = scan_ref[...]
    tile_ids = tile_ref[...]
    device = div(scans, scan_local) * groups + div(tile_ids, tiles)
    stacked = jnp.concatenate(
        [device.astype(jnp.float32), mod(scans, scan_local).astype(jnp.float32), mod(tile_ids, tiles).astype(jnp.float32)],
        axis=0,
    ).astype(jnp.bfloat16)
    spread = (mod(iota((per_scan, entries), 1), per_scan) == iota((per_scan, entries), 0)).astype(jnp.float32)
    wide = dot(stacked, spread.astype(jnp.bfloat16))
    own = div(iota((scan_local, entries), 1), per_scan) == iota((scan_local, entries), 0)
    device_row, mate_row, tile_row = [
        jnp.sum(jnp.where(own, wide[f * scan_local : (f + 1) * scan_local], 0.0), axis=0, keepdims=True)
        for f in range(3)
    ]
    rank_parts = []
    columns = []
    for h in range(entries // LANES):
        across = device_row[:, h * LANES : (h + 1) * LANES]
        columns.append(jnp.broadcast_to(across, (LANES, LANES)).T)
        total = jnp.zeros((1, LANES), jnp.float32)
        for g in range(h + 1):
            same = columns[g] == across
            if g == h:
                same = same & (iota((LANES, LANES), 0) < iota((LANES, LANES), 1))
            total = total + jnp.sum(same.astype(jnp.float32), axis=0, keepdims=True)
        rank_parts.append(total)
    rank_row = jnp.concatenate(rank_parts, axis=1)
    slot_row = (device_row * cap + rank_row).astype(jnp.int32)
    place = (iota((devices * cap, entries), 0) == slot_row).astype(jnp.float32).astype(jnp.bfloat16)
    owner_row = (div(iota((1, entries), 1), per_scan) + 1).astype(jnp.float32)
    field = div(iota((LANES, entries), 0), cap)
    picked = jnp.where(field == 0, owner_row, jnp.where(field == 1, mate_row, tile_row))
    picked = jnp.where(
        (mod(iota((LANES, entries), 0), cap).astype(jnp.float32) == rank_row) & (field < 3), picked, 0.0
    ).astype(jnp.bfloat16)
    towards = (iota((devices, entries), 0).astype(jnp.float32) == device_row).astype(jnp.float32).astype(jnp.bfloat16)
    notes = dot(towards, picked, BOTH_LANES)
    for d in range(devices):
        out_ref[pl.ds(d * block + (COORDS + 1) * cap, 1), :] = notes[d : d + 1]

    for load in loads[2:]:
        load.wait()

    def one_scan(s, carry):
        limit = count_ref[s] - group_ref[0] * group_points
        for h in range(per_scan // 8):
            ids = src_ref[s, pl.ds(h * 8, 8), :]
            lane = mod(ids, LANES)
            tile = div(ids, LANES)
            found = [jnp.zeros((8, LANES), jnp.float32) for _ in range(COORDS)]
            for t in range(tiles):
                here = tile == t
                for a in range(COORDS):
                    row = jnp.broadcast_to(samples_ref[s, a, t : t + 1, :], (8, LANES))
                    found[a] = jnp.where(here, jnp.take_along_axis(row, lane, axis=1), found[a])
            at = pl.multiple_of(s * per_scan + h * 8, 8)
            for a in range(COORDS):
                data_ref[a, pl.ds(at, 8), :] = found[a]
            data_ref[COORDS, pl.ds(at, 8), :] = (ids < limit).astype(jnp.float32)
        return carry

    lax.fori_loop(0, scan_local, one_scan, 0, unroll=4)

    for a in range(COORDS + 1):
        values = data_ref[a]
        if a < COORDS:
            parts = [dot(place, part) for part in pieces(values, 3)]
            moved = (parts[0] + parts[1]) + parts[2]
        else:
            moved = dot(place, values.astype(jnp.bfloat16))
        for d in range(devices):
            out_ref[pl.ds(d * block + a * cap, cap), :] = moved[d * cap : (d + 1) * cap]


def turn(x, amount):
    amount = amount % LANES
    return pltpu.roll(x, amount, 1) if amount else x


def back_layout(scan_local, groups, cap):
    span = groups * cap
    return span, HEAD * span // LANES, WIDTH * scan_local // LANES


def partner(index, k, groups):
    return index ^ k if groups & (groups - 1) == 0 else (index + k) % groups


def pair_kernel(devices, groups, group_ref, count_ref, samples_ref, recv_ref, flat_ref, back_ref, point_ref, mate_ref, note_ref):
    scan_local, _, tiles, _ = samples_ref.shape
    slots = flat_ref.shape[1]
    cap = slots // devices
    block = (COORDS + 1) * cap + 1
    for d in range(devices):
        note_ref[pl.ds(d, 1), :] = recv_ref[pl.ds(d * block + (COORDS + 1) * cap, 1), :]
    notes = note_ref[...].astype(jnp.bfloat16)
    mine = div(iota((devices, slots), 1), cap) == iota((devices, slots), 0)
    rows = []
    for f in range(3):
        spread = (iota((LANES, slots), 0) == mod(iota((LANES, slots), 1), cap) + f * cap).astype(jnp.float32)
        rows.append(
            jnp.sum(jnp.where(mine, dot(notes, spread.astype(jnp.bfloat16)), 0.0), axis=0, keepdims=True)
        )
    flag_row, mate_row, tile_row = rows
    code_row = (mate_row * tiles + tile_row).astype(jnp.int32)
    table = scan_local * tiles
    chosen = (iota((table, slots), 0) == code_row).astype(jnp.float32).astype(jnp.bfloat16)
    base = group_ref[0] * tiles
    point_ids = (base + iota((tiles, LANES), 0)) * LANES + iota((tiles, LANES), 1)
    for a in range(FIELDS):
        values = []
        for b in range(scan_local):
            value = samples_ref[b, a]
            if a >= COORDS:
                value = jnp.where(point_ids < count_ref[b], value, 0.0)
            values.append(value)
        values = jnp.concatenate(values, axis=0)
        turned = jnp.concatenate([values[h : h + LANES].T for h in range(0, table, LANES)], axis=1)
        parts = [dot(part, chosen) for part in pieces(turned, 3)]
        mate_ref[a] = (parts[0] + parts[1]) + parts[2]
    per_chunk = LANES // cap
    for c in range(slots // LANES):
        for a in range(COORDS + 1):
            stack = [
                recv_ref[pl.ds(d * block + a * cap, cap), :] for d in range(c * per_chunk, (c + 1) * per_chunk)
            ]
            point_ref[a, :, c * LANES : (c + 1) * LANES] = jnp.concatenate(stack, axis=0).T
    for c in range(slots // LANES):
        lanes = slice(c * LANES, (c + 1) * LANES)

        def step(k, sums):
            at = pl.ds(pl.multiple_of(k * 8, 8), 8)
            px, py, pz, mask = [point_ref[a, at, lanes] for a in range(COORDS + 1)]
            qx, qy, qz, nx, ny, nz = [mate_ref[a, at, lanes] for a in range(FIELDS)]
            residual = nx * (px - qx) + ny * (py - qy) + nz * (pz - qz)
            weight = mask / (1.0 + residual * residual)
            jac = [py * nz - pz * ny, pz * nx - px * nz, px * ny - py * nx, nx, ny, nz]
            scaled = [weight * j for j in jac]
            terms = [scaled[i] * jac[j] for i, j in PAIRS] + [residual * s for s in scaled]
            return tuple(s + t for s, t in zip(sums, terms))

        zero = jnp.zeros((8, LANES), jnp.float32)
        sums = lax.fori_loop(0, LANES // 8, step, (zero,) * (MAT + FIELDS), unroll=4)
        lines = [jnp.sum(s, axis=0, keepdims=True) for s in sums]
        blank = jnp.zeros((1, LANES), jnp.float32)
        lines[MAT:MAT] = [flag_row[:, lanes], mate_row[:, lanes], blank]
        lines += [blank] * (WIDTH - len(lines))
        flat_ref[:, lanes] = jnp.concatenate(lines, axis=0)
    scans = devices // groups
    span, slot_rows, sum_rows = back_layout(scan_local, groups, cap)
    source = div(div(iota((1, slots), 1), cap), groups) * scan_local + flag_row.astype(jnp.int32) - 1
    source = jnp.where(flag_row > 0.0, source, -1)
    source_hot = (iota((scans * scan_local, slots), 0) == source).astype(jnp.float32).astype(jnp.bfloat16)
    parts = [dot(part, source_hot, BOTH_LANES) for part in pieces(flat_ref[...], 3)]
    sums = (parts[0] + parts[1]) + parts[2]
    slot_lane = div(iota((slot_rows, LANES), 1), span)
    sum_lane = div(iota((sum_rows, LANES), 1), scan_local)
    for scan in range(scans):
        c, start = divmod(scan * span, LANES)
        body = None
        for i in range(LANES // span):
            piece = flat_ref[i * slot_rows : (i + 1) * slot_rows, c * LANES : (c + 1) * LANES]
            piece = turn(piece, i * span - start)
            body = piece if i == 0 else jnp.where(slot_lane == i, piece, body)
        c, start = divmod(scan * scan_local, LANES)
        tail = None
        for i in range(WIDTH // sum_rows):
            piece = turn(sums[i * sum_rows : (i + 1) * sum_rows, c * LANES : (c + 1) * LANES], i * scan_local - start)
            tail = piece if i == 0 else jnp.where(sum_lane == i, piece, tail)
        for c in range(groups):
            at = (scan * groups + c) * (slot_rows + sum_rows)
            back_ref[at : at + slot_rows, :] = body
            back_ref[at + slot_rows : at + slot_rows + sum_rows, :] = tail


def layout(scan_local, groups, scan_total):
    columns = scan_total // groups
    pack = max(1, LANES // columns)
    per_block = -(-(MAT + 1) // pack)
    return columns, pack, per_block


def block_rows(every, row_hot, count):
    high = every.astype(jnp.bfloat16).astype(jnp.float32)
    for part in (high, every - high):
        yield jnp.concatenate(
            [jnp.where(row_hot, part[q : q + 1], 0.0).astype(jnp.bfloat16) for q in range(count)], axis=0
        )


def held_kernel(devices, groups, scan_local, place_ref, flat_ref, *refs):
    out_refs, stage_ref = refs[:-1], refs[-1]
    slots = flat_ref.shape[1]
    cap = slots // devices
    scan_total = scan_local * (devices // groups)
    columns, pack, per_block = layout(scan_local, groups, scan_total)
    every = flat_ref[...]
    row = every[ROW_MATE : ROW_MATE + 1].astype(jnp.int32)
    other = div(div(iota((1, slots), 1), cap), groups) * scan_local + every[ROW_FLAG : ROW_FLAG + 1].astype(jnp.int32) - 1
    own = place_ref[0] * scan_local + row
    row_hot = iota((scan_local, slots), 0) == row
    column = iota((scan_total, slots), 0)
    mix = ((column == own).astype(jnp.float32) - (column == other).astype(jnp.float32)).astype(jnp.bfloat16)
    hess = sum(dot(rows, mix, BOTH_LANES) for rows in block_rows(every, row_hot, MAT))
    lane = iota((scan_local, LANES), 1)
    home = MAT // per_block
    grad = jnp.zeros((scan_local, LANES), jnp.float32)
    for q in range(FIELDS):
        value = jnp.sum(jnp.where(row_hot, every[HEAD + q : HEAD + q + 1], 0.0), axis=1, keepdims=True)
        grad = jnp.where(lane == home * columns + q, -value, grad)
    for c in range(groups):
        side, shift = divmod(c * columns, LANES)
        for r in range(per_block):
            tile = jnp.zeros((scan_local, LANES), jnp.float32)
            for k in range(pack):
                q = k * per_block + r
                if q < MAT:
                    value = hess[q * scan_local : (q + 1) * scan_local, side * LANES : (side + 1) * LANES]
                    value = turn(value, k * columns - shift)
                elif q == MAT:
                    value = grad
                else:
                    continue
                tile = jnp.where(div(lane, columns) == k, value, tile) if pack > 1 else value
            stage_ref[c, r * scan_local : (r + 1) * scan_local, :] = tile
    for k, out_ref in enumerate(out_refs):
        out_ref[...] = stage_ref[partner(place_ref[1], k, groups)]


def close_kernel(devices, groups, cap, place_ref, back_ref, *refs):
    part_refs, (hess_ref, grad_ref, every_ref, hold_ref) = refs[:groups], refs[groups:]
    scan_local, columns = hess_ref.shape[1:]
    per_block = part_refs[0].shape[0] // scan_local
    span, slot_rows, sum_rows = back_layout(scan_local, groups, cap)
    block = slot_rows + sum_rows
    senders = devices // groups
    first = place_ref[1] * (senders * block)
    lane_block = div(iota((slot_rows, LANES), 1), span)
    per_chunk = LANES // span
    for chunk in range(senders // per_chunk):
        found = [back_ref[pl.ds(first + (chunk * per_chunk + u) * block, slot_rows), :] for u in range(per_chunk)]
        for i in range(LANES // span):
            tile = None
            for u in range(per_chunk):
                piece = turn(found[u], (u - i) * span)
                tile = piece if u == 0 else jnp.where(lane_block == u, piece, tile)
            every_ref[i * slot_rows : (i + 1) * slot_rows, chunk * LANES : (chunk + 1) * LANES] = tile
    every = every_ref[...]
    total = every.shape[1]
    row = every[ROW_FLAG : ROW_FLAG + 1].astype(jnp.int32) - 1
    mate = every[ROW_MATE : ROW_MATE + 1].astype(jnp.int32)
    column = div(div(iota((1, total), 1), span), groups) * scan_local + mate
    row_hot = iota((scan_local, total), 0) == row
    mix = (iota((columns, total), 0) == column).astype(jnp.float32).astype(jnp.bfloat16)
    cross = sum(dot(rows, mix, BOTH_LANES) for rows in block_rows(every, row_hot, MAT))
    sums = back_ref[slot_rows:block, :]
    for d in range(1, devices):
        sums = sums + back_ref[d * block + slot_rows : (d + 1) * block, :]
    line = iota((scan_local, LANES), 0)
    lane = iota((scan_local, LANES), 1)

    def by_row(q):
        i, r = divmod(q, sum_rows)
        return jnp.sum(jnp.where(lane == line + i * scan_local, sums[r : r + 1], 0.0), axis=1, keepdims=True)

    whole = part_refs[0][...]
    for part_ref in part_refs[1:]:
        whole = whole + part_ref[...]
    offset = place_ref[0] * scan_local - place_ref[1] * columns
    diagonal = iota((scan_local, columns), 1) == iota((scan_local, columns), 0) + offset
    for q in range(MAT):
        k, r = divmod(q, per_block)
        tile = whole[r * scan_local : (r + 1) * scan_local, k * columns : (k + 1) * columns]
        tile = tile - cross[q * scan_local : (q + 1) * scan_local]
        tile = tile + jnp.where(diagonal, by_row(q), 0.0)
        i, j = PAIRS[q]
        hess_ref[i * FIELDS + j] = tile
        if i != j:
            hess_ref[j * FIELDS + i] = tile
    k, r = divmod(MAT, per_block)
    grad = turn(whole[r * scan_local : (r + 1) * scan_local], -k * columns)
    for q in range(FIELDS):
        grad = grad + jnp.where(lane == q, by_row(HEAD + q), 0.0)
    hold_ref[...] = grad
    part = scan_local // groups
    grad_ref[...] = hold_ref[pl.ds(place_ref[1] * part, part), 0:FIELDS]


def call(kernel, out_shape, smem, vmem, scratch=()):
    body = pl.pallas_call(
        kernel,
        out_shape=out_shape,
        in_specs=[pl.BlockSpec(memory_space=pltpu.SMEM)] * smem + [pl.BlockSpec(memory_space=pltpu.VMEM)] * vmem,
        scratch_shapes=list(scratch),
    )

    def run(*args):
        args = args[:smem] + tuple(pltpu.with_memory_space_constraint(x, pltpu.VMEM) for x in args[smem:])
        return body(*args)

    return run


def f32(*shape):
    return jax.ShapeDtypeStruct(shape, jnp.float32)


def near(*shape):
    return pltpu.VMEM(shape, jnp.float32)


def exchange(x, axes):
    count, width = x.shape
    moved = lax.all_to_all(x.reshape(count, 1, width), axes, split_axis=0, concat_axis=0, tiled=True)
    return moved.reshape(count, width)


def local(samples, point_count, corr_scan, corr_tile, corr_src):
    devices = lax.axis_size(AXES)
    groups = lax.axis_size("grp")
    samples = samples.transpose(0, 2, 1, 3)
    scan_local, tiles, per_scan, entries, cap, block = sizes(samples.shape, corr_scan.shape, devices)
    slots = devices * cap
    scan_total = scan_local * (devices // groups)
    columns, pack, per_block = layout(scan_local, groups, scan_total)
    group = lax.axis_index("grp").astype(jnp.int32)
    place = jnp.stack([lax.axis_index("scan").astype(jnp.int32), group])
    group = group.reshape(1)
    _, slot_rows, sum_rows = back_layout(scan_local, groups, cap)

    def bind(kernel, *args):
        return lambda *refs: kernel(*args, *refs)

    sent, samples = pl.pallas_call(
        bind(send_kernel, devices, groups),
        out_shape=(near(devices * block, LANES), near(*samples.shape)),
        in_specs=[pl.BlockSpec(memory_space=pltpu.SMEM)] * 2 + [pl.BlockSpec(memory_space=pl.ANY)] * 4,
        scratch_shapes=[
            pltpu.VMEM(corr_scan.shape, jnp.int32),
            pltpu.VMEM(corr_tile.shape, jnp.int32),
            pltpu.VMEM(corr_src.shape, jnp.int32),
            pltpu.VMEM((COORDS + 1, entries, LANES), jnp.float32),
            pltpu.SemaphoreType.DMA((4,)),
        ],
    )(group, point_count, samples, corr_scan, corr_tile, corr_src)
    received = exchange(sent, AXES)
    flat, back = call(
        bind(pair_kernel, devices, groups),
        (near(WIDTH, slots), near(devices * (slot_rows + sum_rows), LANES)),
        2,
        2,
        [
            pltpu.VMEM((COORDS + 1, LANES, slots), jnp.float32),
            pltpu.VMEM((FIELDS, LANES, slots), jnp.float32),
            pltpu.VMEM((devices, LANES), jnp.float32),
        ],
    )(group, point_count, samples, received)
    back = exchange(back, AXES)
    share = near(per_block * scan_local, LANES)
    shares = call(
        bind(held_kernel, devices, groups, scan_local),
        (share,) * groups,
        1,
        1,
        [pltpu.VMEM((groups,) + share.shape, jnp.float32)],
    )(place, flat)
    shares = [shares[0]] + [
        lax.ppermute(shares[k], "grp", [(g, partner(g, k, groups)) for g in range(groups)]) for k in range(1, groups)
    ]
    hess, grad = call(
        bind(close_kernel, devices, groups, cap),
        (f32(FIELDS * FIELDS, scan_local, columns), f32(scan_local // groups, FIELDS)),
        1,
        1 + groups,
        [
            pltpu.VMEM((HEAD, (devices // groups) * groups * cap), jnp.float32),
            pltpu.VMEM((scan_local, LANES), jnp.float32),
        ],
    )(place, back, *shares)
    return hess.reshape(FIELDS, FIELDS, scan_local, columns).transpose(2, 0, 1, 3), grad


def solution(mesh):
    placed = (
        P("scan", "grp", None, None),
        P("scan"),
        P("scan", "grp"),
        P("scan", "grp"),
        P("scan", "grp", None),
    )
    return jax.shard_map(
        local,
        mesh=mesh,
        in_specs=placed,
        out_specs=(P("scan", None, None, "grp"), P(AXES, None)),
        check_vma=False,
    )
```

```python
import jax
import jax.numpy as jnp
from jax import lax
from jax.experimental import pallas as pl
from jax.experimental.pallas import tpu as pltpu
from jax.sharding import PartitionSpec as P

LANES = 128
COORDS = 3
FIELDS = 6
PAIRS = [(i, j) for i in range(FIELDS) for j in range(i, FIELDS)]
MAT = len(PAIRS)
ROW_FLAG = MAT
ROW_MATE = MAT + 1
HEAD = MAT + 3
WIDTH = 32
FAR = 2.0**100
BOTH_LANES = (((1,), (1,)), ((), ()))
AXES = ("scan", "grp")


def div(x, n):
    if n & (n - 1) == 0:
        return lax.shift_right_logical(x, jnp.int32(n.bit_length() - 1))
    return x // n


def mod(x, n):
    if n & (n - 1) == 0:
        return x & (n - 1)
    return x % n


def iota(shape, dim):
    return lax.broadcasted_iota(jnp.int32, shape, dim)


def pieces(x, count):
    parts = []
    for _ in range(count - 1):
        part = x.astype(jnp.bfloat16)
        parts.append(part)
        x = x - part.astype(jnp.float32)
    parts.append(x.astype(jnp.bfloat16))
    return parts


def dot(a, b, dims=(((1,), (0,)), ((), ()))):
    return lax.dot_general(a, b, dims, preferred_element_type=jnp.float32)


def sizes(samples_shape, entries_shape, devices):
    scan_local, _, tiles, _ = samples_shape
    per_scan = entries_shape[1]
    entries = scan_local * per_scan
    cap = 2 * entries // devices
    return scan_local, tiles, per_scan, entries, cap, COORDS * cap + 1


def send_kernel(
    devices,
    groups,
    group_ref,
    count_ref,
    samples_hbm,
    scan_hbm,
    tile_hbm,
    src_hbm,
    out_ref,
    samples_ref,
    scan_ref,
    tile_ref,
    src_ref,
    data_ref,
    sems,
):
    scan_local, tiles, per_scan, entries, cap, block = sizes(samples_ref.shape, scan_ref.shape, devices)
    group_points = tiles * LANES
    pairs = ((scan_hbm, scan_ref), (tile_hbm, tile_ref), (src_hbm, src_ref), (samples_hbm, samples_ref))
    loads = [pltpu.make_async_copy(far, here, sems.at[k]) for k, (far, here) in enumerate(pairs)]
    for load in loads:
        load.start()
    for load in loads[:2]:
        load.wait()

    scans = scan_ref[...]
    tile_ids = tile_ref[...]
    device = div(scans, scan_local) * groups + div(tile_ids, tiles)
    stacked = jnp.concatenate(
        [device.astype(jnp.float32), mod(scans, scan_local).astype(jnp.float32), mod(tile_ids, tiles).astype(jnp.float32)],
        axis=0,
    ).astype(jnp.bfloat16)
    spread = (mod(iota((per_scan, entries), 1), per_scan) == iota((per_scan, entries), 0)).astype(jnp.float32)
    wide = dot(stacked, spread.astype(jnp.bfloat16))
    own = div(iota((scan_local, entries), 1), per_scan) == iota((scan_local, entries), 0)
    device_row, mate_row, tile_row = [
        jnp.sum(jnp.where(own, wide[f * scan_local : (f + 1) * scan_local], 0.0), axis=0, keepdims=True)
        for f in range(3)
    ]
    rank_parts = []
    columns = []
    for h in range(entries // LANES):
        across = device_row[:, h * LANES : (h + 1) * LANES]
        columns.append(jnp.broadcast_to(across, (LANES, LANES)).T)
        total = jnp.zeros((1, LANES), jnp.float32)
        for g in range(h + 1):
            same = columns[g] == across
            if g == h:
                same = same & (iota((LANES, LANES), 0) < iota((LANES, LANES), 1))
            total = total + jnp.sum(same.astype(jnp.float32), axis=0, keepdims=True)
        rank_parts.append(total)
    rank_row = jnp.concatenate(rank_parts, axis=1)
    slot_row = (device_row * cap + rank_row).astype(jnp.int32)
    place = (iota((devices * cap, entries), 0) == slot_row).astype(jnp.float32).astype(jnp.bfloat16)
    owner_row = (div(iota((1, entries), 1), per_scan) + 1).astype(jnp.float32)
    field = div(iota((LANES, entries), 0), cap)
    picked = jnp.where(field == 0, owner_row, jnp.where(field == 1, mate_row, tile_row))
    picked = jnp.where(
        (mod(iota((LANES, entries), 0), cap).astype(jnp.float32) == rank_row) & (field < 3), picked, 0.0
    ).astype(jnp.bfloat16)
    towards = (iota((devices, entries), 0).astype(jnp.float32) == device_row).astype(jnp.float32).astype(jnp.bfloat16)
    notes = dot(towards, picked, BOTH_LANES)
    for d in range(devices):
        out_ref[pl.ds(d * block + COORDS * cap, 1), :] = notes[d : d + 1]

    for load in loads[2:]:
        load.wait()

    def one_scan(s, carry):
        limit = count_ref[s] - group_ref[0] * group_points
        for h in range(per_scan // 8):
            ids = src_ref[s, pl.ds(h * 8, 8), :]
            lane = mod(ids, LANES)
            tile = div(ids, LANES)
            found = [jnp.zeros((8, LANES), jnp.float32) for _ in range(COORDS)]
            for t in range(tiles):
                here = tile == t
                for a in range(COORDS):
                    row = jnp.broadcast_to(samples_ref[s, a, t : t + 1, :], (8, LANES))
                    found[a] = jnp.where(here, jnp.take_along_axis(row, lane, axis=1), found[a])
            found[0] = jnp.where(ids < limit, found[0], FAR)
            at = pl.multiple_of(s * per_scan + h * 8, 8)
            for a in range(COORDS):
                data_ref[a, pl.ds(at, 8), :] = found[a]
        return carry

    lax.fori_loop(0, scan_local, one_scan, 0, unroll=4)

    for a in range(COORDS):
        parts = [dot(place, part) for part in pieces(data_ref[a], 3)]
        moved = (parts[0] + parts[1]) + parts[2]
        for d in range(devices):
            out_ref[pl.ds(d * block + a * cap, cap), :] = moved[d * cap : (d + 1) * cap]


def turn(x, amount):
    amount = amount % LANES
    return pltpu.roll(x, amount, 1) if amount else x


def back_layout(scan_local, groups, cap):
    span = groups * cap
    return span, HEAD * span // LANES, WIDTH * scan_local // LANES


def partner(index, k, groups):
    return index ^ k if groups & (groups - 1) == 0 else (index + k) % groups


def pair_kernel(devices, groups, group_ref, count_ref, samples_ref, recv_ref, flat_ref, back_ref, point_ref, mate_ref, note_ref):
    scan_local, _, tiles, _ = samples_ref.shape
    slots = flat_ref.shape[1]
    cap = slots // devices
    block = COORDS * cap + 1
    for d in range(devices):
        note_ref[pl.ds(d, 1), :] = recv_ref[pl.ds(d * block + COORDS * cap, 1), :]
    notes = note_ref[...].astype(jnp.bfloat16)
    mine = div(iota((devices, slots), 1), cap) == iota((devices, slots), 0)
    rows = []
    for f in range(3):
        spread = (iota((LANES, slots), 0) == mod(iota((LANES, slots), 1), cap) + f * cap).astype(jnp.float32)
        rows.append(
            jnp.sum(jnp.where(mine, dot(notes, spread.astype(jnp.bfloat16)), 0.0), axis=0, keepdims=True)
        )
    flag_row, mate_row, tile_row = rows
    code_row = (mate_row * tiles + tile_row).astype(jnp.int32)
    table = scan_local * tiles
    chosen = (iota((table, slots), 0) == code_row).astype(jnp.float32).astype(jnp.bfloat16)
    base = group_ref[0] * tiles
    point_ids = (base + iota((tiles, LANES), 0)) * LANES + iota((tiles, LANES), 1)
    for a in range(FIELDS):
        values = []
        for b in range(scan_local):
            value = samples_ref[b, a]
            if a >= COORDS:
                value = jnp.where(point_ids < count_ref[b], value, 0.0)
            values.append(value)
        values = jnp.concatenate(values, axis=0)
        turned = jnp.concatenate([values[h : h + LANES].T for h in range(0, table, LANES)], axis=1)
        parts = [dot(part, chosen) for part in pieces(turned, 3)]
        mate_ref[a] = (parts[0] + parts[1]) + parts[2]
    per_chunk = LANES // cap
    for c in range(slots // LANES):
        for a in range(COORDS):
            stack = [
                recv_ref[pl.ds(d * block + a * cap, cap), :] for d in range(c * per_chunk, (c + 1) * per_chunk)
            ]
            point_ref[a, :, c * LANES : (c + 1) * LANES] = jnp.concatenate(stack, axis=0).T
    for c in range(slots // LANES):
        lanes = slice(c * LANES, (c + 1) * LANES)

        def step(k, sums):
            at = pl.ds(pl.multiple_of(k * 8, 8), 8)
            px, py, pz = [point_ref[a, at, lanes] for a in range(COORDS)]
            present = px < FAR
            px = jnp.where(present, px, 0.0)
            qx, qy, qz, nx, ny, nz = [mate_ref[a, at, lanes] for a in range(FIELDS)]
            residual = nx * (px - qx) + ny * (py - qy) + nz * (pz - qz)
            weight = jnp.where(present, 1.0 / (1.0 + residual * residual), 0.0)
            jac = [py * nz - pz * ny, pz * nx - px * nz, px * ny - py * nx, nx, ny, nz]
            scaled = [weight * j for j in jac]
            terms = [scaled[i] * jac[j] for i, j in PAIRS] + [residual * s for s in scaled]
            return tuple(s + t for s, t in zip(sums, terms))

        zero = jnp.zeros((8, LANES), jnp.float32)
        sums = lax.fori_loop(0, LANES // 8, step, (zero,) * (MAT + FIELDS), unroll=4)
        filled = flag_row[:, lanes] > 0.0
        lines = [jnp.where(filled, jnp.sum(s, axis=0, keepdims=True), 0.0) for s in sums]
        blank = jnp.zeros((1, LANES), jnp.float32)
        lines[MAT:MAT] = [flag_row[:, lanes], mate_row[:, lanes], blank]
        lines += [blank] * (WIDTH - len(lines))
        flat_ref[:, lanes] = jnp.concatenate(lines, axis=0)
    scans = devices // groups
    span, slot_rows, sum_rows = back_layout(scan_local, groups, cap)
    source = div(div(iota((1, slots), 1), cap), groups) * scan_local + flag_row.astype(jnp.int32) - 1
    source = jnp.where(flag_row > 0.0, source, -1)
    source_hot = (iota((scans * scan_local, slots), 0) == source).astype(jnp.float32).astype(jnp.bfloat16)
    parts = [dot(part, source_hot, BOTH_LANES) for part in pieces(flat_ref[...], 3)]
    sums = (parts[0] + parts[1]) + parts[2]
    slot_lane = div(iota((slot_rows, LANES), 1), span)
    sum_lane = div(iota((sum_rows, LANES), 1), scan_local)
    for scan in range(scans):
        c, start = divmod(scan * span, LANES)
        body = None
        for i in range(LANES // span):
            piece = flat_ref[i * slot_rows : (i + 1) * slot_rows, c * LANES : (c + 1) * LANES]
            piece = turn(piece, i * span - start)
            body = piece if i == 0 else jnp.where(slot_lane == i, piece, body)
        c, start = divmod(scan * scan_local, LANES)
        tail = None
        for i in range(WIDTH // sum_rows):
            piece = turn(sums[i * sum_rows : (i + 1) * sum_rows, c * LANES : (c + 1) * LANES], i * scan_local - start)
            tail = piece if i == 0 else jnp.where(sum_lane == i, piece, tail)
        for c in range(groups):
            at = (scan * groups + c) * (slot_rows + sum_rows)
            back_ref[at : at + slot_rows, :] = body
            back_ref[at + slot_rows : at + slot_rows + sum_rows, :] = tail


def layout(scan_local, groups, scan_total):
    columns = scan_total // groups
    pack = max(1, LANES // columns)
    per_block = -(-(MAT + 1) // pack)
    return columns, pack, per_block


def block_rows(every, row_hot, count):
    high = every.astype(jnp.bfloat16).astype(jnp.float32)
    for part in (high, every - high):
        yield jnp.concatenate(
            [jnp.where(row_hot, part[q : q + 1], 0.0).astype(jnp.bfloat16) for q in range(count)], axis=0
        )


def held_kernel(devices, groups, scan_local, place_ref, flat_ref, *refs):
    out_refs, stage_ref = refs[:-1], refs[-1]
    slots = flat_ref.shape[1]
    cap = slots // devices
    scan_total = scan_local * (devices // groups)
    columns, pack, per_block = layout(scan_local, groups, scan_total)
    every = flat_ref[...]
    row = every[ROW_MATE : ROW_MATE + 1].astype(jnp.int32)
    other = div(div(iota((1, slots), 1), cap), groups) * scan_local + every[ROW_FLAG : ROW_FLAG + 1].astype(jnp.int32) - 1
    own = place_ref[0] * scan_local + row
    row_hot = iota((scan_local, slots), 0) == row
    column = iota((scan_total, slots), 0)
    mix = ((column == own).astype(jnp.float32) - (column == other).astype(jnp.float32)).astype(jnp.bfloat16)
    hess = sum(dot(rows, mix, BOTH_LANES) for rows in block_rows(every, row_hot, MAT))
    lane = iota((scan_local, LANES), 1)
    home = MAT // per_block
    grad = jnp.zeros((scan_local, LANES), jnp.float32)
    for q in range(FIELDS):
        value = jnp.sum(jnp.where(row_hot, every[HEAD + q : HEAD + q + 1], 0.0), axis=1, keepdims=True)
        grad = jnp.where(lane == home * columns + q, -value, grad)
    for c in range(groups):
        side, shift = divmod(c * columns, LANES)
        for r in range(per_block):
            tile = jnp.zeros((scan_local, LANES), jnp.float32)
            for k in range(pack):
                q = k * per_block + r
                if q < MAT:
                    value = hess[q * scan_local : (q + 1) * scan_local, side * LANES : (side + 1) * LANES]
                    value = turn(value, k * columns - shift)
                elif q == MAT:
                    value = grad
                else:
                    continue
                tile = jnp.where(div(lane, columns) == k, value, tile) if pack > 1 else value
            stage_ref[c, r * scan_local : (r + 1) * scan_local, :] = tile
    for k, out_ref in enumerate(out_refs):
        out_ref[...] = stage_ref[partner(place_ref[1], k, groups)]


def close_kernel(devices, groups, cap, place_ref, back_ref, *refs):
    part_refs, (hess_ref, grad_ref, every_ref, hold_ref) = refs[:groups], refs[groups:]
    scan_local, columns = hess_ref.shape[1:]
    per_block = part_refs[0].shape[0] // scan_local
    span, slot_rows, sum_rows = back_layout(scan_local, groups, cap)
    block = slot_rows + sum_rows
    senders = devices // groups
    first = place_ref[1] * (senders * block)
    lane_block = div(iota((slot_rows, LANES), 1), span)
    per_chunk = LANES // span
    for chunk in range(senders // per_chunk):
        found = [back_ref[pl.ds(first + (chunk * per_chunk + u) * block, slot_rows), :] for u in range(per_chunk)]
        for i in range(LANES // span):
            tile = None
            for u in range(per_chunk):
                piece = turn(found[u], (u - i) * span)
                tile = piece if u == 0 else jnp.where(lane_block == u, piece, tile)
            every_ref[i * slot_rows : (i + 1) * slot_rows, chunk * LANES : (chunk + 1) * LANES] = tile
    every = every_ref[...]
    total = every.shape[1]
    row = every[ROW_FLAG : ROW_FLAG + 1].astype(jnp.int32) - 1
    mate = every[ROW_MATE : ROW_MATE + 1].astype(jnp.int32)
    column = div(div(iota((1, total), 1), span), groups) * scan_local + mate
    row_hot = iota((scan_local, total), 0) == row
    mix = (iota((columns, total), 0) == column).astype(jnp.float32).astype(jnp.bfloat16)
    cross = sum(dot(rows, mix, BOTH_LANES) for rows in block_rows(every, row_hot, MAT))
    sums = back_ref[slot_rows:block, :]
    for d in range(1, devices):
        sums = sums + back_ref[d * block + slot_rows : (d + 1) * block, :]
    line = iota((scan_local, LANES), 0)
    lane = iota((scan_local, LANES), 1)

    def by_row(q):
        i, r = divmod(q, sum_rows)
        return jnp.sum(jnp.where(lane == line + i * scan_local, sums[r : r + 1], 0.0), axis=1, keepdims=True)

    whole = part_refs[0][...]
    for part_ref in part_refs[1:]:
        whole = whole + part_ref[...]
    offset = place_ref[0] * scan_local - place_ref[1] * columns
    diagonal = iota((scan_local, columns), 1) == iota((scan_local, columns), 0) + offset
    for q in range(MAT):
        k, r = divmod(q, per_block)
        tile = whole[r * scan_local : (r + 1) * scan_local, k * columns : (k + 1) * columns]
        tile = tile - cross[q * scan_local : (q + 1) * scan_local]
        tile = tile + jnp.where(diagonal, by_row(q), 0.0)
        i, j = PAIRS[q]
        hess_ref[i * FIELDS + j] = tile
        if i != j:
            hess_ref[j * FIELDS + i] = tile
    k, r = divmod(MAT, per_block)
    grad = turn(whole[r * scan_local : (r + 1) * scan_local], -k * columns)
    for q in range(FIELDS):
        grad = grad + jnp.where(lane == q, by_row(HEAD + q), 0.0)
    hold_ref[...] = grad
    part = scan_local // groups
    grad_ref[...] = hold_ref[pl.ds(place_ref[1] * part, part), 0:FIELDS]


def call(kernel, out_shape, smem, vmem, scratch=()):
    body = pl.pallas_call(
        kernel,
        out_shape=out_shape,
        in_specs=[pl.BlockSpec(memory_space=pltpu.SMEM)] * smem + [pl.BlockSpec(memory_space=pltpu.VMEM)] * vmem,
        scratch_shapes=list(scratch),
    )

    def run(*args):
        args = args[:smem] + tuple(pltpu.with_memory_space_constraint(x, pltpu.VMEM) for x in args[smem:])
        return body(*args)

    return run


def f32(*shape):
    return jax.ShapeDtypeStruct(shape, jnp.float32)


def near(*shape):
    return pltpu.VMEM(shape, jnp.float32)


def exchange(x, axes):
    count, width = x.shape
    moved = lax.all_to_all(x.reshape(count, 1, width), axes, split_axis=0, concat_axis=0, tiled=True)
    return moved.reshape(count, width)


def local(samples, point_count, corr_scan, corr_tile, corr_src):
    devices = lax.axis_size(AXES)
    groups = lax.axis_size("grp")
    samples = samples.transpose(0, 2, 1, 3)
    scan_local, tiles, per_scan, entries, cap, block = sizes(samples.shape, corr_scan.shape, devices)
    slots = devices * cap
    scan_total = scan_local * (devices // groups)
    columns, pack, per_block = layout(scan_local, groups, scan_total)
    group = lax.axis_index("grp").astype(jnp.int32)
    place = jnp.stack([lax.axis_index("scan").astype(jnp.int32), group])
    group = group.reshape(1)
    _, slot_rows, sum_rows = back_layout(scan_local, groups, cap)

    def bind(kernel, *args):
        return lambda *refs: kernel(*args, *refs)

    sent, samples = pl.pallas_call(
        bind(send_kernel, devices, groups),
        out_shape=(near(devices * block, LANES), near(*samples.shape)),
        in_specs=[pl.BlockSpec(memory_space=pltpu.SMEM)] * 2 + [pl.BlockSpec(memory_space=pl.ANY)] * 4,
        scratch_shapes=[
            pltpu.VMEM(corr_scan.shape, jnp.int32),
            pltpu.VMEM(corr_tile.shape, jnp.int32),
            pltpu.VMEM(corr_src.shape, jnp.int32),
            pltpu.VMEM((COORDS, entries, LANES), jnp.float32),
            pltpu.SemaphoreType.DMA((4,)),
        ],
    )(group, point_count, samples, corr_scan, corr_tile, corr_src)
    received = exchange(sent, AXES)
    flat, back = call(
        bind(pair_kernel, devices, groups),
        (near(WIDTH, slots), near(devices * (slot_rows + sum_rows), LANES)),
        2,
        2,
        [
            pltpu.VMEM((COORDS, LANES, slots), jnp.float32),
            pltpu.VMEM((FIELDS, LANES, slots), jnp.float32),
            pltpu.VMEM((devices, LANES), jnp.float32),
        ],
    )(group, point_count, samples, received)
    back = exchange(back, AXES)
    share = near(per_block * scan_local, LANES)
    shares = call(
        bind(held_kernel, devices, groups, scan_local),
        (share,) * groups,
        1,
        1,
        [pltpu.VMEM((groups,) + share.shape, jnp.float32)],
    )(place, flat)
    shares = [shares[0]] + [
        lax.ppermute(shares[k], "grp", [(g, partner(g, k, groups)) for g in range(groups)]) for k in range(1, groups)
    ]
    hess, grad = call(
        bind(close_kernel, devices, groups, cap),
        (f32(FIELDS * FIELDS, scan_local, columns), f32(scan_local // groups, FIELDS)),
        1,
        1 + groups,
        [
            pltpu.VMEM((HEAD, (devices // groups) * groups * cap), jnp.float32),
            pltpu.VMEM((scan_local, LANES), jnp.float32),
        ],
    )(place, back, *shares)
    return hess.reshape(FIELDS, FIELDS, scan_local, columns).transpose(2, 0, 1, 3), grad


def solution(mesh):
    placed = (
        P("scan", "grp", None, None),
        P("scan"),
        P("scan", "grp"),
        P("scan", "grp"),
        P("scan", "grp", None),
    )
    return jax.shard_map(
        local,
        mesh=mesh,
        in_specs=placed,
        out_specs=(P("scan", None, None, "grp"), P(AXES, None)),
        check_vma=False,
    )
```

```python
import jax
import jax.numpy as jnp
from jax import lax
from jax.experimental import pallas as pl
from jax.experimental.pallas import tpu as pltpu
from jax.sharding import PartitionSpec as P

LANES = 128
COORDS = 3
FIELDS = 6
PAIRS = [(i, j) for i in range(FIELDS) for j in range(i, FIELDS)]
MAT = len(PAIRS)
ROW_FLAG = MAT
ROW_MATE = MAT + 1
HEAD = MAT + 3
WIDTH = 32
FAR = 2.0**100
BOTH_LANES = (((1,), (1,)), ((), ()))
AXES = ("scan", "grp")


def div(x, n):
    if n & (n - 1) == 0:
        return lax.shift_right_logical(x, jnp.int32(n.bit_length() - 1))
    return x // n


def mod(x, n):
    if n & (n - 1) == 0:
        return x & (n - 1)
    return x % n


def iota(shape, dim):
    return lax.broadcasted_iota(jnp.int32, shape, dim)


def pieces(x, count):
    parts = []
    for _ in range(count - 1):
        part = x.astype(jnp.bfloat16)
        parts.append(part)
        x = x - part.astype(jnp.float32)
    parts.append(x.astype(jnp.bfloat16))
    return parts


def dot(a, b, dims=(((1,), (0,)), ((), ()))):
    return lax.dot_general(a, b, dims, preferred_element_type=jnp.float32)


def sizes(samples_shape, entries_shape, devices):
    scan_local, _, tiles, _ = samples_shape
    per_scan = entries_shape[1]
    entries = scan_local * per_scan
    cap = 2 * entries // devices
    return scan_local, tiles, per_scan, entries, cap, COORDS * cap + 1


def send_kernel(
    devices,
    groups,
    group_ref,
    count_hbm,
    samples_hbm,
    scan_hbm,
    tile_hbm,
    src_hbm,
    out_ref,
    samples_ref,
    count_ref,
    scan_ref,
    tile_ref,
    src_ref,
    data_ref,
    sems,
):
    scan_local, tiles, per_scan, entries, cap, block = sizes(samples_ref.shape, scan_ref.shape, devices)
    group_points = tiles * LANES
    pairs = (
        (scan_hbm, scan_ref),
        (tile_hbm, tile_ref),
        (count_hbm, count_ref),
        (src_hbm, src_ref),
        (samples_hbm, samples_ref),
    )
    loads = [pltpu.make_async_copy(far, here, sems.at[k]) for k, (far, here) in enumerate(pairs)]
    for load in loads:
        load.start()
    for load in loads[:2]:
        load.wait()

    scans = scan_ref[...]
    tile_ids = tile_ref[...]
    device = div(scans, scan_local) * groups + div(tile_ids, tiles)
    stacked = jnp.concatenate(
        [device.astype(jnp.float32), mod(scans, scan_local).astype(jnp.float32), mod(tile_ids, tiles).astype(jnp.float32)],
        axis=0,
    ).astype(jnp.bfloat16)
    spread = (mod(iota((per_scan, entries), 1), per_scan) == iota((per_scan, entries), 0)).astype(jnp.float32)
    wide = dot(stacked, spread.astype(jnp.bfloat16))
    own = div(iota((scan_local, entries), 1), per_scan) == iota((scan_local, entries), 0)
    device_row, mate_row, tile_row = [
        jnp.sum(jnp.where(own, wide[f * scan_local : (f + 1) * scan_local], 0.0), axis=0, keepdims=True)
        for f in range(3)
    ]
    rank_parts = []
    columns = []
    for h in range(entries // LANES):
        across = device_row[:, h * LANES : (h + 1) * LANES]
        columns.append(jnp.broadcast_to(across, (LANES, LANES)).T)
        total = jnp.zeros((1, LANES), jnp.float32)
        for g in range(h + 1):
            same = columns[g] == across
            if g == h:
                same = same & (iota((LANES, LANES), 0) < iota((LANES, LANES), 1))
            total = total + jnp.sum(same.astype(jnp.float32), axis=0, keepdims=True)
        rank_parts.append(total)
    rank_row = jnp.concatenate(rank_parts, axis=1)
    slot_row = (device_row * cap + rank_row).astype(jnp.int32)
    place = (iota((devices * cap, entries), 0) == slot_row).astype(jnp.float32).astype(jnp.bfloat16)
    owner_row = (div(iota((1, entries), 1), per_scan) + 1).astype(jnp.float32)
    field = div(iota((LANES, entries), 0), cap)
    picked = jnp.where(field == 0, owner_row, jnp.where(field == 1, mate_row, tile_row))
    picked = jnp.where(
        (mod(iota((LANES, entries), 0), cap).astype(jnp.float32) == rank_row) & (field < 3), picked, 0.0
    ).astype(jnp.bfloat16)
    towards = (iota((devices, entries), 0).astype(jnp.float32) == device_row).astype(jnp.float32).astype(jnp.bfloat16)
    notes = dot(towards, picked, BOTH_LANES)
    for d in range(devices):
        out_ref[pl.ds(d * block + COORDS * cap, 1), :] = notes[d : d + 1]

    for load in loads[2:]:
        load.wait()

    def one_scan(s, carry):
        limit = count_ref[s] - group_ref[0] * group_points
        for h in range(per_scan // 8):
            ids = src_ref[s, pl.ds(h * 8, 8), :]
            lane = mod(ids, LANES)
            tile = div(ids, LANES)
            found = [jnp.zeros((8, LANES), jnp.float32) for _ in range(COORDS)]
            for t in range(tiles):
                here = tile == t
                for a in range(COORDS):
                    row = jnp.broadcast_to(samples_ref[s, a, t : t + 1, :], (8, LANES))
                    found[a] = jnp.where(here, jnp.take_along_axis(row, lane, axis=1), found[a])
            found[0] = jnp.where(ids < limit, found[0], FAR)
            at = pl.multiple_of(s * per_scan + h * 8, 8)
            for a in range(COORDS):
                data_ref[a, pl.ds(at, 8), :] = found[a]
        present = iota((tiles, LANES), 0) * LANES + iota((tiles, LANES), 1) < limit
        for a in range(COORDS, FIELDS):
            samples_ref[s, a] = jnp.where(present, samples_ref[s, a], 0.0)
        return carry

    lax.fori_loop(0, scan_local, one_scan, 0, unroll=4)

    for a in range(COORDS):
        parts = [dot(place, part) for part in pieces(data_ref[a], 3)]
        moved = (parts[0] + parts[1]) + parts[2]
        for d in range(devices):
            out_ref[pl.ds(d * block + a * cap, cap), :] = moved[d * cap : (d + 1) * cap]


def turn(x, amount):
    amount = amount % LANES
    return pltpu.roll(x, amount, 1) if amount else x


def back_layout(scan_local, groups, cap):
    span = groups * cap
    return span, HEAD * span // LANES, WIDTH * scan_local // LANES


def partner(index, k, groups):
    return index ^ k if groups & (groups - 1) == 0 else (index + k) % groups


def pair_kernel(devices, groups, samples_ref, recv_ref, flat_ref, back_ref, point_ref, mate_ref, note_ref):
    scan_local, _, tiles, _ = samples_ref.shape
    slots = flat_ref.shape[1]
    cap = slots // devices
    block = COORDS * cap + 1
    for d in range(devices):
        note_ref[pl.ds(d, 1), :] = recv_ref[pl.ds(d * block + COORDS * cap, 1), :]
    notes = note_ref[...].astype(jnp.bfloat16)
    mine = div(iota((devices, slots), 1), cap) == iota((devices, slots), 0)
    rows = []
    for f in range(3):
        spread = (iota((LANES, slots), 0) == mod(iota((LANES, slots), 1), cap) + f * cap).astype(jnp.float32)
        rows.append(
            jnp.sum(jnp.where(mine, dot(notes, spread.astype(jnp.bfloat16)), 0.0), axis=0, keepdims=True)
        )
    flag_row, mate_row, tile_row = rows
    code_row = (mate_row * tiles + tile_row).astype(jnp.int32)
    table = scan_local * tiles
    chosen = (iota((table, slots), 0) == code_row).astype(jnp.float32).astype(jnp.bfloat16)
    for a in range(FIELDS):
        values = jnp.concatenate([samples_ref[b, a] for b in range(scan_local)], axis=0)
        turned = jnp.concatenate([values[h : h + LANES].T for h in range(0, table, LANES)], axis=1)
        parts = [dot(part, chosen) for part in pieces(turned, 3)]
        mate_ref[a] = (parts[0] + parts[1]) + parts[2]
    per_chunk = LANES // cap
    for c in range(slots // LANES):
        for a in range(COORDS):
            stack = [
                recv_ref[pl.ds(d * block + a * cap, cap), :] for d in range(c * per_chunk, (c + 1) * per_chunk)
            ]
            point_ref[a, :, c * LANES : (c + 1) * LANES] = jnp.concatenate(stack, axis=0).T
    for c in range(slots // LANES):
        lanes = slice(c * LANES, (c + 1) * LANES)

        def step(k, sums):
            at = pl.ds(pl.multiple_of(k * 8, 8), 8)
            px, py, pz = [point_ref[a, at, lanes] for a in range(COORDS)]
            present = px < FAR
            px = jnp.where(present, px, 0.0)
            qx, qy, qz, nx, ny, nz = [mate_ref[a, at, lanes] for a in range(FIELDS)]
            residual = nx * (px - qx) + ny * (py - qy) + nz * (pz - qz)
            weight = jnp.where(present, 1.0 / (1.0 + residual * residual), 0.0)
            jac = [py * nz - pz * ny, pz * nx - px * nz, px * ny - py * nx, nx, ny, nz]
            scaled = [weight * j for j in jac]
            terms = [scaled[i] * jac[j] for i, j in PAIRS] + [residual * s for s in scaled]
            return tuple(s + t for s, t in zip(sums, terms))

        zero = jnp.zeros((8, LANES), jnp.float32)
        sums = lax.fori_loop(0, LANES // 8, step, (zero,) * (MAT + FIELDS), unroll=4)
        filled = flag_row[:, lanes] > 0.0
        lines = [jnp.where(filled, jnp.sum(s, axis=0, keepdims=True), 0.0) for s in sums]
        blank = jnp.zeros((1, LANES), jnp.float32)
        lines[MAT:MAT] = [flag_row[:, lanes], mate_row[:, lanes], blank]
        lines += [blank] * (WIDTH - len(lines))
        flat_ref[:, lanes] = jnp.concatenate(lines, axis=0)
    scans = devices // groups
    span, slot_rows, sum_rows = back_layout(scan_local, groups, cap)
    source = div(div(iota((1, slots), 1), cap), groups) * scan_local + flag_row.astype(jnp.int32) - 1
    source = jnp.where(flag_row > 0.0, source, -1)
    source_hot = (iota((scans * scan_local, slots), 0) == source).astype(jnp.float32).astype(jnp.bfloat16)
    parts = [dot(part, source_hot, BOTH_LANES) for part in pieces(flat_ref[...], 3)]
    sums = (parts[0] + parts[1]) + parts[2]
    slot_lane = div(iota((slot_rows, LANES), 1), span)
    sum_lane = div(iota((sum_rows, LANES), 1), scan_local)
    for scan in range(scans):
        c, start = divmod(scan * span, LANES)
        body = None
        for i in range(LANES // span):
            piece = flat_ref[i * slot_rows : (i + 1) * slot_rows, c * LANES : (c + 1) * LANES]
            piece = turn(piece, i * span - start)
            body = piece if i == 0 else jnp.where(slot_lane == i, piece, body)
        c, start = divmod(scan * scan_local, LANES)
        tail = None
        for i in range(WIDTH // sum_rows):
            piece = turn(sums[i * sum_rows : (i + 1) * sum_rows, c * LANES : (c + 1) * LANES], i * scan_local - start)
            tail = piece if i == 0 else jnp.where(sum_lane == i, piece, tail)
        for c in range(groups):
            at = (scan * groups + c) * (slot_rows + sum_rows)
            back_ref[at : at + slot_rows, :] = body
            back_ref[at + slot_rows : at + slot_rows + sum_rows, :] = tail


def layout(scan_local, groups, scan_total):
    columns = scan_total // groups
    pack = max(1, LANES // columns)
    per_block = -(-(MAT + 1) // pack)
    return columns, pack, per_block


def block_rows(every, row_hot, count):
    high = every.astype(jnp.bfloat16).astype(jnp.float32)
    for part in (high, every - high):
        yield jnp.concatenate(
            [jnp.where(row_hot, part[q : q + 1], 0.0).astype(jnp.bfloat16) for q in range(count)], axis=0
        )


def held_kernel(devices, groups, scan_local, scan_ref, group_ref, flat_ref, *refs):
    out_refs, stage_ref = refs[:-1], refs[-1]
    slots = flat_ref.shape[1]
    cap = slots // devices
    scan_total = scan_local * (devices // groups)
    columns, pack, per_block = layout(scan_local, groups, scan_total)
    every = flat_ref[...]
    row = every[ROW_MATE : ROW_MATE + 1].astype(jnp.int32)
    other = div(div(iota((1, slots), 1), cap), groups) * scan_local + every[ROW_FLAG : ROW_FLAG + 1].astype(jnp.int32) - 1
    own = scan_ref[0] * scan_local + row
    row_hot = iota((scan_local, slots), 0) == row
    column = iota((scan_total, slots), 0)
    mix = ((column == own).astype(jnp.float32) - (column == other).astype(jnp.float32)).astype(jnp.bfloat16)
    hess = sum(dot(rows, mix, BOTH_LANES) for rows in block_rows(every, row_hot, MAT))
    lane = iota((scan_local, LANES), 1)
    home = MAT // per_block
    grad = jnp.zeros((scan_local, LANES), jnp.float32)
    for q in range(FIELDS):
        value = jnp.sum(jnp.where(row_hot, every[HEAD + q : HEAD + q + 1], 0.0), axis=1, keepdims=True)
        grad = jnp.where(lane == home * columns + q, -value, grad)
    for c in range(groups):
        side, shift = divmod(c * columns, LANES)
        for r in range(per_block):
            tile = jnp.zeros((scan_local, LANES), jnp.float32)
            for k in range(pack):
                q = k * per_block + r
                if q < MAT:
                    value = hess[q * scan_local : (q + 1) * scan_local, side * LANES : (side + 1) * LANES]
                    value = turn(value, k * columns - shift)
                elif q == MAT:
                    value = grad
                else:
                    continue
                tile = jnp.where(div(lane, columns) == k, value, tile) if pack > 1 else value
            stage_ref[c, r * scan_local : (r + 1) * scan_local, :] = tile
    for k, out_ref in enumerate(out_refs):
        out_ref[...] = stage_ref[partner(group_ref[0], k, groups)]


def close_kernel(devices, groups, cap, scan_ref, group_ref, back_ref, *refs):
    part_refs, (hess_ref, grad_ref, every_ref, hold_ref) = refs[:groups], refs[groups:]
    scan_local, columns = hess_ref.shape[1:]
    per_block = part_refs[0].shape[0] // scan_local
    span, slot_rows, sum_rows = back_layout(scan_local, groups, cap)
    block = slot_rows + sum_rows
    senders = devices // groups
    first = group_ref[0] * (senders * block)
    lane_block = div(iota((slot_rows, LANES), 1), span)
    per_chunk = LANES // span
    for chunk in range(senders // per_chunk):
        found = [back_ref[pl.ds(first + (chunk * per_chunk + u) * block, slot_rows), :] for u in range(per_chunk)]
        for i in range(LANES // span):
            tile = None
            for u in range(per_chunk):
                piece = turn(found[u], (u - i) * span)
                tile = piece if u == 0 else jnp.where(lane_block == u, piece, tile)
            every_ref[i * slot_rows : (i + 1) * slot_rows, chunk * LANES : (chunk + 1) * LANES] = tile
    every = every_ref[...]
    total = every.shape[1]
    row = every[ROW_FLAG : ROW_FLAG + 1].astype(jnp.int32) - 1
    mate = every[ROW_MATE : ROW_MATE + 1].astype(jnp.int32)
    column = div(div(iota((1, total), 1), span), groups) * scan_local + mate
    row_hot = iota((scan_local, total), 0) == row
    mix = (iota((columns, total), 0) == column).astype(jnp.float32).astype(jnp.bfloat16)
    cross = sum(dot(rows, mix, BOTH_LANES) for rows in block_rows(every, row_hot, MAT))
    sums = back_ref[slot_rows:block, :]
    for d in range(1, devices):
        sums = sums + back_ref[d * block + slot_rows : (d + 1) * block, :]
    line = iota((scan_local, LANES), 0)
    lane = iota((scan_local, LANES), 1)

    def by_row(q):
        i, r = divmod(q, sum_rows)
        return jnp.sum(jnp.where(lane == line + i * scan_local, sums[r : r + 1], 0.0), axis=1, keepdims=True)

    whole = part_refs[0][...]
    for part_ref in part_refs[1:]:
        whole = whole + part_ref[...]
    offset = scan_ref[0] * scan_local - group_ref[0] * columns
    diagonal = iota((scan_local, columns), 1) == iota((scan_local, columns), 0) + offset
    for q in range(MAT):
        k, r = divmod(q, per_block)
        tile = whole[r * scan_local : (r + 1) * scan_local, k * columns : (k + 1) * columns]
        tile = tile - cross[q * scan_local : (q + 1) * scan_local]
        tile = tile + jnp.where(diagonal, by_row(q), 0.0)
        i, j = PAIRS[q]
        hess_ref[i * FIELDS + j] = tile
        if i != j:
            hess_ref[j * FIELDS + i] = tile
    k, r = divmod(MAT, per_block)
    grad = turn(whole[r * scan_local : (r + 1) * scan_local], -k * columns)
    for q in range(FIELDS):
        grad = grad + jnp.where(lane == q, by_row(HEAD + q), 0.0)
    hold_ref[...] = grad
    part = scan_local // groups
    grad_ref[...] = hold_ref[pl.ds(group_ref[0] * part, part), 0:FIELDS]


def call(kernel, out_shape, smem, vmem, scratch=()):
    body = pl.pallas_call(
        kernel,
        out_shape=out_shape,
        in_specs=[pl.BlockSpec(memory_space=pltpu.SMEM)] * smem + [pl.BlockSpec(memory_space=pltpu.VMEM)] * vmem,
        scratch_shapes=list(scratch),
    )

    def run(*args):
        args = args[:smem] + tuple(pltpu.with_memory_space_constraint(x, pltpu.VMEM) for x in args[smem:])
        return body(*args)

    return run


def f32(*shape):
    return jax.ShapeDtypeStruct(shape, jnp.float32)


def near(*shape):
    return pltpu.VMEM(shape, jnp.float32)


def exchange(x, axes):
    count, width = x.shape
    moved = lax.all_to_all(x.reshape(count, 1, width), axes, split_axis=0, concat_axis=0, tiled=True)
    return moved.reshape(count, width)


def local(samples, point_count, corr_scan, corr_tile, corr_src):
    devices = lax.axis_size(AXES)
    groups = lax.axis_size("grp")
    samples = samples.transpose(0, 2, 1, 3)
    scan_local, tiles, per_scan, entries, cap, block = sizes(samples.shape, corr_scan.shape, devices)
    slots = devices * cap
    scan_total = scan_local * (devices // groups)
    columns, pack, per_block = layout(scan_local, groups, scan_total)
    group = lax.axis_index("grp").astype(jnp.int32).reshape(1)
    scan = lax.axis_index("scan").astype(jnp.int32).reshape(1)
    _, slot_rows, sum_rows = back_layout(scan_local, groups, cap)

    def bind(kernel, *args):
        return lambda *refs: kernel(*args, *refs)

    sent, samples = pl.pallas_call(
        bind(send_kernel, devices, groups),
        out_shape=(near(devices * block, LANES), near(*samples.shape)),
        in_specs=[pl.BlockSpec(memory_space=pltpu.SMEM)] + [pl.BlockSpec(memory_space=pl.ANY)] * 5,
        scratch_shapes=[
            pltpu.SMEM(point_count.shape, jnp.int32),
            pltpu.VMEM(corr_scan.shape, jnp.int32),
            pltpu.VMEM(corr_tile.shape, jnp.int32),
            pltpu.VMEM(corr_src.shape, jnp.int32),
            pltpu.VMEM((COORDS, entries, LANES), jnp.float32),
            pltpu.SemaphoreType.DMA((5,)),
        ],
    )(group, point_count, samples, corr_scan, corr_tile, corr_src)
    received = exchange(sent, AXES)
    flat, back = call(
        bind(pair_kernel, devices, groups),
        (near(WIDTH, slots), near(devices * (slot_rows + sum_rows), LANES)),
        0,
        2,
        [
            pltpu.VMEM((COORDS, LANES, slots), jnp.float32),
            pltpu.VMEM((FIELDS, LANES, slots), jnp.float32),
            pltpu.VMEM((devices, LANES), jnp.float32),
        ],
    )(samples, received)
    back = exchange(back, AXES)
    share = near(per_block * scan_local, LANES)
    shares = call(
        bind(held_kernel, devices, groups, scan_local),
        (share,) * groups,
        2,
        1,
        [pltpu.VMEM((groups,) + share.shape, jnp.float32)],
    )(scan, group, flat)
    shares = [shares[0]] + [
        lax.ppermute(shares[k], "grp", [(g, partner(g, k, groups)) for g in range(groups)]) for k in range(1, groups)
    ]
    hess, grad = call(
        bind(close_kernel, devices, groups, cap),
        (f32(FIELDS * FIELDS, scan_local, columns), f32(scan_local // groups, FIELDS)),
        2,
        1 + groups,
        [
            pltpu.VMEM((HEAD, (devices // groups) * groups * cap), jnp.float32),
            pltpu.VMEM((scan_local, LANES), jnp.float32),
        ],
    )(scan, group, back, *shares)
    return hess.reshape(FIELDS, FIELDS, scan_local, columns).transpose(2, 0, 1, 3), grad


def solution(mesh):
    placed = (
        P("scan", "grp", None, None),
        P("scan"),
        P("scan", "grp"),
        P("scan", "grp"),
        P("scan", "grp", None),
    )
    return jax.shard_map(
        local,
        mesh=mesh,
        in_specs=placed,
        out_specs=(P("scan", None, None, "grp"), P(AXES, None)),
        check_vma=False,
    )
```

```python
import jax
import jax.numpy as jnp
from jax import lax
from jax.experimental import pallas as pl
from jax.experimental.pallas import tpu as pltpu
from jax.sharding import PartitionSpec as P

LANES = 128
COORDS = 3
FIELDS = 6
PAIRS = [(i, j) for i in range(FIELDS) for j in range(i, FIELDS)]
MAT = len(PAIRS)
ROW_FLAG = MAT
ROW_MATE = MAT + 1
HEAD = MAT + 3
WIDTH = 32
FAR = 2.0**100
BOTH_LANES = (((1,), (1,)), ((), ()))
AXES = ("scan", "grp")


def div(x, n):
    if n & (n - 1) == 0:
        return lax.shift_right_logical(x, jnp.int32(n.bit_length() - 1))
    return x // n


def mod(x, n):
    if n & (n - 1) == 0:
        return x & (n - 1)
    return x % n


def iota(shape, dim):
    return lax.broadcasted_iota(jnp.int32, shape, dim)


def pieces(x, count):
    parts = []
    for _ in range(count - 1):
        part = x.astype(jnp.bfloat16)
        parts.append(part)
        x = x - part.astype(jnp.float32)
    parts.append(x.astype(jnp.bfloat16))
    return parts


def dot(a, b, dims=(((1,), (0,)), ((), ()))):
    return lax.dot_general(a, b, dims, preferred_element_type=jnp.float32)


def sizes(samples_shape, entries_shape, devices):
    scan_local, _, tiles, _ = samples_shape
    per_scan = entries_shape[1]
    entries = scan_local * per_scan
    cap = 2 * entries // devices
    return scan_local, tiles, per_scan, entries, cap, COORDS * cap + 1


def send_kernel(
    devices,
    groups,
    place_ref,
    group_ref,
    count_hbm,
    samples_hbm,
    scan_hbm,
    tile_hbm,
    src_hbm,
    out_ref,
    samples_ref,
    count_ref,
    scan_ref,
    tile_ref,
    src_ref,
    data_ref,
    sems,
):
    scan_local, tiles, per_scan, entries, cap, block = sizes(samples_ref.shape, scan_ref.shape, devices)
    group_points = tiles * LANES
    pairs = (
        (scan_hbm, scan_ref),
        (tile_hbm, tile_ref),
        (count_hbm, count_ref),
        (src_hbm, src_ref),
        (samples_hbm, samples_ref),
    )
    loads = [pltpu.make_async_copy(far, here, sems.at[k]) for k, (far, here) in enumerate(pairs)]
    for load in loads:
        load.start()
    for load in loads[:2]:
        load.wait()

    scans = scan_ref[...]
    tile_ids = tile_ref[...]
    device = div(scans, scan_local) * groups + div(tile_ids, tiles)
    stacked = jnp.concatenate(
        [device.astype(jnp.float32), mod(scans, scan_local).astype(jnp.float32), mod(tile_ids, tiles).astype(jnp.float32)],
        axis=0,
    ).astype(jnp.bfloat16)
    spread = (mod(iota((per_scan, entries), 1), per_scan) == iota((per_scan, entries), 0)).astype(jnp.float32)
    wide = dot(stacked, spread.astype(jnp.bfloat16))
    own = div(iota((scan_local, entries), 1), per_scan) == iota((scan_local, entries), 0)
    device_row, mate_row, tile_row = [
        jnp.sum(jnp.where(own, wide[f * scan_local : (f + 1) * scan_local], 0.0), axis=0, keepdims=True)
        for f in range(3)
    ]
    rank_parts = []
    columns = []
    for h in range(entries // LANES):
        across = device_row[:, h * LANES : (h + 1) * LANES]
        columns.append(jnp.broadcast_to(across, (LANES, LANES)).T)
        total = jnp.zeros((1, LANES), jnp.float32)
        for g in range(h + 1):
            same = columns[g] == across
            if g == h:
                same = same & (iota((LANES, LANES), 0) < iota((LANES, LANES), 1))
            total = total + jnp.sum(same.astype(jnp.float32), axis=0, keepdims=True)
        rank_parts.append(total)
    rank_row = jnp.concatenate(rank_parts, axis=1)
    slot_row = (device_row * cap + rank_row).astype(jnp.int32)
    place = (iota((devices * cap, entries), 0) == slot_row).astype(jnp.float32).astype(jnp.bfloat16)
    owner_row = (div(iota((1, entries), 1), per_scan) + 1).astype(jnp.float32)
    field = div(iota((LANES, entries), 0), cap)
    picked = jnp.where(field == 0, owner_row, jnp.where(field == 1, mate_row, tile_row))
    picked = jnp.where(
        (mod(iota((LANES, entries), 0), cap).astype(jnp.float32) == rank_row) & (field < 3), picked, 0.0
    ).astype(jnp.bfloat16)
    towards = (iota((devices, entries), 0).astype(jnp.float32) == device_row).astype(jnp.float32).astype(jnp.bfloat16)
    notes = dot(towards, picked, BOTH_LANES)
    for d in range(devices):
        out_ref[pl.ds(d * block + COORDS * cap, 1), :] = notes[d : d + 1]

    for load in loads[2:]:
        load.wait()

    def one_scan(s, carry):
        limit = count_ref[s] - group_ref[0] * group_points
        for h in range(per_scan // 8):
            ids = src_ref[s, pl.ds(h * 8, 8), :]
            lane = mod(ids, LANES)
            tile = div(ids, LANES)
            found = [jnp.zeros((8, LANES), jnp.float32) for _ in range(COORDS)]
            for t in range(tiles):
                here = tile == t
                for a in range(COORDS):
                    row = jnp.broadcast_to(samples_ref[s, a, t : t + 1, :], (8, LANES))
                    found[a] = jnp.where(here, jnp.take_along_axis(row, lane, axis=1), found[a])
            found[0] = jnp.where(ids < limit, found[0], FAR)
            at = pl.multiple_of(s * per_scan + h * 8, 8)
            for a in range(COORDS):
                data_ref[a, pl.ds(at, 8), :] = found[a]
        present = iota((tiles, LANES), 0) * LANES + iota((tiles, LANES), 1) < limit
        for a in range(COORDS, FIELDS):
            samples_ref[s, a] = jnp.where(present, samples_ref[s, a], 0.0)
        return carry

    lax.fori_loop(0, scan_local, one_scan, 0, unroll=8)

    for a in range(COORDS):
        parts = [dot(place, part) for part in pieces(data_ref[a], 3)]
        moved = (parts[0] + parts[1]) + parts[2]
        for d in range(devices):
            out_ref[pl.ds(d * block + a * cap, cap), :] = moved[d * cap : (d + 1) * cap]


def turn(x, amount):
    amount = amount % LANES
    return pltpu.roll(x, amount, 1) if amount else x


def back_layout(scan_local, groups, cap):
    span = groups * cap
    slot_rows = HEAD * span // LANES
    sum_rows = WIDTH * scan_local // LANES
    if FIELDS * (scan_local // groups) <= span:
        turns, grad_row = divmod(HEAD - 1, slot_rows)
        grad_lane, used = turns * span, slot_rows
    else:
        grad_row, grad_lane, used = slot_rows, 0, slot_rows + 1
    return span, slot_rows, sum_rows, grad_row, grad_lane, max(used, sum_rows)


def partner(index, k, groups):
    return index ^ k if groups & (groups - 1) == 0 else (index + k) % groups


def pair_kernel(devices, groups, place_ref, samples_ref, recv_ref, flat_ref, back_ref, point_ref, mate_ref, note_ref):
    scan_local, _, tiles, _ = samples_ref.shape
    slots = flat_ref.shape[1]
    cap = slots // devices
    block = COORDS * cap + 1
    scans = devices // groups
    for d in range(devices):
        note_ref[pl.ds(d, 1), :] = recv_ref[pl.ds(d * block + COORDS * cap, 1), :]
    notes = note_ref[...].astype(jnp.bfloat16)
    mine = div(iota((devices, slots), 1), cap) == iota((devices, slots), 0)
    rows = []
    for f in range(3):
        spread = (iota((LANES, slots), 0) == mod(iota((LANES, slots), 1), cap) + f * cap).astype(jnp.float32)
        rows.append(
            jnp.sum(jnp.where(mine, dot(notes, spread.astype(jnp.bfloat16)), 0.0), axis=0, keepdims=True)
        )
    flag_row, mate_row, tile_row = rows
    code_row = (mate_row * tiles + tile_row).astype(jnp.int32)
    table = scan_local * tiles
    chosen = (iota((table, slots), 0) == code_row).astype(jnp.float32).astype(jnp.bfloat16)
    for a in range(FIELDS):
        values = jnp.concatenate([samples_ref[b, a] for b in range(scan_local)], axis=0)
        turned = jnp.concatenate([values[h : h + LANES].T for h in range(0, table, LANES)], axis=1)
        parts = [dot(part, chosen) for part in pieces(turned, 3)]
        mate_ref[a] = (parts[0] + parts[1]) + parts[2]
    per_chunk = LANES // cap
    for c in range(slots // LANES):
        for a in range(COORDS):
            stack = [
                recv_ref[pl.ds(d * block + a * cap, cap), :] for d in range(c * per_chunk, (c + 1) * per_chunk)
            ]
            point_ref[a, :, c * LANES : (c + 1) * LANES] = jnp.concatenate(stack, axis=0).T
    for c in range(slots // LANES):
        lanes = slice(c * LANES, (c + 1) * LANES)

        def step(k, sums):
            at = pl.ds(pl.multiple_of(k * 8, 8), 8)
            px, py, pz = [point_ref[a, at, lanes] for a in range(COORDS)]
            present = px < FAR
            px = jnp.where(present, px, 0.0)
            qx, qy, qz, nx, ny, nz = [mate_ref[a, at, lanes] for a in range(FIELDS)]
            residual = nx * (px - qx) + ny * (py - qy) + nz * (pz - qz)
            weight = jnp.where(present, 1.0 / (1.0 + residual * residual), 0.0)
            jac = [py * nz - pz * ny, pz * nx - px * nz, px * ny - py * nx, nx, ny, nz]
            scaled = [weight * j for j in jac]
            terms = [scaled[i] * jac[j] for i, j in PAIRS] + [residual * s for s in scaled]
            return tuple(s + t for s, t in zip(sums, terms))

        zero = jnp.zeros((8, LANES), jnp.float32)
        sums = lax.fori_loop(0, LANES // 8, step, (zero,) * (MAT + FIELDS), unroll=16)
        filled = flag_row[:, lanes] > 0.0
        lines = [jnp.where(filled, jnp.sum(s, axis=0, keepdims=True), 0.0) for s in sums]
        blank = jnp.zeros((1, LANES), jnp.float32)
        lines[MAT:MAT] = [flag_row[:, lanes], mate_row[:, lanes], blank]
        lines += [blank] * (WIDTH - len(lines))
        flat_ref[:, lanes] = jnp.concatenate(lines, axis=0)
    scans = devices // groups
    span, slot_rows, sum_rows, grad_row, grad_lane, rows = back_layout(scan_local, groups, cap)
    columns = scans * scan_local // groups
    near_group = div(place_ref[0] * scan_local, columns)
    peer = div(div(iota((1, slots), 1), cap), groups)
    member = flag_row.astype(jnp.int32) - 1
    source = jnp.where(member >= 0, peer * scan_local + member, -1)
    source_hot = (iota((scans * scan_local, slots), 0) == source).astype(jnp.float32).astype(jnp.bfloat16)
    parts = [dot(part, source_hot, BOTH_LANES) for part in pieces(flat_ref[...], 3)]
    sums = (parts[0] + parts[1]) + parts[2]
    share = scan_local // groups
    few = iota((FIELDS * share, slots), 0)
    chosen = jnp.concatenate(
        [jnp.broadcast_to(flat_ref[HEAD + q : HEAD + q + 1, :], (share, slots)) for q in range(FIELDS)], axis=0
    )
    chosen = jnp.where(member == near_group * share + mod(few, share), chosen, 0.0)
    blank = [jnp.zeros((n, slots), jnp.float32) for n in (grad_lane, LANES - grad_lane - FIELDS * share)]
    chosen = jnp.concatenate([blank[0], chosen, blank[1]] if grad_lane else [chosen, blank[1]], axis=0)
    peer_hot = (iota((scans, slots), 0) == peer).astype(jnp.float32).astype(jnp.bfloat16)
    parts = [dot(peer_hot, part, BOTH_LANES) for part in pieces(chosen, 3)]
    grads = (parts[0] + parts[1]) + parts[2]
    slot_lane = div(iota((slot_rows, LANES), 1), span)
    sum_lane = div(iota((sum_rows, LANES), 1), scan_local)
    tails = []
    for scan in range(scans):
        c, start = divmod(scan * span, LANES)
        body = None
        for i in range(LANES // span):
            piece = flat_ref[i * slot_rows : (i + 1) * slot_rows, c * LANES : (c + 1) * LANES]
            piece = turn(piece, i * span - start)
            body = piece if i == 0 else jnp.where(slot_lane == i, piece, body)
        if grad_row < slot_rows:
            body = jnp.where(
                (iota((slot_rows, LANES), 0) == grad_row) & (iota((slot_rows, LANES), 1) >= grad_lane),
                grads[scan : scan + 1],
                body,
            )
        c, start = divmod(scan * scan_local, LANES)
        tail = None
        for i in range(WIDTH // sum_rows):
            piece = turn(sums[i * sum_rows : (i + 1) * sum_rows, c * LANES : (c + 1) * LANES], i * scan_local - start)
            tail = piece if i == 0 else jnp.where(sum_lane == i, piece, tail)
        tails.append(tail)
        for c in range(groups):
            at = (scan * groups + c) * rows
            back_ref[at : at + slot_rows, :] = body
            if rows > slot_rows:
                back_ref[at + slot_rows : at + rows, :] = jnp.broadcast_to(
                    grads[scan : scan + 1], (rows - slot_rows, LANES)
                )
    for c in range(groups):

        @pl.when(near_group != c)
        def _():
            for scan in range(scans):
                at = (scan * groups + c) * rows
                back_ref[at : at + sum_rows, :] = tails[scan]


def layout(scan_local, groups, scan_total):
    columns = scan_total // groups
    pack = max(1, LANES // columns)
    per_block = -(-(MAT + 1) // pack)
    return columns, pack, per_block


def block_rows(every, row_hot, count):
    high = every.astype(jnp.bfloat16).astype(jnp.float32)
    for part in (high, every - high):
        yield jnp.concatenate(
            [jnp.where(row_hot, part[q : q + 1], 0.0).astype(jnp.bfloat16) for q in range(count)], axis=0
        )


def held_kernel(devices, groups, scan_local, scan_ref, group_ref, flat_ref, *refs):
    out_refs, stage_ref = refs[:-1], refs[-1]
    slots = flat_ref.shape[1]
    cap = slots // devices
    scan_total = scan_local * (devices // groups)
    columns, pack, per_block = layout(scan_local, groups, scan_total)
    every = flat_ref[...]
    row = every[ROW_MATE : ROW_MATE + 1].astype(jnp.int32)
    other = div(div(iota((1, slots), 1), cap), groups) * scan_local + every[ROW_FLAG : ROW_FLAG + 1].astype(jnp.int32) - 1
    own = scan_ref[0] * scan_local + row
    row_hot = iota((scan_local, slots), 0) == row
    column = iota((scan_total, slots), 0)
    mix = ((column == own).astype(jnp.float32) - (column == other).astype(jnp.float32)).astype(jnp.bfloat16)
    hess = sum(dot(rows, mix, BOTH_LANES) for rows in block_rows(every, row_hot, MAT))
    lane = iota((scan_local, LANES), 1)
    home = MAT // per_block
    grad = jnp.zeros((scan_local, LANES), jnp.float32)
    for q in range(FIELDS):
        value = jnp.sum(jnp.where(row_hot, every[HEAD + q : HEAD + q + 1], 0.0), axis=1, keepdims=True)
        grad = jnp.where(lane == home * columns + q, -value, grad)
    for c in range(groups):
        side, shift = divmod(c * columns, LANES)
        for r in range(per_block):
            tile = jnp.zeros((scan_local, LANES), jnp.float32)
            for k in range(pack):
                q = k * per_block + r
                if q < MAT:
                    value = hess[q * scan_local : (q + 1) * scan_local, side * LANES : (side + 1) * LANES]
                    value = turn(value, k * columns - shift)
                elif q == MAT:
                    value = grad
                else:
                    continue
                tile = jnp.where(div(lane, columns) == k, value, tile) if pack > 1 else value
            stage_ref[c, r * scan_local : (r + 1) * scan_local, :] = tile
    for k, out_ref in enumerate(out_refs):
        out_ref[...] = stage_ref[partner(group_ref[0], k, groups)]


def close_kernel(devices, groups, cap, scan_ref, group_ref, back_ref, *refs):
    part_refs, (hess_ref, grad_ref, every_ref, hold_ref) = refs[:groups], refs[groups:]
    scan_local, columns = hess_ref.shape[1:]
    per_block = part_refs[0].shape[0] // scan_local
    span, slot_rows, sum_rows, grad_row, grad_lane, block = back_layout(scan_local, groups, cap)
    senders = devices // groups
    first = group_ref[0] * (senders * block)
    lane_block = div(iota((slot_rows, LANES), 1), span)
    per_chunk = LANES // span
    for chunk in range(senders // per_chunk):
        found = [back_ref[pl.ds(first + (chunk * per_chunk + u) * block, slot_rows), :] for u in range(per_chunk)]
        for i in range(LANES // span):
            tile = None
            for u in range(per_chunk):
                piece = turn(found[u], (u - i) * span)
                tile = piece if u == 0 else jnp.where(lane_block == u, piece, tile)
            every_ref[i * slot_rows : (i + 1) * slot_rows, chunk * LANES : (chunk + 1) * LANES] = tile
    every = every_ref[...]
    total = every.shape[1]
    row = every[ROW_FLAG : ROW_FLAG + 1].astype(jnp.int32) - 1
    mate = every[ROW_MATE : ROW_MATE + 1].astype(jnp.int32)
    column = div(div(iota((1, total), 1), span), groups) * scan_local + mate
    row_hot = iota((scan_local, total), 0) == row
    offset = scan_ref[0] * scan_local - group_ref[0] * columns
    line = iota((columns, total), 0)
    mix = (line == row + offset).astype(jnp.float32) - (line == column).astype(jnp.float32)
    mix = mix.astype(jnp.bfloat16)
    cross = sum(dot(rows, mix, BOTH_LANES) for rows in block_rows(every, row_hot, MAT))
    sums = jnp.zeros((sum_rows, LANES), jnp.float32)
    for c in range(groups):
        part = back_ref[c * senders * block : c * senders * block + sum_rows, :]
        for d in range(c * senders + 1, (c + 1) * senders):
            part = part + back_ref[d * block : d * block + sum_rows, :]
        sums = sums + jnp.where(group_ref[0] != c, part, 0.0)
    near = back_ref[pl.ds(first + grad_row, 1), :]
    for u in range(1, senders):
        near = near + back_ref[pl.ds(first + u * block + grad_row, 1), :]
    line = iota((scan_local, LANES), 0)
    lane = iota((scan_local, LANES), 1)

    def by_row(q):
        i, r = divmod(q, sum_rows)
        return jnp.sum(jnp.where(lane == line + i * scan_local, sums[r : r + 1], 0.0), axis=1, keepdims=True)

    whole = part_refs[0][...]
    for part_ref in part_refs[1:]:
        whole = whole + part_ref[...]
    diagonal = iota((scan_local, columns), 1) == iota((scan_local, columns), 0) + offset
    for q in range(MAT):
        k, r = divmod(q, per_block)
        tile = whole[r * scan_local : (r + 1) * scan_local, k * columns : (k + 1) * columns]
        tile = tile + cross[q * scan_local : (q + 1) * scan_local]
        tile = tile + jnp.where(diagonal, by_row(q), 0.0)
        i, j = PAIRS[q]
        hess_ref[i * FIELDS + j] = tile
        if i != j:
            hess_ref[j * FIELDS + i] = tile
    k, r = divmod(MAT, per_block)
    grad = turn(whole[r * scan_local : (r + 1) * scan_local], -k * columns)
    for q in range(FIELDS):
        grad = grad + jnp.where(lane == q, by_row(HEAD + q), 0.0)
    hold_ref[...] = grad
    part = scan_local // groups
    own = jnp.zeros((part, LANES), jnp.float32)
    for q in range(FIELDS):
        spot = grad_lane + q * part + iota((part, LANES), 0) == iota((part, LANES), 1)
        value = jnp.sum(jnp.where(spot, near, 0.0), axis=1, keepdims=True)
        own = jnp.where(iota((part, LANES), 1) == q, value, own)
    hold = hold_ref[pl.ds(group_ref[0] * part, part), :] + own
    grad_ref[...] = hold[:, 0:FIELDS]


def call(kernel, out_shape, smem, vmem, scratch=()):
    body = pl.pallas_call(
        kernel,
        out_shape=out_shape,
        in_specs=[pl.BlockSpec(memory_space=pltpu.SMEM)] * smem + [pl.BlockSpec(memory_space=pltpu.VMEM)] * vmem,
        scratch_shapes=list(scratch),
    )

    def run(*args):
        args = args[:smem] + tuple(pltpu.with_memory_space_constraint(x, pltpu.VMEM) for x in args[smem:])
        return body(*args)

    return run


def f32(*shape):
    return jax.ShapeDtypeStruct(shape, jnp.float32)


def near(*shape):
    return pltpu.VMEM(shape, jnp.float32)


def exchange(x, axes):
    count, width = x.shape
    moved = lax.all_to_all(x.reshape(count, 1, width), axes, split_axis=0, concat_axis=0, tiled=True)
    return moved.reshape(count, width)


def local(samples, point_count, corr_scan, corr_tile, corr_src):
    devices = lax.axis_size(AXES)
    groups = lax.axis_size("grp")
    samples = samples.transpose(0, 2, 1, 3)
    scan_local, tiles, per_scan, entries, cap, block = sizes(samples.shape, corr_scan.shape, devices)
    slots = devices * cap
    scan_total = scan_local * (devices // groups)
    columns, pack, per_block = layout(scan_local, groups, scan_total)
    group = lax.axis_index("grp").astype(jnp.int32).reshape(1)
    scan = lax.axis_index("scan").astype(jnp.int32).reshape(1)
    back_rows = back_layout(scan_local, groups, cap)[-1]

    def bind(kernel, *args):
        return lambda *refs: kernel(*args, *refs)

    sent, samples = pl.pallas_call(
        bind(send_kernel, devices, groups),
        out_shape=(near(devices * block, LANES), near(*samples.shape)),
        in_specs=[pl.BlockSpec(memory_space=pltpu.SMEM)] * 2 + [pl.BlockSpec(memory_space=pl.ANY)] * 5,
        scratch_shapes=[
            pltpu.SMEM(point_count.shape, jnp.int32),
            pltpu.VMEM(corr_scan.shape, jnp.int32),
            pltpu.VMEM(corr_tile.shape, jnp.int32),
            pltpu.VMEM(corr_src.shape, jnp.int32),
            pltpu.VMEM((COORDS, entries, LANES), jnp.float32),
            pltpu.SemaphoreType.DMA((5,)),
        ],
    )(scan, group, point_count, samples, corr_scan, corr_tile, corr_src)
    received = exchange(sent, AXES)
    flat, back = call(
        bind(pair_kernel, devices, groups),
        (near(WIDTH, slots), near(devices * back_rows, LANES)),
        1,
        2,
        [
            pltpu.VMEM((COORDS, LANES, slots), jnp.float32),
            pltpu.VMEM((FIELDS, LANES, slots), jnp.float32),
            pltpu.VMEM((devices, LANES), jnp.float32),
        ],
    )(scan, samples, received)
    back = exchange(back, AXES)
    share = near(per_block * scan_local, LANES)
    shares = call(
        bind(held_kernel, devices, groups, scan_local),
        (share,) * groups,
        2,
        1,
        [pltpu.VMEM((groups,) + share.shape, jnp.float32)],
    )(scan, group, flat)
    shares = [shares[0]] + [
        lax.ppermute(shares[k], "grp", [(g, partner(g, k, groups)) for g in range(groups)]) for k in range(1, groups)
    ]
    hess, grad = call(
        bind(close_kernel, devices, groups, cap),
        (f32(FIELDS * FIELDS, scan_local, columns), f32(scan_local // groups, FIELDS)),
        2,
        1 + groups,
        [
            pltpu.VMEM((HEAD, (devices // groups) * groups * cap), jnp.float32),
            pltpu.VMEM((scan_local, LANES), jnp.float32),
        ],
    )(scan, group, back, *shares)
    return hess.reshape(FIELDS, FIELDS, scan_local, columns).transpose(2, 0, 1, 3), grad


def solution(mesh):
    placed = (
        P("scan", "grp", None, None),
        P("scan"),
        P("scan", "grp"),
        P("scan", "grp"),
        P("scan", "grp", None),
    )
    return jax.shard_map(
        local,
        mesh=mesh,
        in_specs=placed,
        out_specs=(P("scan", None, None, "grp"), P(AXES, None)),
        check_vma=False,
    )
```

```python
import jax
import jax.numpy as jnp
from jax import lax
from jax.experimental import pallas as pl
from jax.experimental.pallas import tpu as pltpu
from jax.sharding import PartitionSpec as P

LANES = 128
COORDS = 3
FIELDS = 6
PAIRS = [(i, j) for i in range(FIELDS) for j in range(i, FIELDS)]
MAT = len(PAIRS)
ROW_FLAG = MAT
ROW_MATE = MAT + 1
HEAD = MAT + 3
WIDTH = 32
FAR = 2.0**100
BOTH_LANES = (((1,), (1,)), ((), ()))
AXES = ("scan", "grp")


def div(x, n):
    if n & (n - 1) == 0:
        return lax.shift_right_logical(x, jnp.int32(n.bit_length() - 1))
    return x // n


def mod(x, n):
    if n & (n - 1) == 0:
        return x & (n - 1)
    return x % n


def iota(shape, dim):
    return lax.broadcasted_iota(jnp.int32, shape, dim)


def pieces(x, count):
    parts = []
    for _ in range(count - 1):
        part = x.astype(jnp.bfloat16)
        parts.append(part)
        x = x - part.astype(jnp.float32)
    parts.append(x.astype(jnp.bfloat16))
    return parts


def dot(a, b, dims=(((1,), (0,)), ((), ()))):
    return lax.dot_general(a, b, dims, preferred_element_type=jnp.float32)


def sizes(samples_shape, entries_shape, devices):
    scan_local, _, tiles, _ = samples_shape
    per_scan = entries_shape[1]
    entries = scan_local * per_scan
    cap = 2 * entries // devices
    return scan_local, tiles, per_scan, entries, cap, COORDS * cap + 1


def send_kernel(
    devices,
    groups,
    place_ref,
    group_ref,
    count_hbm,
    samples_hbm,
    scan_hbm,
    tile_hbm,
    src_hbm,
    out_ref,
    samples_ref,
    count_ref,
    scan_ref,
    tile_ref,
    src_ref,
    data_ref,
    sems,
):
    scan_local, tiles, per_scan, entries, cap, block = sizes(samples_ref.shape, scan_ref.shape, devices)
    group_points = tiles * LANES
    pairs = (
        (scan_hbm, scan_ref),
        (tile_hbm, tile_ref),
        (count_hbm, count_ref),
        (src_hbm, src_ref),
        (samples_hbm, samples_ref),
    )
    loads = [pltpu.make_async_copy(far, here, sems.at[k]) for k, (far, here) in enumerate(pairs)]
    for load in loads:
        load.start()
    for load in loads[:2]:
        load.wait()

    scans = scan_ref[...]
    tile_ids = tile_ref[...]
    device = div(scans, scan_local) * groups + div(tile_ids, tiles)
    stacked = jnp.concatenate(
        [device.astype(jnp.float32), mod(scans, scan_local).astype(jnp.float32), mod(tile_ids, tiles).astype(jnp.float32)],
        axis=0,
    ).astype(jnp.bfloat16)
    spread = (mod(iota((per_scan, entries), 1), per_scan) == iota((per_scan, entries), 0)).astype(jnp.float32)
    wide = dot(stacked, spread.astype(jnp.bfloat16))
    own = div(iota((scan_local, entries), 1), per_scan) == iota((scan_local, entries), 0)
    device_row, mate_row, tile_row = [
        jnp.sum(jnp.where(own, wide[f * scan_local : (f + 1) * scan_local], 0.0), axis=0, keepdims=True)
        for f in range(3)
    ]
    rank_parts = []
    columns = []
    for h in range(entries // LANES):
        across = device_row[:, h * LANES : (h + 1) * LANES]
        columns.append(jnp.broadcast_to(across, (LANES, LANES)).T)
        total = jnp.zeros((1, LANES), jnp.float32)
        for g in range(h + 1):
            same = columns[g] == across
            if g == h:
                same = same & (iota((LANES, LANES), 0) < iota((LANES, LANES), 1))
            total = total + jnp.sum(same.astype(jnp.float32), axis=0, keepdims=True)
        rank_parts.append(total)
    rank_row = jnp.concatenate(rank_parts, axis=1)
    slot_row = (device_row * cap + rank_row).astype(jnp.int32)
    place = (iota((devices * cap, entries), 0) == slot_row).astype(jnp.float32).astype(jnp.bfloat16)
    owner_row = (div(iota((1, entries), 1), per_scan) + 1).astype(jnp.float32)
    field = div(iota((LANES, entries), 0), cap)
    picked = jnp.where(field == 0, owner_row, jnp.where(field == 1, mate_row, tile_row))
    picked = jnp.where(
        (mod(iota((LANES, entries), 0), cap).astype(jnp.float32) == rank_row) & (field < 3), picked, 0.0
    ).astype(jnp.bfloat16)
    towards = (iota((devices, entries), 0).astype(jnp.float32) == device_row).astype(jnp.float32).astype(jnp.bfloat16)
    notes = dot(towards, picked, BOTH_LANES)
    for d in range(devices):
        out_ref[pl.ds(d * block + COORDS * cap, 1), :] = notes[d : d + 1]

    for load in loads[2:]:
        load.wait()

    def one_scan(s, carry):
        limit = count_ref[s] - group_ref[0] * group_points
        for h in range(per_scan // 8):
            ids = src_ref[s, pl.ds(h * 8, 8), :]
            lane = mod(ids, LANES)
            tile = div(ids, LANES)
            found = [jnp.zeros((8, LANES), jnp.float32) for _ in range(COORDS)]
            for t in range(tiles):
                here = tile == t
                for a in range(COORDS):
                    row = jnp.broadcast_to(samples_ref[s, a, t : t + 1, :], (8, LANES))
                    found[a] = jnp.where(here, jnp.take_along_axis(row, lane, axis=1), found[a])
            found[0] = jnp.where(ids < limit, found[0], FAR)
            at = pl.multiple_of(s * per_scan + h * 8, 8)
            for a in range(COORDS):
                data_ref[a, pl.ds(at, 8), :] = found[a]
        present = iota((tiles, LANES), 0) * LANES + iota((tiles, LANES), 1) < limit
        for a in range(COORDS, FIELDS):
            samples_ref[s, a] = jnp.where(present, samples_ref[s, a], 0.0)
        return carry

    lax.fori_loop(0, scan_local, one_scan, 0, unroll=8)

    thirds = [jnp.concatenate(part, axis=1) for part in zip(*[pieces(data_ref[a], 3) for a in range(COORDS)])]
    moved = dot(jnp.concatenate([place] * 3, axis=1), jnp.concatenate(thirds, axis=0))
    for a in range(COORDS):
        for d in range(devices):
            out_ref[pl.ds(d * block + a * cap, cap), :] = moved[d * cap : (d + 1) * cap, a * LANES : (a + 1) * LANES]


def turn(x, amount):
    amount = amount % LANES
    return pltpu.roll(x, amount, 1) if amount else x


def back_layout(scan_local, groups, cap):
    span = groups * cap
    slot_rows = HEAD * span // LANES
    sum_rows = WIDTH * scan_local // LANES
    if FIELDS * (scan_local // groups) <= span:
        turns, grad_row = divmod(HEAD - 1, slot_rows)
        grad_lane, used = turns * span, slot_rows
    else:
        grad_row, grad_lane, used = slot_rows, 0, slot_rows + 1
    return span, slot_rows, sum_rows, grad_row, grad_lane, max(used, sum_rows)


def partner(index, k, groups):
    return index ^ k if groups & (groups - 1) == 0 else (index + k) % groups


def pair_kernel(devices, groups, place_ref, samples_ref, recv_ref, flat_ref, back_hbm, back_ref, point_ref, mate_ref, note_ref, sems):
    scan_local, _, tiles, _ = samples_ref.shape
    slots = flat_ref.shape[1]
    cap = slots // devices
    block = COORDS * cap + 1
    scans = devices // groups
    for d in range(devices):
        note_ref[pl.ds(d, 1), :] = recv_ref[pl.ds(d * block + COORDS * cap, 1), :]
    notes = note_ref[...].astype(jnp.bfloat16)
    mine = div(iota((devices, slots), 1), cap) == iota((devices, slots), 0)
    rows = []
    for f in range(3):
        spread = (iota((LANES, slots), 0) == mod(iota((LANES, slots), 1), cap) + f * cap).astype(jnp.float32)
        rows.append(
            jnp.sum(jnp.where(mine, dot(notes, spread.astype(jnp.bfloat16)), 0.0), axis=0, keepdims=True)
        )
    flag_row, mate_row, tile_row = rows
    code_row = (mate_row * tiles + tile_row).astype(jnp.int32)
    table = scan_local * tiles
    chosen = (iota((table, slots), 0) == code_row).astype(jnp.float32).astype(jnp.bfloat16)
    for a in range(FIELDS):
        values = jnp.concatenate([samples_ref[b, a] for b in range(scan_local)], axis=0)
        turned = jnp.concatenate([values[h : h + LANES].T for h in range(0, table, LANES)], axis=1)
        parts = [dot(part, chosen) for part in pieces(turned, 3)]
        mate_ref[a] = (parts[0] + parts[1]) + parts[2]
    per_chunk = LANES // cap
    for c in range(slots // LANES):
        for a in range(COORDS):
            stack = [
                recv_ref[pl.ds(d * block + a * cap, cap), :] for d in range(c * per_chunk, (c + 1) * per_chunk)
            ]
            point_ref[a, :, c * LANES : (c + 1) * LANES] = jnp.concatenate(stack, axis=0).T
    span, slot_rows, sum_rows, grad_row, grad_lane, rows = back_layout(scan_local, groups, cap)
    near_group = div(place_ref[0] * scan_local, scans * scan_local // groups)
    share = scan_local // groups
    slot_lane = div(iota((slot_rows, LANES), 1), span)
    sum_lane = div(iota((sum_rows, LANES), 1), scan_local)
    grad_spot = (iota((slot_rows, LANES), 0) == grad_row) & (iota((slot_rows, LANES), 1) >= grad_lane)
    peer = div(iota((1, LANES), 1), span)
    per_line = LANES // span
    stores = []
    for c in range(slots // LANES):
        lanes = slice(c * LANES, (c + 1) * LANES)

        def step(k, sums):
            at = pl.ds(pl.multiple_of(k * 8, 8), 8)
            px, py, pz = [point_ref[a, at, lanes] for a in range(COORDS)]
            present = px < FAR
            px = jnp.where(present, px, 0.0)
            qx, qy, qz, nx, ny, nz = [mate_ref[a, at, lanes] for a in range(FIELDS)]
            residual = nx * (px - qx) + ny * (py - qy) + nz * (pz - qz)
            weight = jnp.where(present, 1.0 / (1.0 + residual * residual), 0.0)
            jac = [py * nz - pz * ny, pz * nx - px * nz, px * ny - py * nx, nx, ny, nz]
            scaled = [weight * j for j in jac]
            terms = [scaled[i] * jac[j] for i, j in PAIRS] + [residual * s for s in scaled]
            return tuple(s + t for s, t in zip(sums, terms))

        zero = jnp.zeros((8, LANES), jnp.float32)
        sums = lax.fori_loop(0, LANES // 8, step, (zero,) * (MAT + FIELDS), unroll=16)
        filled = flag_row[:, lanes] > 0.0
        lines = [jnp.where(filled, jnp.sum(s, axis=0, keepdims=True), 0.0) for s in sums]
        blank = jnp.zeros((1, LANES), jnp.float32)
        lines[MAT:MAT] = [flag_row[:, lanes], mate_row[:, lanes], blank]
        lines += [blank] * (WIDTH - len(lines))
        flat = jnp.concatenate(lines, axis=0)
        flat_ref[:, lanes] = flat
        member = flag_row[:, lanes].astype(jnp.int32) - 1
        source = jnp.where(member >= 0, peer * scan_local + member, -1)
        source_hot = (iota((LANES, LANES), 0) == source).astype(jnp.float32).astype(jnp.bfloat16)
        totals = dot(
            jnp.concatenate(pieces(flat, 3), axis=1), jnp.concatenate([source_hot] * 3, axis=1), BOTH_LANES
        )
        chosen = jnp.concatenate(
            [jnp.broadcast_to(flat[HEAD + q : HEAD + q + 1, :], (share, LANES)) for q in range(FIELDS)], axis=0
        )
        chosen = jnp.where(member == near_group * share + mod(iota(chosen.shape, 0), share), chosen, 0.0)
        below = jnp.zeros((LANES - grad_lane - FIELDS * share, LANES), jnp.float32)
        above = [jnp.zeros((grad_lane, LANES), jnp.float32)] if grad_lane else []
        chosen = jnp.concatenate(above + [chosen, below], axis=0)
        peer_hot = (iota((8, LANES), 0) == peer).astype(jnp.float32).astype(jnp.bfloat16)
        grads = dot(
            jnp.concatenate([peer_hot] * 3, axis=1), jnp.concatenate(pieces(chosen, 3), axis=1), BOTH_LANES
        )
        for u in range(per_line):
            body = None
            for i in range(per_line):
                piece = turn(flat[i * slot_rows : (i + 1) * slot_rows], (i - u) * span)
                body = piece if i == 0 else jnp.where(slot_lane == i, piece, body)
            if grad_row < slot_rows:
                body = jnp.where(grad_spot, grads[u : u + 1], body)
            else:
                body = jnp.concatenate([body, grads[u : u + 1]], axis=0)
            tail = None
            for i in range(WIDTH // sum_rows):
                piece = turn(totals[i * sum_rows : (i + 1) * sum_rows], (i - u) * scan_local)
                tail = piece if i == 0 else jnp.where(sum_lane == i, piece, tail)
            for g in range(groups):
                at = ((c * per_line + u) * groups + g) * rows
                back_ref[at : at + body.shape[0], :] = body
                back_ref[at : at + sum_rows, :] = jnp.where(near_group != g, tail, body[0:sum_rows])
        at = pl.ds(c * per_line * groups * rows, per_line * groups * rows)
        stores.append(pltpu.make_async_copy(back_ref.at[at], back_hbm.at[at], sems.at[c]))
        stores[-1].start()
    for store in stores:
        store.wait()


def layout(scan_local, groups, scan_total):
    columns = scan_total // groups
    pack = max(1, LANES // columns)
    per_block = -(-(MAT + 1) // pack)
    return columns, pack, per_block


def block_rows(every, row_hot, count):
    high = every.astype(jnp.bfloat16).astype(jnp.float32)
    for part in (high, every - high):
        yield jnp.concatenate(
            [jnp.where(row_hot, part[q : q + 1], 0.0).astype(jnp.bfloat16) for q in range(count)], axis=0
        )


def held_kernel(devices, groups, scan_local, scan_ref, group_ref, flat_ref, *refs):
    out_refs, stage_ref = refs[:-1], refs[-1]
    slots = flat_ref.shape[1]
    cap = slots // devices
    scan_total = scan_local * (devices // groups)
    columns, pack, per_block = layout(scan_local, groups, scan_total)
    every = flat_ref[...]
    row = every[ROW_MATE : ROW_MATE + 1].astype(jnp.int32)
    other = div(div(iota((1, slots), 1), cap), groups) * scan_local + every[ROW_FLAG : ROW_FLAG + 1].astype(jnp.int32) - 1
    own = scan_ref[0] * scan_local + row
    row_hot = iota((scan_local, slots), 0) == row
    column = iota((scan_total, slots), 0)
    mix = ((column == own).astype(jnp.float32) - (column == other).astype(jnp.float32)).astype(jnp.bfloat16)
    hess = sum(dot(rows, mix, BOTH_LANES) for rows in block_rows(every, row_hot, MAT))
    lane = iota((scan_local, LANES), 1)
    home = MAT // per_block
    grad = jnp.zeros((scan_local, LANES), jnp.float32)
    for q in range(FIELDS):
        value = jnp.sum(jnp.where(row_hot, every[HEAD + q : HEAD + q + 1], 0.0), axis=1, keepdims=True)
        grad = jnp.where(lane == home * columns + q, -value, grad)
    for c in range(groups):
        side, shift = divmod(c * columns, LANES)
        for r in range(per_block):
            tile = jnp.zeros((scan_local, LANES), jnp.float32)
            for k in range(pack):
                q = k * per_block + r
                if q < MAT:
                    value = hess[q * scan_local : (q + 1) * scan_local, side * LANES : (side + 1) * LANES]
                    value = turn(value, k * columns - shift)
                elif q == MAT:
                    value = grad
                else:
                    continue
                tile = jnp.where(div(lane, columns) == k, value, tile) if pack > 1 else value
            stage_ref[c, r * scan_local : (r + 1) * scan_local, :] = tile
    for k, out_ref in enumerate(out_refs):
        out_ref[...] = stage_ref[partner(group_ref[0], k, groups)]


def close_kernel(devices, groups, cap, scan_ref, group_ref, back_ref, *refs):
    part_refs, (hess_ref, grad_ref, every_ref, hold_ref) = refs[:groups], refs[groups:]
    scan_local, columns = hess_ref.shape[1:]
    per_block = part_refs[0].shape[0] // scan_local
    span, slot_rows, sum_rows, grad_row, grad_lane, block = back_layout(scan_local, groups, cap)
    senders = devices // groups
    first = group_ref[0] * (senders * block)
    lane_block = div(iota((slot_rows, LANES), 1), span)
    per_chunk = LANES // span
    for chunk in range(senders // per_chunk):
        found = [back_ref[pl.ds(first + (chunk * per_chunk + u) * block, slot_rows), :] for u in range(per_chunk)]
        for i in range(LANES // span):
            tile = None
            for u in range(per_chunk):
                piece = turn(found[u], (u - i) * span)
                tile = piece if u == 0 else jnp.where(lane_block == u, piece, tile)
            every_ref[i * slot_rows : (i + 1) * slot_rows, chunk * LANES : (chunk + 1) * LANES] = tile
    every = every_ref[...]
    total = every.shape[1]
    row = every[ROW_FLAG : ROW_FLAG + 1].astype(jnp.int32) - 1
    mate = every[ROW_MATE : ROW_MATE + 1].astype(jnp.int32)
    column = div(div(iota((1, total), 1), span), groups) * scan_local + mate
    row_hot = iota((scan_local, total), 0) == row
    offset = scan_ref[0] * scan_local - group_ref[0] * columns
    line = iota((columns, total), 0)
    mix = (line == row + offset).astype(jnp.float32) - (line == column).astype(jnp.float32)
    mix = mix.astype(jnp.bfloat16)
    rows = jnp.concatenate(list(block_rows(every, row_hot, MAT)), axis=1)
    cross = dot(rows, jnp.concatenate([mix, mix], axis=1), BOTH_LANES)
    sums = jnp.zeros((sum_rows, LANES), jnp.float32)
    for c in range(groups):
        part = back_ref[c * senders * block : c * senders * block + sum_rows, :]
        for d in range(c * senders + 1, (c + 1) * senders):
            part = part + back_ref[d * block : d * block + sum_rows, :]
        sums = sums + jnp.where(group_ref[0] != c, part, 0.0)
    near = back_ref[pl.ds(first + grad_row, 1), :]
    for u in range(1, senders):
        near = near + back_ref[pl.ds(first + u * block + grad_row, 1), :]
    line = iota((scan_local, LANES), 0)
    lane = iota((scan_local, LANES), 1)

    def by_row(q):
        i, r = divmod(q, sum_rows)
        return jnp.sum(jnp.where(lane == line + i * scan_local, sums[r : r + 1], 0.0), axis=1, keepdims=True)

    whole = part_refs[0][...]
    for part_ref in part_refs[1:]:
        whole = whole + part_ref[...]
    diagonal = iota((scan_local, columns), 1) == iota((scan_local, columns), 0) + offset
    shifted = pltpu.roll(sums, mod(offset + LANES * (devices // groups), LANES), 1)
    facing = [turn(shifted, -n * scan_local) for n in range(WIDTH // sum_rows)]
    for q in range(MAT):
        k, r = divmod(q, per_block)
        tile = whole[r * scan_local : (r + 1) * scan_local, k * columns : (k + 1) * columns]
        tile = tile + cross[q * scan_local : (q + 1) * scan_local]
        n, r = divmod(q, sum_rows)
        tile = tile + jnp.where(diagonal, facing[n][r : r + 1, 0:columns], 0.0)
        i, j = PAIRS[q]
        hess_ref[i * FIELDS + j] = tile
        if i != j:
            hess_ref[j * FIELDS + i] = tile
    k, r = divmod(MAT, per_block)
    grad = turn(whole[r * scan_local : (r + 1) * scan_local], -k * columns)
    for q in range(FIELDS):
        grad = grad + jnp.where(lane == q, by_row(HEAD + q), 0.0)
    hold_ref[...] = grad
    part = scan_local // groups
    own = jnp.zeros((part, LANES), jnp.float32)
    for q in range(FIELDS):
        spot = grad_lane + q * part + iota((part, LANES), 0) == iota((part, LANES), 1)
        value = jnp.sum(jnp.where(spot, near, 0.0), axis=1, keepdims=True)
        own = jnp.where(iota((part, LANES), 1) == q, value, own)
    hold = hold_ref[pl.ds(group_ref[0] * part, part), :] + own
    grad_ref[...] = hold[:, 0:FIELDS]


def call(kernel, out_shape, smem, vmem, scratch=(), out_specs=None):
    body = pl.pallas_call(
        kernel,
        out_shape=out_shape,
        in_specs=[pl.BlockSpec(memory_space=pltpu.SMEM)] * smem + [pl.BlockSpec(memory_space=pltpu.VMEM)] * vmem,
        scratch_shapes=list(scratch),
        **({} if out_specs is None else {"out_specs": out_specs}),
    )

    def run(*args):
        args = args[:smem] + tuple(pltpu.with_memory_space_constraint(x, pltpu.VMEM) for x in args[smem:])
        return body(*args)

    return run


def f32(*shape):
    return jax.ShapeDtypeStruct(shape, jnp.float32)


def near(*shape):
    return pltpu.VMEM(shape, jnp.float32)


def exchange(x, axes):
    count, width = x.shape
    moved = lax.all_to_all(x.reshape(count, 1, width), axes, split_axis=0, concat_axis=0, tiled=True)
    return moved.reshape(count, width)


def local(samples, point_count, corr_scan, corr_tile, corr_src):
    devices = lax.axis_size(AXES)
    groups = lax.axis_size("grp")
    samples = samples.transpose(0, 2, 1, 3)
    scan_local, tiles, per_scan, entries, cap, block = sizes(samples.shape, corr_scan.shape, devices)
    slots = devices * cap
    scan_total = scan_local * (devices // groups)
    columns, pack, per_block = layout(scan_local, groups, scan_total)
    group = lax.axis_index("grp").astype(jnp.int32).reshape(1)
    scan = lax.axis_index("scan").astype(jnp.int32).reshape(1)
    back_rows = back_layout(scan_local, groups, cap)[-1]

    def bind(kernel, *args):
        return lambda *refs: kernel(*args, *refs)

    sent, samples = pl.pallas_call(
        bind(send_kernel, devices, groups),
        out_shape=(near(devices * block, LANES), near(*samples.shape)),
        in_specs=[pl.BlockSpec(memory_space=pltpu.SMEM)] * 2 + [pl.BlockSpec(memory_space=pl.ANY)] * 5,
        scratch_shapes=[
            pltpu.SMEM(point_count.shape, jnp.int32),
            pltpu.VMEM(corr_scan.shape, jnp.int32),
            pltpu.VMEM(corr_tile.shape, jnp.int32),
            pltpu.VMEM(corr_src.shape, jnp.int32),
            pltpu.VMEM((COORDS, entries, LANES), jnp.float32),
            pltpu.SemaphoreType.DMA((5,)),
        ],
    )(scan, group, point_count, samples, corr_scan, corr_tile, corr_src)
    received = exchange(sent, AXES)
    flat, back = call(
        bind(pair_kernel, devices, groups),
        (near(WIDTH, slots), f32(devices * back_rows, LANES)),
        1,
        2,
        [
            pltpu.VMEM((devices * back_rows, LANES), jnp.float32),
            pltpu.VMEM((COORDS, LANES, slots), jnp.float32),
            pltpu.VMEM((FIELDS, LANES, slots), jnp.float32),
            pltpu.VMEM((devices, LANES), jnp.float32),
            pltpu.SemaphoreType.DMA((slots // LANES,)),
        ],
        (pl.BlockSpec(memory_space=pltpu.VMEM), pl.BlockSpec(memory_space=pl.ANY)),
    )(scan, samples, received)
    back = exchange(back, AXES)
    share = near(per_block * scan_local, LANES)
    shares = call(
        bind(held_kernel, devices, groups, scan_local),
        (share,) * groups,
        2,
        1,
        [pltpu.VMEM((groups,) + share.shape, jnp.float32)],
    )(scan, group, flat)
    shares = [shares[0]] + [
        lax.ppermute(shares[k], "grp", [(g, partner(g, k, groups)) for g in range(groups)]) for k in range(1, groups)
    ]
    hess, grad = call(
        bind(close_kernel, devices, groups, cap),
        (f32(FIELDS * FIELDS, scan_local, columns), f32(scan_local // groups, FIELDS)),
        2,
        1 + groups,
        [
            pltpu.VMEM((HEAD, (devices // groups) * groups * cap), jnp.float32),
            pltpu.VMEM((scan_local, LANES), jnp.float32),
        ],
    )(scan, group, back, *shares)
    return hess.reshape(FIELDS, FIELDS, scan_local, columns).transpose(2, 0, 1, 3), grad


def solution(mesh):
    placed = (
        P("scan", "grp", None, None),
        P("scan"),
        P("scan", "grp"),
        P("scan", "grp"),
        P("scan", "grp", None),
    )
    return jax.shard_map(
        local,
        mesh=mesh,
        in_specs=placed,
        out_specs=(P("scan", None, None, "grp"), P(AXES, None)),
        check_vma=False,
    )
```

```python
import jax
import jax.numpy as jnp
from jax import lax
from jax.experimental import pallas as pl
from jax.experimental.pallas import tpu as pltpu
from jax.sharding import PartitionSpec as P

LANES = 128
COORDS = 3
FIELDS = 6
PAIRS = [(i, j) for i in range(FIELDS) for j in range(i, FIELDS)]
MAT = len(PAIRS)
ROW_FLAG = MAT
ROW_MATE = MAT + 1
HEAD = MAT + 3
WIDTH = 32
FAR = 2.0**100
BOTH_LANES = (((1,), (1,)), ((), ()))
AXES = ("scan", "grp")


def div(x, n):
    if n & (n - 1) == 0:
        return lax.shift_right_logical(x, jnp.int32(n.bit_length() - 1))
    return x // n


def mod(x, n):
    if n & (n - 1) == 0:
        return x & (n - 1)
    return x % n


def iota(shape, dim):
    return lax.broadcasted_iota(jnp.int32, shape, dim)


def pieces(x, count):
    parts = []
    for _ in range(count - 1):
        part = x.astype(jnp.bfloat16)
        parts.append(part)
        x = x - part.astype(jnp.float32)
    parts.append(x.astype(jnp.bfloat16))
    return parts


def dot(a, b, dims=(((1,), (0,)), ((), ()))):
    return lax.dot_general(a, b, dims, preferred_element_type=jnp.float32)


def sizes(samples_shape, entries_shape, devices):
    scan_local, _, tiles, _ = samples_shape
    per_scan = entries_shape[1]
    entries = scan_local * per_scan
    cap = 2 * entries // devices
    return scan_local, tiles, per_scan, entries, cap, COORDS * cap + 1


def send_kernel(
    devices,
    groups,
    count_hbm,
    samples_hbm,
    scan_hbm,
    tile_hbm,
    src_hbm,
    out_ref,
    samples_ref,
    count_ref,
    scan_ref,
    tile_ref,
    src_ref,
    data_ref,
    sems,
):
    scan_local, tiles, per_scan, entries, cap, block = sizes(samples_ref.shape, scan_ref.shape, devices)
    group_points = tiles * LANES
    pairs = (
        (scan_hbm, scan_ref),
        (tile_hbm, tile_ref),
        (count_hbm, count_ref),
        (src_hbm, src_ref),
        (samples_hbm, samples_ref),
    )
    loads = [pltpu.make_async_copy(far, here, sems.at[k]) for k, (far, here) in enumerate(pairs)]
    for load in loads:
        load.start()
    for load in loads[:2]:
        load.wait()

    scans = scan_ref[...]
    tile_ids = tile_ref[...]
    device = div(scans, scan_local) * groups + div(tile_ids, tiles)
    stacked = jnp.concatenate(
        [device.astype(jnp.float32), mod(scans, scan_local).astype(jnp.float32), mod(tile_ids, tiles).astype(jnp.float32)],
        axis=0,
    ).astype(jnp.bfloat16)
    spread = (mod(iota((per_scan, entries), 1), per_scan) == iota((per_scan, entries), 0)).astype(jnp.float32)
    wide = dot(stacked, spread.astype(jnp.bfloat16))
    own = div(iota((scan_local, entries), 1), per_scan) == iota((scan_local, entries), 0)
    device_row, mate_row, tile_row = [
        jnp.sum(jnp.where(own, wide[f * scan_local : (f + 1) * scan_local], 0.0), axis=0, keepdims=True)
        for f in range(3)
    ]
    rank_parts = []
    columns = []
    for h in range(entries // LANES):
        across = device_row[:, h * LANES : (h + 1) * LANES]
        columns.append(jnp.broadcast_to(across, (LANES, LANES)).T)
        total = jnp.zeros((1, LANES), jnp.float32)
        for g in range(h + 1):
            same = columns[g] == across
            if g == h:
                same = same & (iota((LANES, LANES), 0) < iota((LANES, LANES), 1))
            total = total + jnp.sum(same.astype(jnp.float32), axis=0, keepdims=True)
        rank_parts.append(total)
    rank_row = jnp.concatenate(rank_parts, axis=1)
    slot_row = (device_row * cap + rank_row).astype(jnp.int32)
    place = (iota((devices * cap, entries), 0) == slot_row).astype(jnp.float32).astype(jnp.bfloat16)
    owner_row = (div(iota((1, entries), 1), per_scan) + 1).astype(jnp.float32)
    field = div(iota((LANES, entries), 0), cap)
    picked = jnp.where(field == 0, owner_row, jnp.where(field == 1, mate_row, tile_row))
    picked = jnp.where(
        (mod(iota((LANES, entries), 0), cap).astype(jnp.float32) == rank_row) & (field < 3), picked, 0.0
    ).astype(jnp.bfloat16)
    towards = (iota((devices, entries), 0).astype(jnp.float32) == device_row).astype(jnp.float32).astype(jnp.bfloat16)
    notes = dot(towards, picked, BOTH_LANES)
    for d in range(devices):
        out_ref[pl.ds(d * block + COORDS * cap, 1), :] = notes[d : d + 1]

    for load in loads[2:]:
        load.wait()

    def one_scan(s, carry):
        limit = count_ref[s] - lax.axis_index("grp") * group_points
        for h in range(per_scan // 8):
            ids = src_ref[s, pl.ds(h * 8, 8), :]
            lane = mod(ids, LANES)
            tile = div(ids, LANES)
            found = [jnp.zeros((8, LANES), jnp.float32) for _ in range(COORDS)]
            for t in range(tiles):
                here = tile == t
                for a in range(COORDS):
                    row = jnp.broadcast_to(samples_ref[s, a, t : t + 1, :], (8, LANES))
                    found[a] = jnp.where(here, jnp.take_along_axis(row, lane, axis=1), found[a])
            found[0] = jnp.where(ids < limit, found[0], FAR)
            at = pl.multiple_of(s * per_scan + h * 8, 8)
            for a in range(COORDS):
                data_ref[a, pl.ds(at, 8), :] = found[a]
        present = iota((tiles, LANES), 0) * LANES + iota((tiles, LANES), 1) < limit
        for a in range(COORDS, FIELDS):
            samples_ref[s, a] = jnp.where(present, samples_ref[s, a], 0.0)
        return carry

    lax.fori_loop(0, scan_local, one_scan, 0, unroll=8)

    thirds = [jnp.concatenate(part, axis=1) for part in zip(*[pieces(data_ref[a], 3) for a in range(COORDS)])]
    moved = dot(jnp.concatenate([place] * 3, axis=1), jnp.concatenate(thirds, axis=0))
    for a in range(COORDS):
        for d in range(devices):
            out_ref[pl.ds(d * block + a * cap, cap), :] = moved[d * cap : (d + 1) * cap, a * LANES : (a + 1) * LANES]


def turn(x, amount):
    amount = amount % LANES
    return pltpu.roll(x, amount, 1) if amount else x


def back_layout(scan_local, groups, cap):
    span = groups * cap
    slot_rows = HEAD * span // LANES
    sum_rows = WIDTH * scan_local // LANES
    if FIELDS * (scan_local // groups) <= span:
        turns, grad_row = divmod(HEAD - 1, slot_rows)
        grad_lane, used = turns * span, slot_rows
    else:
        grad_row, grad_lane, used = slot_rows, 0, slot_rows + 1
    return span, slot_rows, sum_rows, grad_row, grad_lane, max(used, sum_rows)


def partner(index, k, groups):
    return index ^ k if groups & (groups - 1) == 0 else (index + k) % groups


def pair_kernel(devices, groups, samples_ref, recv_ref, flat_ref, back_hbm, back_ref, point_ref, mate_ref, note_ref, sems):
    scan_local, _, tiles, _ = samples_ref.shape
    slots = flat_ref.shape[1]
    cap = slots // devices
    block = COORDS * cap + 1
    scans = devices // groups
    for d in range(devices):
        note_ref[pl.ds(d, 1), :] = recv_ref[pl.ds(d * block + COORDS * cap, 1), :]
    notes = note_ref[...].astype(jnp.bfloat16)
    mine = div(iota((devices, slots), 1), cap) == iota((devices, slots), 0)
    rows = []
    for f in range(3):
        spread = (iota((LANES, slots), 0) == mod(iota((LANES, slots), 1), cap) + f * cap).astype(jnp.float32)
        rows.append(
            jnp.sum(jnp.where(mine, dot(notes, spread.astype(jnp.bfloat16)), 0.0), axis=0, keepdims=True)
        )
    flag_row, mate_row, tile_row = rows
    code_row = (mate_row * tiles + tile_row).astype(jnp.int32)
    table = scan_local * tiles
    chosen = (iota((table, slots), 0) == code_row).astype(jnp.float32).astype(jnp.bfloat16)
    for a in range(FIELDS):
        values = jnp.concatenate([samples_ref[b, a] for b in range(scan_local)], axis=0)
        turned = jnp.concatenate([values[h : h + LANES].T for h in range(0, table, LANES)], axis=1)
        parts = [dot(part, chosen) for part in pieces(turned, 3)]
        mate_ref[a] = (parts[0] + parts[1]) + parts[2]
    per_chunk = LANES // cap
    for c in range(slots // LANES):
        for a in range(COORDS):
            stack = [
                recv_ref[pl.ds(d * block + a * cap, cap), :] for d in range(c * per_chunk, (c + 1) * per_chunk)
            ]
            point_ref[a, :, c * LANES : (c + 1) * LANES] = jnp.concatenate(stack, axis=0).T
    span, slot_rows, sum_rows, grad_row, grad_lane, rows = back_layout(scan_local, groups, cap)
    near_group = div(lax.axis_index("scan") * scan_local, scans * scan_local // groups)
    share = scan_local // groups
    slot_lane = div(iota((slot_rows, LANES), 1), span)
    sum_lane = div(iota((sum_rows, LANES), 1), scan_local)
    grad_spot = (iota((slot_rows, LANES), 0) == grad_row) & (iota((slot_rows, LANES), 1) >= grad_lane)
    peer = div(iota((1, LANES), 1), span)
    per_line = LANES // span
    stores = []
    for c in range(slots // LANES):
        lanes = slice(c * LANES, (c + 1) * LANES)

        def step(k, sums):
            at = pl.ds(pl.multiple_of(k * 8, 8), 8)
            px, py, pz = [point_ref[a, at, lanes] for a in range(COORDS)]
            present = px < FAR
            px = jnp.where(present, px, 0.0)
            qx, qy, qz, nx, ny, nz = [mate_ref[a, at, lanes] for a in range(FIELDS)]
            residual = nx * (px - qx) + ny * (py - qy) + nz * (pz - qz)
            weight = jnp.where(present, 1.0 / (1.0 + residual * residual), 0.0)
            jac = [py * nz - pz * ny, pz * nx - px * nz, px * ny - py * nx, nx, ny, nz]
            scaled = [weight * j for j in jac]
            terms = [scaled[i] * jac[j] for i, j in PAIRS] + [residual * s for s in scaled]
            return tuple(s + t for s, t in zip(sums, terms))

        zero = jnp.zeros((8, LANES), jnp.float32)
        sums = lax.fori_loop(0, LANES // 8, step, (zero,) * (MAT + FIELDS), unroll=16)
        filled = flag_row[:, lanes] > 0.0
        lines = [jnp.where(filled, jnp.sum(s, axis=0, keepdims=True), 0.0) for s in sums]
        blank = jnp.zeros((1, LANES), jnp.float32)
        lines[MAT:MAT] = [flag_row[:, lanes], mate_row[:, lanes], blank]
        lines += [blank] * (WIDTH - len(lines))
        flat = jnp.concatenate(lines, axis=0)
        flat_ref[:, lanes] = flat
        member = flag_row[:, lanes].astype(jnp.int32) - 1
        source = jnp.where(member >= 0, peer * scan_local + member, -1)
        source_hot = (iota((LANES, LANES), 0) == source).astype(jnp.float32).astype(jnp.bfloat16)
        totals = dot(
            jnp.concatenate(pieces(flat, 3), axis=1), jnp.concatenate([source_hot] * 3, axis=1), BOTH_LANES
        )
        chosen = jnp.concatenate(
            [jnp.broadcast_to(flat[HEAD + q : HEAD + q + 1, :], (share, LANES)) for q in range(FIELDS)], axis=0
        )
        chosen = jnp.where(member == near_group * share + mod(iota(chosen.shape, 0), share), chosen, 0.0)
        below = jnp.zeros((LANES - grad_lane - FIELDS * share, LANES), jnp.float32)
        above = [jnp.zeros((grad_lane, LANES), jnp.float32)] if grad_lane else []
        chosen = jnp.concatenate(above + [chosen, below], axis=0)
        peer_hot = (iota((8, LANES), 0) == peer).astype(jnp.float32).astype(jnp.bfloat16)
        grads = dot(
            jnp.concatenate([peer_hot] * 3, axis=1), jnp.concatenate(pieces(chosen, 3), axis=1), BOTH_LANES
        )
        for u in range(per_line):
            body = None
            for i in range(per_line):
                piece = turn(flat[i * slot_rows : (i + 1) * slot_rows], (i - u) * span)
                body = piece if i == 0 else jnp.where(slot_lane == i, piece, body)
            if grad_row < slot_rows:
                body = jnp.where(grad_spot, grads[u : u + 1], body)
            else:
                body = jnp.concatenate([body, grads[u : u + 1]], axis=0)
            tail = None
            for i in range(WIDTH // sum_rows):
                piece = turn(totals[i * sum_rows : (i + 1) * sum_rows], (i - u) * scan_local)
                tail = piece if i == 0 else jnp.where(sum_lane == i, piece, tail)
            for g in range(groups):
                at = ((c * per_line + u) * groups + g) * rows
                back_ref[at : at + body.shape[0], :] = body
                back_ref[at : at + sum_rows, :] = jnp.where(near_group != g, tail, body[0:sum_rows])
        at = pl.ds(c * per_line * groups * rows, per_line * groups * rows)
        stores.append(pltpu.make_async_copy(back_ref.at[at], back_hbm.at[at], sems.at[c]))
        stores[-1].start()
    for store in stores:
        store.wait()


def layout(scan_local, groups, scan_total):
    columns = scan_total // groups
    pack = max(1, LANES // columns)
    per_block = -(-(MAT + 1) // pack)
    return columns, pack, per_block


def block_rows(every, row_hot, count):
    high = every.astype(jnp.bfloat16).astype(jnp.float32)
    for part in (high, every - high):
        yield jnp.concatenate(
            [jnp.where(row_hot, part[q : q + 1], 0.0).astype(jnp.bfloat16) for q in range(count)], axis=0
        )


def held_kernel(devices, groups, scan_local, flat_ref, *refs):
    out_refs, stage_ref = refs[:-1], refs[-1]
    slots = flat_ref.shape[1]
    cap = slots // devices
    scan_total = scan_local * (devices // groups)
    columns, pack, per_block = layout(scan_local, groups, scan_total)
    every = flat_ref[...]
    row = every[ROW_MATE : ROW_MATE + 1].astype(jnp.int32)
    other = div(div(iota((1, slots), 1), cap), groups) * scan_local + every[ROW_FLAG : ROW_FLAG + 1].astype(jnp.int32) - 1
    own = lax.axis_index("scan") * scan_local + row
    row_hot = iota((scan_local, slots), 0) == row
    column = iota((scan_total, slots), 0)
    mix = ((column == own).astype(jnp.float32) - (column == other).astype(jnp.float32)).astype(jnp.bfloat16)
    hess = sum(dot(rows, mix, BOTH_LANES) for rows in block_rows(every, row_hot, MAT))
    lane = iota((scan_local, LANES), 1)
    home = MAT // per_block
    grad = jnp.zeros((scan_local, LANES), jnp.float32)
    for q in range(FIELDS):
        value = jnp.sum(jnp.where(row_hot, every[HEAD + q : HEAD + q + 1], 0.0), axis=1, keepdims=True)
        grad = jnp.where(lane == home * columns + q, -value, grad)
    for c in range(groups):
        side, shift = divmod(c * columns, LANES)
        for r in range(per_block):
            tile = jnp.zeros((scan_local, LANES), jnp.float32)
            for k in range(pack):
                q = k * per_block + r
                if q < MAT:
                    value = hess[q * scan_local : (q + 1) * scan_local, side * LANES : (side + 1) * LANES]
                    value = turn(value, k * columns - shift)
                elif q == MAT:
                    value = grad
                else:
                    continue
                tile = jnp.where(div(lane, columns) == k, value, tile) if pack > 1 else value
            stage_ref[c, r * scan_local : (r + 1) * scan_local, :] = tile
    for k, out_ref in enumerate(out_refs):
        out_ref[...] = stage_ref[partner(lax.axis_index("grp"), k, groups)]


def close_kernel(devices, groups, cap, back_ref, *refs):
    part_refs, (hess_ref, grad_ref, every_ref, hold_ref) = refs[:groups], refs[groups:]
    scan_local, columns = hess_ref.shape[1:]
    per_block = part_refs[0].shape[0] // scan_local
    span, slot_rows, sum_rows, grad_row, grad_lane, block = back_layout(scan_local, groups, cap)
    senders = devices // groups
    first = lax.axis_index("grp") * (senders * block)
    lane_block = div(iota((slot_rows, LANES), 1), span)
    per_chunk = LANES // span
    for chunk in range(senders // per_chunk):
        found = [back_ref[pl.ds(first + (chunk * per_chunk + u) * block, slot_rows), :] for u in range(per_chunk)]
        for i in range(LANES // span):
            tile = None
            for u in range(per_chunk):
                piece = turn(found[u], (u - i) * span)
                tile = piece if u == 0 else jnp.where(lane_block == u, piece, tile)
            every_ref[i * slot_rows : (i + 1) * slot_rows, chunk * LANES : (chunk + 1) * LANES] = tile
    every = every_ref[...]
    total = every.shape[1]
    row = every[ROW_FLAG : ROW_FLAG + 1].astype(jnp.int32) - 1
    mate = every[ROW_MATE : ROW_MATE + 1].astype(jnp.int32)
    column = div(div(iota((1, total), 1), span), groups) * scan_local + mate
    row_hot = iota((scan_local, total), 0) == row
    offset = lax.axis_index("scan") * scan_local - lax.axis_index("grp") * columns
    line = iota((columns, total), 0)
    mix = (line == row + offset).astype(jnp.float32) - (line == column).astype(jnp.float32)
    mix = mix.astype(jnp.bfloat16)
    rows = jnp.concatenate(list(block_rows(every, row_hot, MAT)), axis=1)
    cross = dot(rows, jnp.concatenate([mix, mix], axis=1), BOTH_LANES)
    sums = jnp.zeros((sum_rows, LANES), jnp.float32)
    for c in range(groups):
        part = back_ref[c * senders * block : c * senders * block + sum_rows, :]
        for d in range(c * senders + 1, (c + 1) * senders):
            part = part + back_ref[d * block : d * block + sum_rows, :]
        sums = sums + jnp.where(lax.axis_index("grp") != c, part, 0.0)
    near = back_ref[pl.ds(first + grad_row, 1), :]
    for u in range(1, senders):
        near = near + back_ref[pl.ds(first + u * block + grad_row, 1), :]
    line = iota((scan_local, LANES), 0)
    lane = iota((scan_local, LANES), 1)

    def by_row(q):
        i, r = divmod(q, sum_rows)
        return jnp.sum(jnp.where(lane == line + i * scan_local, sums[r : r + 1], 0.0), axis=1, keepdims=True)

    whole = part_refs[0][...]
    for part_ref in part_refs[1:]:
        whole = whole + part_ref[...]
    diagonal = iota((scan_local, columns), 1) == iota((scan_local, columns), 0) + offset
    shifted = pltpu.roll(sums, mod(offset + LANES * (devices // groups), LANES), 1)
    facing = [turn(shifted, -n * scan_local) for n in range(WIDTH // sum_rows)]
    for q in range(MAT):
        k, r = divmod(q, per_block)
        tile = whole[r * scan_local : (r + 1) * scan_local, k * columns : (k + 1) * columns]
        tile = tile + cross[q * scan_local : (q + 1) * scan_local]
        n, r = divmod(q, sum_rows)
        tile = tile + jnp.where(diagonal, facing[n][r : r + 1, 0:columns], 0.0)
        i, j = PAIRS[q]
        hess_ref[i * FIELDS + j] = tile
        if i != j:
            hess_ref[j * FIELDS + i] = tile
    k, r = divmod(MAT, per_block)
    grad = turn(whole[r * scan_local : (r + 1) * scan_local], -k * columns)
    for q in range(FIELDS):
        grad = grad + jnp.where(lane == q, by_row(HEAD + q), 0.0)
    hold_ref[...] = grad
    part = scan_local // groups
    own = jnp.zeros((part, LANES), jnp.float32)
    for q in range(FIELDS):
        spot = grad_lane + q * part + iota((part, LANES), 0) == iota((part, LANES), 1)
        value = jnp.sum(jnp.where(spot, near, 0.0), axis=1, keepdims=True)
        own = jnp.where(iota((part, LANES), 1) == q, value, own)
    hold = hold_ref[pl.ds(lax.axis_index("grp") * part, part), :] + own
    grad_ref[...] = hold[:, 0:FIELDS]


def call(kernel, out_shape, smem, vmem, scratch=(), out_specs=None):
    body = pl.pallas_call(
        kernel,
        out_shape=out_shape,
        in_specs=[pl.BlockSpec(memory_space=pltpu.SMEM)] * smem + [pl.BlockSpec(memory_space=pltpu.VMEM)] * vmem,
        scratch_shapes=list(scratch),
        **({} if out_specs is None else {"out_specs": out_specs}),
    )

    def run(*args):
        args = args[:smem] + tuple(pltpu.with_memory_space_constraint(x, pltpu.VMEM) for x in args[smem:])
        return body(*args)

    return run


def f32(*shape):
    return jax.ShapeDtypeStruct(shape, jnp.float32)


def near(*shape):
    return pltpu.VMEM(shape, jnp.float32)


def exchange(x, axes):
    count, width = x.shape
    moved = lax.all_to_all(x.reshape(count, 1, width), axes, split_axis=0, concat_axis=0, tiled=True)
    return moved.reshape(count, width)


def local(samples, point_count, corr_scan, corr_tile, corr_src):
    devices = lax.axis_size(AXES)
    groups = lax.axis_size("grp")
    samples = samples.transpose(0, 2, 1, 3)
    scan_local, tiles, per_scan, entries, cap, block = sizes(samples.shape, corr_scan.shape, devices)
    slots = devices * cap
    scan_total = scan_local * (devices // groups)
    columns, pack, per_block = layout(scan_local, groups, scan_total)
    back_rows = back_layout(scan_local, groups, cap)[-1]

    def bind(kernel, *args):
        return lambda *refs: kernel(*args, *refs)

    sent, samples = pl.pallas_call(
        bind(send_kernel, devices, groups),
        out_shape=(near(devices * block, LANES), near(*samples.shape)),
        in_specs=[pl.BlockSpec(memory_space=pl.ANY)] * 5,
        scratch_shapes=[
            pltpu.SMEM(point_count.shape, jnp.int32),
            pltpu.VMEM(corr_scan.shape, jnp.int32),
            pltpu.VMEM(corr_tile.shape, jnp.int32),
            pltpu.VMEM(corr_src.shape, jnp.int32),
            pltpu.VMEM((COORDS, entries, LANES), jnp.float32),
            pltpu.SemaphoreType.DMA((5,)),
        ],
    )(point_count, samples, corr_scan, corr_tile, corr_src)
    received = exchange(sent, AXES)
    flat, back = call(
        bind(pair_kernel, devices, groups),
        (near(WIDTH, slots), f32(devices * back_rows, LANES)),
        0,
        2,
        [
            pltpu.VMEM((devices * back_rows, LANES), jnp.float32),
            pltpu.VMEM((COORDS, LANES, slots), jnp.float32),
            pltpu.VMEM((FIELDS, LANES, slots), jnp.float32),
            pltpu.VMEM((devices, LANES), jnp.float32),
            pltpu.SemaphoreType.DMA((slots // LANES,)),
        ],
        (pl.BlockSpec(memory_space=pltpu.VMEM), pl.BlockSpec(memory_space=pl.ANY)),
    )(samples, received)
    back = exchange(back, AXES)
    share = near(per_block * scan_local, LANES)
    shares = call(
        bind(held_kernel, devices, groups, scan_local),
        (share,) * groups,
        0,
        1,
        [pltpu.VMEM((groups,) + share.shape, jnp.float32)],
    )(flat)
    shares = [shares[0]] + [
        lax.ppermute(shares[k], "grp", [(g, partner(g, k, groups)) for g in range(groups)]) for k in range(1, groups)
    ]
    hess, grad = call(
        bind(close_kernel, devices, groups, cap),
        (f32(FIELDS * FIELDS, scan_local, columns), f32(scan_local // groups, FIELDS)),
        0,
        1 + groups,
        [
            pltpu.VMEM((HEAD, (devices // groups) * groups * cap), jnp.float32),
            pltpu.VMEM((scan_local, LANES), jnp.float32),
        ],
    )(back, *shares)
    return hess.reshape(FIELDS, FIELDS, scan_local, columns).transpose(2, 0, 1, 3), grad


def solution(mesh):
    placed = (
        P("scan", "grp", None, None),
        P("scan"),
        P("scan", "grp"),
        P("scan", "grp"),
        P("scan", "grp", None),
    )
    return jax.shard_map(
        local,
        mesh=mesh,
        in_specs=placed,
        out_specs=(P("scan", None, None, "grp"), P(AXES, None)),
        check_vma=False,
    )
```

```python
import jax
import jax.numpy as jnp
from jax import lax
from jax.experimental import pallas as pl
from jax.experimental.pallas import tpu as pltpu
from jax.sharding import PartitionSpec as P

LANES = 128
COORDS = 3
FIELDS = 6
PAIRS = [(i, j) for i in range(FIELDS) for j in range(i, FIELDS)]
MAT = len(PAIRS)
ROW_FLAG = MAT
ROW_MATE = MAT + 1
HEAD = MAT + 3
WIDTH = 32
SENT = COORDS + 1
BOTH_LANES = (((1,), (1,)), ((), ()))
AXES = ("scan", "grp")


def div(x, n):
    if n & (n - 1) == 0:
        return lax.shift_right_logical(x, jnp.int32(n.bit_length() - 1))
    return x // n


def mod(x, n):
    if n & (n - 1) == 0:
        return x & (n - 1)
    return x % n


def iota(shape, dim):
    return lax.broadcasted_iota(jnp.int32, shape, dim)


def pieces(x, count):
    parts = []
    for _ in range(count - 1):
        part = x.astype(jnp.bfloat16)
        parts.append(part)
        x = x - part.astype(jnp.float32)
    parts.append(x.astype(jnp.bfloat16))
    return parts


def dot(a, b, dims=(((1,), (0,)), ((), ()))):
    return lax.dot_general(a, b, dims, preferred_element_type=jnp.float32)


def sizes(samples_shape, entries_shape, devices):
    scan_local, _, tiles, _ = samples_shape
    per_scan = entries_shape[1]
    entries = scan_local * per_scan
    cap = 2 * entries // devices
    return scan_local, tiles, per_scan, entries, cap, SENT * cap + 1


def send_kernel(
    devices,
    groups,
    count_hbm,
    samples_hbm,
    scan_hbm,
    tile_hbm,
    src_hbm,
    out_ref,
    samples_ref,
    count_ref,
    scan_ref,
    tile_ref,
    src_ref,
    data_ref,
    sems,
):
    scan_local, tiles, per_scan, entries, cap, block = sizes(samples_ref.shape, scan_ref.shape, devices)
    group_points = tiles * LANES
    pairs = (
        (scan_hbm, scan_ref),
        (tile_hbm, tile_ref),
        (count_hbm, count_ref),
        (src_hbm, src_ref),
        (samples_hbm, samples_ref),
    )
    loads = [pltpu.make_async_copy(far, here, sems.at[k]) for k, (far, here) in enumerate(pairs)]
    for load in loads:
        load.start()
    for load in loads[:2]:
        load.wait()

    scans = scan_ref[...]
    tile_ids = tile_ref[...]
    device = div(scans, scan_local) * groups + div(tile_ids, tiles)
    stacked = jnp.concatenate(
        [device.astype(jnp.float32), mod(scans, scan_local).astype(jnp.float32), mod(tile_ids, tiles).astype(jnp.float32)],
        axis=0,
    ).astype(jnp.bfloat16)
    spread = (mod(iota((per_scan, entries), 1), per_scan) == iota((per_scan, entries), 0)).astype(jnp.float32)
    wide = dot(stacked, spread.astype(jnp.bfloat16))
    own = div(iota((scan_local, entries), 1), per_scan) == iota((scan_local, entries), 0)
    device_row, mate_row, tile_row = [
        jnp.sum(jnp.where(own, wide[f * scan_local : (f + 1) * scan_local], 0.0), axis=0, keepdims=True)
        for f in range(3)
    ]
    rank_parts = []
    columns = []
    for h in range(entries // LANES):
        across = device_row[:, h * LANES : (h + 1) * LANES]
        columns.append(jnp.broadcast_to(across, (LANES, LANES)).T)
        total = jnp.zeros((1, LANES), jnp.float32)
        for g in range(h + 1):
            same = columns[g] == across
            if g == h:
                same = same & (iota((LANES, LANES), 0) < iota((LANES, LANES), 1))
            total = total + jnp.sum(same.astype(jnp.float32), axis=0, keepdims=True)
        rank_parts.append(total)
    rank_row = jnp.concatenate(rank_parts, axis=1)
    slot_row = (device_row * cap + rank_row).astype(jnp.int32)
    place = (iota((devices * cap, entries), 0) == slot_row).astype(jnp.float32).astype(jnp.bfloat16)
    owner_row = (div(iota((1, entries), 1), per_scan) + 1).astype(jnp.float32)
    field = div(iota((LANES, entries), 0), cap)
    picked = jnp.where(field == 0, owner_row, jnp.where(field == 1, mate_row, tile_row))
    picked = jnp.where(
        (mod(iota((LANES, entries), 0), cap).astype(jnp.float32) == rank_row) & (field < 3), picked, 0.0
    ).astype(jnp.bfloat16)
    towards = (iota((devices, entries), 0).astype(jnp.float32) == device_row).astype(jnp.float32).astype(jnp.bfloat16)
    notes = dot(towards, picked, BOTH_LANES)
    for d in range(devices):
        out_ref[pl.ds(d * block + SENT * cap, 1), :] = notes[d : d + 1]

    for load in loads[2:]:
        load.wait()

    def one_scan(s, carry):
        limit = count_ref[s] - lax.axis_index("grp") * group_points
        for h in range(per_scan // 8):
            ids = src_ref[s, pl.ds(h * 8, 8), :]
            lane = mod(ids, LANES)
            tile = div(ids, LANES)
            found = [jnp.zeros((8, LANES), jnp.float32) for _ in range(COORDS)]
            for t in range(tiles):
                here = tile == t
                for a in range(COORDS):
                    row = jnp.broadcast_to(samples_ref[s, a, t : t + 1, :], (8, LANES))
                    found[a] = jnp.where(here, jnp.take_along_axis(row, lane, axis=1), found[a])
            found.append((ids < limit).astype(jnp.float32))
            at = pl.multiple_of(s * per_scan + h * 8, 8)
            for a in range(SENT):
                data_ref[a, pl.ds(at, 8), :] = found[a]
        present = iota((tiles, LANES), 0) * LANES + iota((tiles, LANES), 1) < limit
        for a in range(COORDS, FIELDS):
            samples_ref[s, a] = jnp.where(present, samples_ref[s, a], 0.0)
        return carry

    lax.fori_loop(0, scan_local, one_scan, 0, unroll=8)

    thirds = [jnp.concatenate(part, axis=1) for part in zip(*[pieces(data_ref[a], 3) for a in range(SENT)])]
    moved = dot(jnp.concatenate([place] * 3, axis=1), jnp.concatenate(thirds, axis=0))
    for a in range(SENT):
        for d in range(devices):
            out_ref[pl.ds(d * block + a * cap, cap), :] = moved[d * cap : (d + 1) * cap, a * LANES : (a + 1) * LANES]


def turn(x, amount):
    amount = amount % LANES
    return pltpu.roll(x, amount, 1) if amount else x


def back_layout(scan_local, groups, cap):
    span = groups * cap
    slot_rows = HEAD * span // LANES
    sum_rows = WIDTH * scan_local // LANES
    if FIELDS * (scan_local // groups) <= span:
        turns, grad_row = divmod(HEAD - 1, slot_rows)
        grad_lane, used = turns * span, slot_rows
    else:
        grad_row, grad_lane, used = slot_rows, 0, slot_rows + 1
    return span, slot_rows, sum_rows, grad_row, grad_lane, max(used, sum_rows)


def partner(index, k, groups):
    return index ^ k if groups & (groups - 1) == 0 else (index + k) % groups


def pair_kernel(devices, groups, samples_ref, recv_ref, flat_ref, back_hbm, back_ref, point_ref, mate_ref, note_ref, sems):
    scan_local, _, tiles, _ = samples_ref.shape
    slots = flat_ref.shape[1]
    cap = slots // devices
    block = SENT * cap + 1
    scans = devices // groups
    for d in range(devices):
        note_ref[pl.ds(d, 1), :] = recv_ref[pl.ds(d * block + SENT * cap, 1), :]
    notes = note_ref[...].astype(jnp.bfloat16)
    mine = div(iota((devices, slots), 1), cap) == iota((devices, slots), 0)
    rows = []
    for f in range(3):
        spread = (iota((LANES, slots), 0) == mod(iota((LANES, slots), 1), cap) + f * cap).astype(jnp.float32)
        rows.append(
            jnp.sum(jnp.where(mine, dot(notes, spread.astype(jnp.bfloat16)), 0.0), axis=0, keepdims=True)
        )
    flag_row, mate_row, tile_row = rows
    code_row = (mate_row * tiles + tile_row).astype(jnp.int32)
    table = scan_local * tiles
    chosen = (iota((table, slots), 0) == code_row).astype(jnp.float32).astype(jnp.bfloat16)
    for a in range(FIELDS):
        values = jnp.concatenate([samples_ref[b, a] for b in range(scan_local)], axis=0)
        turned = jnp.concatenate([values[h : h + LANES].T for h in range(0, table, LANES)], axis=1)
        parts = [dot(part, chosen) for part in pieces(turned, 3)]
        mate_ref[a] = (parts[0] + parts[1]) + parts[2]
    per_chunk = LANES // cap
    for c in range(slots // LANES):
        for a in range(SENT):
            stack = [
                recv_ref[pl.ds(d * block + a * cap, cap), :] for d in range(c * per_chunk, (c + 1) * per_chunk)
            ]
            point_ref[a, :, c * LANES : (c + 1) * LANES] = jnp.concatenate(stack, axis=0).T
    span, slot_rows, sum_rows, grad_row, grad_lane, rows = back_layout(scan_local, groups, cap)
    near_group = div(lax.axis_index("scan") * scan_local, scans * scan_local // groups)
    share = scan_local // groups
    slot_lane = div(iota((slot_rows, LANES), 1), span)
    sum_lane = div(iota((sum_rows, LANES), 1), scan_local)
    grad_spot = (iota((slot_rows, LANES), 0) == grad_row) & (iota((slot_rows, LANES), 1) >= grad_lane)
    peer = div(iota((1, LANES), 1), span)
    per_line = LANES // span
    stores = []
    for c in range(slots // LANES):
        lanes = slice(c * LANES, (c + 1) * LANES)

        def step(k, sums):
            at = pl.ds(pl.multiple_of(k * 8, 8), 8)
            px, py, pz, mask = [point_ref[a, at, lanes] for a in range(SENT)]
            qx, qy, qz, nx, ny, nz = [mate_ref[a, at, lanes] for a in range(FIELDS)]
            residual = nx * (px - qx) + ny * (py - qy) + nz * (pz - qz)
            weight = mask / (1.0 + residual * residual)
            jac = [py * nz - pz * ny, pz * nx - px * nz, px * ny - py * nx, nx, ny, nz]
            scaled = [weight * j for j in jac]
            terms = [scaled[i] * jac[j] for i, j in PAIRS] + [residual * s for s in scaled]
            return tuple(s + t for s, t in zip(sums, terms))

        zero = jnp.zeros((8, LANES), jnp.float32)
        sums = lax.fori_loop(0, LANES // 8, step, (zero,) * (MAT + FIELDS), unroll=16)
        lines = [jnp.sum(s, axis=0, keepdims=True) for s in sums]
        blank = jnp.zeros((1, LANES), jnp.float32)
        lines[MAT:MAT] = [flag_row[:, lanes], mate_row[:, lanes], blank]
        lines += [blank] * (WIDTH - len(lines))
        flat = jnp.concatenate(lines, axis=0)
        flat_ref[:, lanes] = flat
        member = flag_row[:, lanes].astype(jnp.int32) - 1
        source = jnp.where(member >= 0, peer * scan_local + member, -1)
        source_hot = (iota((LANES, LANES), 0) == source).astype(jnp.float32).astype(jnp.bfloat16)
        totals = dot(
            jnp.concatenate(pieces(flat, 3), axis=1), jnp.concatenate([source_hot] * 3, axis=1), BOTH_LANES
        )
        chosen = jnp.concatenate(
            [jnp.broadcast_to(flat[HEAD + q : HEAD + q + 1, :], (share, LANES)) for q in range(FIELDS)], axis=0
        )
        chosen = jnp.where(member == near_group * share + mod(iota(chosen.shape, 0), share), chosen, 0.0)
        below = jnp.zeros((LANES - grad_lane - FIELDS * share, LANES), jnp.float32)
        above = [jnp.zeros((grad_lane, LANES), jnp.float32)] if grad_lane else []
        chosen = jnp.concatenate(above + [chosen, below], axis=0)
        peer_hot = (iota((8, LANES), 0) == peer).astype(jnp.float32).astype(jnp.bfloat16)
        grads = dot(
            jnp.concatenate([peer_hot] * 3, axis=1), jnp.concatenate(pieces(chosen, 3), axis=1), BOTH_LANES
        )
        for u in range(per_line):
            body = None
            for i in range(per_line):
                piece = turn(flat[i * slot_rows : (i + 1) * slot_rows], (i - u) * span)
                body = piece if i == 0 else jnp.where(slot_lane == i, piece, body)
            if grad_row < slot_rows:
                body = jnp.where(grad_spot, grads[u : u + 1], body)
            else:
                body = jnp.concatenate([body, grads[u : u + 1]], axis=0)
            tail = None
            for i in range(WIDTH // sum_rows):
                piece = turn(totals[i * sum_rows : (i + 1) * sum_rows], (i - u) * scan_local)
                tail = piece if i == 0 else jnp.where(sum_lane == i, piece, tail)
            for g in range(groups):
                at = ((c * per_line + u) * groups + g) * rows
                back_ref[at : at + body.shape[0], :] = body
                back_ref[at : at + sum_rows, :] = jnp.where(near_group != g, tail, body[0:sum_rows])
        at = pl.ds(c * per_line * groups * rows, per_line * groups * rows)
        stores.append(pltpu.make_async_copy(back_ref.at[at], back_hbm.at[at], sems.at[c]))
        stores[-1].start()
    for store in stores:
        store.wait()


def layout(scan_local, groups, scan_total):
    columns = scan_total // groups
    pack = max(1, LANES // columns)
    per_block = -(-(MAT + 1) // pack)
    return columns, pack, per_block


def block_rows(every, row_hot, count):
    high = every.astype(jnp.bfloat16).astype(jnp.float32)
    for part in (high, every - high):
        yield jnp.concatenate(
            [jnp.where(row_hot, part[q : q + 1], 0.0).astype(jnp.bfloat16) for q in range(count)], axis=0
        )


def held_kernel(devices, groups, scan_local, flat_ref, *refs):
    out_refs, stage_ref = refs[:-1], refs[-1]
    slots = flat_ref.shape[1]
    cap = slots // devices
    scan_total = scan_local * (devices // groups)
    columns, pack, per_block = layout(scan_local, groups, scan_total)
    every = flat_ref[...]
    row = every[ROW_MATE : ROW_MATE + 1].astype(jnp.int32)
    other = div(div(iota((1, slots), 1), cap), groups) * scan_local + every[ROW_FLAG : ROW_FLAG + 1].astype(jnp.int32) - 1
    own = lax.axis_index("scan") * scan_local + row
    row_hot = iota((scan_local, slots), 0) == row
    column = iota((scan_total, slots), 0)
    mix = ((column == own).astype(jnp.float32) - (column == other).astype(jnp.float32)).astype(jnp.bfloat16)
    hess = sum(dot(rows, mix, BOTH_LANES) for rows in block_rows(every, row_hot, MAT))
    lane = iota((scan_local, LANES), 1)
    home = MAT // per_block
    grad = jnp.zeros((scan_local, LANES), jnp.float32)
    for q in range(FIELDS):
        value = jnp.sum(jnp.where(row_hot, every[HEAD + q : HEAD + q + 1], 0.0), axis=1, keepdims=True)
        grad = jnp.where(lane == home * columns + q, -value, grad)
    for c in range(groups):
        side, shift = divmod(c * columns, LANES)
        for r in range(per_block):
            tile = jnp.zeros((scan_local, LANES), jnp.float32)
            for k in range(pack):
                q = k * per_block + r
                if q < MAT:
                    value = hess[q * scan_local : (q + 1) * scan_local, side * LANES : (side + 1) * LANES]
                    value = turn(value, k * columns - shift)
                elif q == MAT:
                    value = grad
                else:
                    continue
                tile = jnp.where(div(lane, columns) == k, value, tile) if pack > 1 else value
            stage_ref[c, r * scan_local : (r + 1) * scan_local, :] = tile
    for k, out_ref in enumerate(out_refs):
        out_ref[...] = stage_ref[partner(lax.axis_index("grp"), k, groups)]


def close_kernel(devices, groups, cap, back_ref, *refs):
    part_refs, (hess_ref, grad_ref, every_ref, hold_ref) = refs[:groups], refs[groups:]
    scan_local, columns = hess_ref.shape[1:]
    per_block = part_refs[0].shape[0] // scan_local
    span, slot_rows, sum_rows, grad_row, grad_lane, block = back_layout(scan_local, groups, cap)
    senders = devices // groups
    first = lax.axis_index("grp") * (senders * block)
    lane_block = div(iota((slot_rows, LANES), 1), span)
    per_chunk = LANES // span
    for chunk in range(senders // per_chunk):
        found = [back_ref[pl.ds(first + (chunk * per_chunk + u) * block, slot_rows), :] for u in range(per_chunk)]
        for i in range(LANES // span):
            tile = None
            for u in range(per_chunk):
                piece = turn(found[u], (u - i) * span)
                tile = piece if u == 0 else jnp.where(lane_block == u, piece, tile)
            every_ref[i * slot_rows : (i + 1) * slot_rows, chunk * LANES : (chunk + 1) * LANES] = tile
    every = every_ref[...]
    total = every.shape[1]
    row = every[ROW_FLAG : ROW_FLAG + 1].astype(jnp.int32) - 1
    mate = every[ROW_MATE : ROW_MATE + 1].astype(jnp.int32)
    column = div(div(iota((1, total), 1), span), groups) * scan_local + mate
    row_hot = iota((scan_local, total), 0) == row
    offset = lax.axis_index("scan") * scan_local - lax.axis_index("grp") * columns
    line = iota((columns, total), 0)
    mix = (line == row + offset).astype(jnp.float32) - (line == column).astype(jnp.float32)
    mix = mix.astype(jnp.bfloat16)
    rows = jnp.concatenate(list(block_rows(every, row_hot, MAT)), axis=1)
    cross = dot(rows, jnp.concatenate([mix, mix], axis=1), BOTH_LANES)
    sums = jnp.zeros((sum_rows, LANES), jnp.float32)
    for c in range(groups):
        part = back_ref[c * senders * block : c * senders * block + sum_rows, :]
        for d in range(c * senders + 1, (c + 1) * senders):
            part = part + back_ref[d * block : d * block + sum_rows, :]
        sums = sums + jnp.where(lax.axis_index("grp") != c, part, 0.0)
    near = back_ref[pl.ds(first + grad_row, 1), :]
    for u in range(1, senders):
        near = near + back_ref[pl.ds(first + u * block + grad_row, 1), :]
    line = iota((scan_local, LANES), 0)
    lane = iota((scan_local, LANES), 1)

    def by_row(q):
        i, r = divmod(q, sum_rows)
        return jnp.sum(jnp.where(lane == line + i * scan_local, sums[r : r + 1], 0.0), axis=1, keepdims=True)

    whole = part_refs[0][...]
    for part_ref in part_refs[1:]:
        whole = whole + part_ref[...]
    diagonal = iota((scan_local, columns), 1) == iota((scan_local, columns), 0) + offset
    shifted = pltpu.roll(sums, mod(offset + LANES * (devices // groups), LANES), 1)
    facing = [turn(shifted, -n * scan_local) for n in range(WIDTH // sum_rows)]
    for q in range(MAT):
        k, r = divmod(q, per_block)
        tile = whole[r * scan_local : (r + 1) * scan_local, k * columns : (k + 1) * columns]
        tile = tile + cross[q * scan_local : (q + 1) * scan_local]
        n, r = divmod(q, sum_rows)
        tile = tile + jnp.where(diagonal, facing[n][r : r + 1, 0:columns], 0.0)
        i, j = PAIRS[q]
        hess_ref[i * FIELDS + j] = tile
        if i != j:
            hess_ref[j * FIELDS + i] = tile
    k, r = divmod(MAT, per_block)
    grad = turn(whole[r * scan_local : (r + 1) * scan_local], -k * columns)
    for q in range(FIELDS):
        grad = grad + jnp.where(lane == q, by_row(HEAD + q), 0.0)
    hold_ref[...] = grad
    part = scan_local // groups
    own = jnp.zeros((part, LANES), jnp.float32)
    for q in range(FIELDS):
        spot = grad_lane + q * part + iota((part, LANES), 0) == iota((part, LANES), 1)
        value = jnp.sum(jnp.where(spot, near, 0.0), axis=1, keepdims=True)
        own = jnp.where(iota((part, LANES), 1) == q, value, own)
    hold = hold_ref[pl.ds(lax.axis_index("grp") * part, part), :] + own
    grad_ref[...] = hold[:, 0:FIELDS]


def call(kernel, out_shape, smem, vmem, scratch=(), out_specs=None):
    body = pl.pallas_call(
        kernel,
        out_shape=out_shape,
        in_specs=[pl.BlockSpec(memory_space=pltpu.SMEM)] * smem + [pl.BlockSpec(memory_space=pltpu.VMEM)] * vmem,
        scratch_shapes=list(scratch),
        **({} if out_specs is None else {"out_specs": out_specs}),
    )

    def run(*args):
        args = args[:smem] + tuple(pltpu.with_memory_space_constraint(x, pltpu.VMEM) for x in args[smem:])
        return body(*args)

    return run


def f32(*shape):
    return jax.ShapeDtypeStruct(shape, jnp.float32)


def near(*shape):
    return pltpu.VMEM(shape, jnp.float32)


def exchange(x, axes):
    count, width = x.shape
    moved = lax.all_to_all(x.reshape(count, 1, width), axes, split_axis=0, concat_axis=0, tiled=True)
    return moved.reshape(count, width)


def local(samples, point_count, corr_scan, corr_tile, corr_src):
    devices = lax.axis_size(AXES)
    groups = lax.axis_size("grp")
    samples = samples.transpose(0, 2, 1, 3)
    scan_local, tiles, per_scan, entries, cap, block = sizes(samples.shape, corr_scan.shape, devices)
    slots = devices * cap
    scan_total = scan_local * (devices // groups)
    columns, pack, per_block = layout(scan_local, groups, scan_total)
    back_rows = back_layout(scan_local, groups, cap)[-1]

    def bind(kernel, *args):
        return lambda *refs: kernel(*args, *refs)

    sent, samples = pl.pallas_call(
        bind(send_kernel, devices, groups),
        out_shape=(near(devices * block, LANES), near(*samples.shape)),
        in_specs=[pl.BlockSpec(memory_space=pl.ANY)] * 5,
        scratch_shapes=[
            pltpu.SMEM(point_count.shape, jnp.int32),
            pltpu.VMEM(corr_scan.shape, jnp.int32),
            pltpu.VMEM(corr_tile.shape, jnp.int32),
            pltpu.VMEM(corr_src.shape, jnp.int32),
            pltpu.VMEM((SENT, entries, LANES), jnp.float32),
            pltpu.SemaphoreType.DMA((5,)),
        ],
    )(point_count, samples, corr_scan, corr_tile, corr_src)
    received = exchange(sent, AXES)
    flat, back = call(
        bind(pair_kernel, devices, groups),
        (near(WIDTH, slots), f32(devices * back_rows, LANES)),
        0,
        2,
        [
            pltpu.VMEM((devices * back_rows, LANES), jnp.float32),
            pltpu.VMEM((SENT, LANES, slots), jnp.float32),
            pltpu.VMEM((FIELDS, LANES, slots), jnp.float32),
            pltpu.VMEM((devices, LANES), jnp.float32),
            pltpu.SemaphoreType.DMA((slots // LANES,)),
        ],
        (pl.BlockSpec(memory_space=pltpu.VMEM), pl.BlockSpec(memory_space=pl.ANY)),
    )(samples, received)
    back = exchange(back, AXES)
    share = near(per_block * scan_local, LANES)
    shares = call(
        bind(held_kernel, devices, groups, scan_local),
        (share,) * groups,
        0,
        1,
        [pltpu.VMEM((groups,) + share.shape, jnp.float32)],
    )(flat)
    shares = [shares[0]] + [
        lax.ppermute(shares[k], "grp", [(g, partner(g, k, groups)) for g in range(groups)]) for k in range(1, groups)
    ]
    hess, grad = call(
        bind(close_kernel, devices, groups, cap),
        (f32(FIELDS * FIELDS, scan_local, columns), f32(scan_local // groups, FIELDS)),
        0,
        1 + groups,
        [
            pltpu.VMEM((HEAD, (devices // groups) * groups * cap), jnp.float32),
            pltpu.VMEM((scan_local, LANES), jnp.float32),
        ],
    )(back, *shares)
    return hess.reshape(FIELDS, FIELDS, scan_local, columns).transpose(2, 0, 1, 3), grad


def solution(mesh):
    placed = (
        P("scan", "grp", None, None),
        P("scan"),
        P("scan", "grp"),
        P("scan", "grp"),
        P("scan", "grp", None),
    )
    return jax.shard_map(
        local,
        mesh=mesh,
        in_specs=placed,
        out_specs=(P("scan", None, None, "grp"), P(AXES, None)),
        check_vma=False,
    )
```

```python
import jax
import jax.numpy as jnp
from jax import lax
from jax.experimental import pallas as pl
from jax.experimental.pallas import tpu as pltpu
from jax.sharding import PartitionSpec as P

LANES = 128
COORDS = 3
FIELDS = 6
PAIRS = [(i, j) for i in range(FIELDS) for j in range(i, FIELDS)]
MAT = len(PAIRS)
ROW_FLAG = MAT
ROW_MATE = MAT + 1
HEAD = MAT + 3
WIDTH = 32
SENT = COORDS + 1
BOTH_LANES = (((1,), (1,)), ((), ()))
AXES = ("scan", "grp")


def div(x, n):
    if n & (n - 1) == 0:
        return lax.shift_right_logical(x, jnp.int32(n.bit_length() - 1))
    return x // n


def mod(x, n):
    if n & (n - 1) == 0:
        return x & (n - 1)
    return x % n


def iota(shape, dim):
    return lax.broadcasted_iota(jnp.int32, shape, dim)


def pieces(x, count):
    parts = []
    for _ in range(count - 1):
        part = x.astype(jnp.bfloat16)
        parts.append(part)
        x = x - part.astype(jnp.float32)
    parts.append(x.astype(jnp.bfloat16))
    return parts


def dot(a, b, dims=(((1,), (0,)), ((), ()))):
    return lax.dot_general(a, b, dims, preferred_element_type=jnp.float32)


def sizes(samples_shape, entries_shape, devices):
    scan_local, _, tiles, _ = samples_shape
    per_scan = entries_shape[1]
    entries = scan_local * per_scan
    cap = 2 * entries // devices
    return scan_local, tiles, per_scan, entries, cap, SENT * cap + 1


def send_kernel(
    devices,
    groups,
    count_hbm,
    samples_hbm,
    scan_hbm,
    tile_hbm,
    src_hbm,
    out_ref,
    samples_ref,
    limit_ref,
    count_ref,
    scan_ref,
    tile_ref,
    src_ref,
    data_ref,
    sems,
):
    scan_local, tiles, per_scan, entries, cap, block = sizes(samples_ref.shape, scan_ref.shape, devices)
    group_points = tiles * LANES
    pairs = (
        (scan_hbm, scan_ref),
        (tile_hbm, tile_ref),
        (count_hbm, count_ref),
        (src_hbm, src_ref),
        (samples_hbm.at[:, 0:COORDS], samples_ref.at[:, 0:COORDS]),
        (samples_hbm.at[:, COORDS:FIELDS], samples_ref.at[:, COORDS:FIELDS]),
    )
    loads = [pltpu.make_async_copy(far, here, sems.at[k]) for k, (far, here) in enumerate(pairs)]
    for load in loads:
        load.start()
    for load in loads[:2]:
        load.wait()

    scans = scan_ref[...]
    tile_ids = tile_ref[...]
    device = div(scans, scan_local) * groups + div(tile_ids, tiles)
    stacked = jnp.concatenate(
        [device.astype(jnp.float32), mod(scans, scan_local).astype(jnp.float32), mod(tile_ids, tiles).astype(jnp.float32)],
        axis=0,
    ).astype(jnp.bfloat16)
    spread = (mod(iota((per_scan, entries), 1), per_scan) == iota((per_scan, entries), 0)).astype(jnp.float32)
    wide = dot(stacked, spread.astype(jnp.bfloat16))
    own = div(iota((scan_local, entries), 1), per_scan) == iota((scan_local, entries), 0)
    device_row, mate_row, tile_row = [
        jnp.sum(jnp.where(own, wide[f * scan_local : (f + 1) * scan_local], 0.0), axis=0, keepdims=True)
        for f in range(3)
    ]
    rank_parts = []
    columns = []
    for h in range(entries // LANES):
        across = device_row[:, h * LANES : (h + 1) * LANES]
        columns.append(jnp.broadcast_to(across, (LANES, LANES)).T)
        total = jnp.zeros((1, LANES), jnp.float32)
        for g in range(h + 1):
            same = columns[g] == across
            if g == h:
                same = same & (iota((LANES, LANES), 0) < iota((LANES, LANES), 1))
            total = total + jnp.sum(same.astype(jnp.float32), axis=0, keepdims=True)
        rank_parts.append(total)
    rank_row = jnp.concatenate(rank_parts, axis=1)
    slot_row = (device_row * cap + rank_row).astype(jnp.int32)
    place = (iota((devices * cap, entries), 0) == slot_row).astype(jnp.float32).astype(jnp.bfloat16)
    owner_row = (div(iota((1, entries), 1), per_scan) + 1).astype(jnp.float32)
    field = div(iota((LANES, entries), 0), cap)
    picked = jnp.where(field == 0, owner_row, jnp.where(field == 1, mate_row, tile_row))
    picked = jnp.where(
        (mod(iota((LANES, entries), 0), cap).astype(jnp.float32) == rank_row) & (field < 3), picked, 0.0
    ).astype(jnp.bfloat16)
    towards = (iota((devices, entries), 0).astype(jnp.float32) == device_row).astype(jnp.float32).astype(jnp.bfloat16)
    notes = dot(towards, picked, BOTH_LANES)
    for d in range(devices):
        out_ref[pl.ds(d * block + SENT * cap, 1), :] = notes[d : d + 1]

    for load in loads[2:-1]:
        load.wait()

    def one_scan(s, carry):
        limit = count_ref[s] - lax.axis_index("grp") * group_points
        for h in range(per_scan // 8):
            ids = src_ref[s, pl.ds(h * 8, 8), :]
            lane = mod(ids, LANES)
            tile = div(ids, LANES)
            found = [jnp.zeros((8, LANES), jnp.float32) for _ in range(COORDS)]
            for t in range(tiles):
                here = tile == t
                for a in range(COORDS):
                    row = jnp.broadcast_to(samples_ref[s, a, t : t + 1, :], (8, LANES))
                    found[a] = jnp.where(here, jnp.take_along_axis(row, lane, axis=1), found[a])
            found.append((ids < limit).astype(jnp.float32))
            at = pl.multiple_of(s * per_scan + h * 8, 8)
            for a in range(SENT):
                data_ref[a, pl.ds(at, 8), :] = found[a]
        limit_ref[pl.ds(s, 1), :] = jnp.full((1, LANES), limit, jnp.int32)
        return carry

    lax.fori_loop(0, scan_local, one_scan, 0, unroll=8)

    thirds = [jnp.concatenate(part, axis=1) for part in zip(*[pieces(data_ref[a], 3) for a in range(SENT)])]
    moved = dot(jnp.concatenate([place] * 3, axis=1), jnp.concatenate(thirds, axis=0))
    for a in range(SENT):
        for d in range(devices):
            out_ref[pl.ds(d * block + a * cap, cap), :] = moved[d * cap : (d + 1) * cap, a * LANES : (a + 1) * LANES]
    loads[-1].wait()


def turn(x, amount):
    amount = amount % LANES
    return pltpu.roll(x, amount, 1) if amount else x


def back_layout(scan_local, groups, cap):
    span = groups * cap
    slot_rows = HEAD * span // LANES
    sum_rows = WIDTH * scan_local // LANES
    if FIELDS * (scan_local // groups) <= span:
        turns, grad_row = divmod(HEAD - 1, slot_rows)
        grad_lane, used = turns * span, slot_rows
    else:
        grad_row, grad_lane, used = slot_rows, 0, slot_rows + 1
    return span, slot_rows, sum_rows, grad_row, grad_lane, max(used, sum_rows)


def partner(index, k, groups):
    return index ^ k if groups & (groups - 1) == 0 else (index + k) % groups


def pair_kernel(devices, groups, limit_ref, samples_ref, recv_ref, flat_ref, back_hbm, back_ref, point_ref, mate_ref, note_ref, sems):
    scan_local, _, tiles, _ = samples_ref.shape
    slots = flat_ref.shape[1]
    cap = slots // devices
    block = SENT * cap + 1
    scans = devices // groups
    for d in range(devices):
        note_ref[pl.ds(d, 1), :] = recv_ref[pl.ds(d * block + SENT * cap, 1), :]
    notes = note_ref[...].astype(jnp.bfloat16)
    mine = div(iota((devices, slots), 1), cap) == iota((devices, slots), 0)
    rows = []
    for f in range(3):
        spread = (iota((LANES, slots), 0) == mod(iota((LANES, slots), 1), cap) + f * cap).astype(jnp.float32)
        rows.append(
            jnp.sum(jnp.where(mine, dot(notes, spread.astype(jnp.bfloat16)), 0.0), axis=0, keepdims=True)
        )
    flag_row, mate_row, tile_row = rows
    code_row = (mate_row * tiles + tile_row).astype(jnp.int32)
    table = scan_local * tiles
    chosen = (iota((table, slots), 0) == code_row).astype(jnp.float32).astype(jnp.bfloat16)
    spot = iota((tiles, LANES), 0) * LANES + iota((tiles, LANES), 1)
    for a in range(FIELDS):
        values = [samples_ref[b, a] for b in range(scan_local)]
        if a >= COORDS:
            values = [jnp.where(spot < limit_ref[b : b + 1, :], value, 0.0) for b, value in enumerate(values)]
        values = jnp.concatenate(values, axis=0)
        turned = jnp.concatenate([values[h : h + LANES].T for h in range(0, table, LANES)], axis=1)
        parts = [dot(part, chosen) for part in pieces(turned, 3)]
        mate_ref[a] = (parts[0] + parts[1]) + parts[2]
    per_chunk = LANES // cap
    for c in range(slots // LANES):
        for a in range(SENT):
            stack = [
                recv_ref[pl.ds(d * block + a * cap, cap), :] for d in range(c * per_chunk, (c + 1) * per_chunk)
            ]
            point_ref[a, :, c * LANES : (c + 1) * LANES] = jnp.concatenate(stack, axis=0).T
    span, slot_rows, sum_rows, grad_row, grad_lane, rows = back_layout(scan_local, groups, cap)
    near_group = div(lax.axis_index("scan") * scan_local, scans * scan_local // groups)
    share = scan_local // groups
    slot_lane = div(iota((slot_rows, LANES), 1), span)
    sum_lane = div(iota((sum_rows, LANES), 1), scan_local)
    grad_spot = (iota((slot_rows, LANES), 0) == grad_row) & (iota((slot_rows, LANES), 1) >= grad_lane)
    peer = div(iota((1, LANES), 1), span)
    per_line = LANES // span
    stores = []
    for c in range(slots // LANES):
        lanes = slice(c * LANES, (c + 1) * LANES)

        def step(k, sums):
            at = pl.ds(pl.multiple_of(k * 8, 8), 8)
            px, py, pz, mask = [point_ref[a, at, lanes] for a in range(SENT)]
            qx, qy, qz, nx, ny, nz = [mate_ref[a, at, lanes] for a in range(FIELDS)]
            residual = nx * (px - qx) + ny * (py - qy) + nz * (pz - qz)
            weight = mask / (1.0 + residual * residual)
            jac = [py * nz - pz * ny, pz * nx - px * nz, px * ny - py * nx, nx, ny, nz]
            scaled = [weight * j for j in jac]
            terms = [scaled[i] * jac[j] for i, j in PAIRS] + [residual * s for s in scaled]
            return tuple(s + t for s, t in zip(sums, terms))

        zero = jnp.zeros((8, LANES), jnp.float32)
        sums = lax.fori_loop(0, LANES // 8, step, (zero,) * (MAT + FIELDS), unroll=16)
        lines = [jnp.sum(s, axis=0, keepdims=True) for s in sums]
        blank = jnp.zeros((1, LANES), jnp.float32)
        lines[MAT:MAT] = [flag_row[:, lanes], mate_row[:, lanes], blank]
        lines += [blank] * (WIDTH - len(lines))
        flat = jnp.concatenate(lines, axis=0)
        flat_ref[:, lanes] = flat
        member = flag_row[:, lanes].astype(jnp.int32) - 1
        source = jnp.where(member >= 0, peer * scan_local + member, -1)
        source_hot = (iota((LANES, LANES), 0) == source).astype(jnp.float32).astype(jnp.bfloat16)
        totals = dot(
            jnp.concatenate(pieces(flat, 3), axis=1), jnp.concatenate([source_hot] * 3, axis=1), BOTH_LANES
        )
        chosen = jnp.concatenate(
            [jnp.broadcast_to(flat[HEAD + q : HEAD + q + 1, :], (share, LANES)) for q in range(FIELDS)], axis=0
        )
        chosen = jnp.where(member == near_group * share + mod(iota(chosen.shape, 0), share), chosen, 0.0)
        below = jnp.zeros((LANES - grad_lane - FIELDS * share, LANES), jnp.float32)
        above = [jnp.zeros((grad_lane, LANES), jnp.float32)] if grad_lane else []
        chosen = jnp.concatenate(above + [chosen, below], axis=0)
        peer_hot = (iota((8, LANES), 0) == peer).astype(jnp.float32).astype(jnp.bfloat16)
        grads = dot(
            jnp.concatenate([peer_hot] * 3, axis=1), jnp.concatenate(pieces(chosen, 3), axis=1), BOTH_LANES
        )
        for u in range(per_line):
            body = None
            for i in range(per_line):
                piece = turn(flat[i * slot_rows : (i + 1) * slot_rows], (i - u) * span)
                body = piece if i == 0 else jnp.where(slot_lane == i, piece, body)
            if grad_row < slot_rows:
                body = jnp.where(grad_spot, grads[u : u + 1], body)
            else:
                body = jnp.concatenate([body, grads[u : u + 1]], axis=0)
            tail = None
            for i in range(WIDTH // sum_rows):
                piece = turn(totals[i * sum_rows : (i + 1) * sum_rows], (i - u) * scan_local)
                tail = piece if i == 0 else jnp.where(sum_lane == i, piece, tail)
            for g in range(groups):
                at = ((c * per_line + u) * groups + g) * rows
                back_ref[at : at + body.shape[0], :] = body
                back_ref[at : at + sum_rows, :] = jnp.where(near_group != g, tail, body[0:sum_rows])
        at = pl.ds(c * per_line * groups * rows, per_line * groups * rows)
        stores.append(pltpu.make_async_copy(back_ref.at[at], back_hbm.at[at], sems.at[c]))
        stores[-1].start()
    for store in stores:
        store.wait()


def layout(scan_local, groups, scan_total):
    columns = scan_total // groups
    pack = max(1, LANES // columns)
    per_block = -(-(MAT + 1) // pack)
    return columns, pack, per_block


def block_rows(every, row_hot, count):
    high = every.astype(jnp.bfloat16).astype(jnp.float32)
    for part in (high, every - high):
        yield jnp.concatenate(
            [jnp.where(row_hot, part[q : q + 1], 0.0).astype(jnp.bfloat16) for q in range(count)], axis=0
        )


def held_kernel(devices, groups, scan_local, flat_ref, *refs):
    out_refs, stage_ref = refs[:-1], refs[-1]
    slots = flat_ref.shape[1]
    cap = slots // devices
    scan_total = scan_local * (devices // groups)
    columns, pack, per_block = layout(scan_local, groups, scan_total)
    every = flat_ref[...]
    row = every[ROW_MATE : ROW_MATE + 1].astype(jnp.int32)
    other = div(div(iota((1, slots), 1), cap), groups) * scan_local + every[ROW_FLAG : ROW_FLAG + 1].astype(jnp.int32) - 1
    own = lax.axis_index("scan") * scan_local + row
    row_hot = iota((scan_local, slots), 0) == row
    column = iota((scan_total, slots), 0)
    mix = ((column == own).astype(jnp.float32) - (column == other).astype(jnp.float32)).astype(jnp.bfloat16)
    hess = sum(dot(rows, mix, BOTH_LANES) for rows in block_rows(every, row_hot, MAT))
    lane = iota((scan_local, LANES), 1)
    home = MAT // per_block
    grad = jnp.zeros((scan_local, LANES), jnp.float32)
    for q in range(FIELDS):
        value = jnp.sum(jnp.where(row_hot, every[HEAD + q : HEAD + q + 1], 0.0), axis=1, keepdims=True)
        grad = jnp.where(lane == home * columns + q, -value, grad)
    for c in range(groups):
        side, shift = divmod(c * columns, LANES)
        for r in range(per_block):
            tile = jnp.zeros((scan_local, LANES), jnp.float32)
            for k in range(pack):
                q = k * per_block + r
                if q < MAT:
                    value = hess[q * scan_local : (q + 1) * scan_local, side * LANES : (side + 1) * LANES]
                    value = turn(value, k * columns - shift)
                elif q == MAT:
                    value = grad
                else:
                    continue
                tile = jnp.where(div(lane, columns) == k, value, tile) if pack > 1 else value
            stage_ref[c, r * scan_local : (r + 1) * scan_local, :] = tile
    for k, out_ref in enumerate(out_refs):
        out_ref[...] = stage_ref[partner(lax.axis_index("grp"), k, groups)]


def close_kernel(devices, groups, cap, back_ref, *refs):
    part_refs, (hess_ref, grad_ref, every_ref, hold_ref) = refs[:groups], refs[groups:]
    scan_local, columns = hess_ref.shape[1:]
    per_block = part_refs[0].shape[0] // scan_local
    span, slot_rows, sum_rows, grad_row, grad_lane, block = back_layout(scan_local, groups, cap)
    senders = devices // groups
    first = lax.axis_index("grp") * (senders * block)
    lane_block = div(iota((slot_rows, LANES), 1), span)
    per_chunk = LANES // span
    for chunk in range(senders // per_chunk):
        found = [back_ref[pl.ds(first + (chunk * per_chunk + u) * block, slot_rows), :] for u in range(per_chunk)]
        for i in range(LANES // span):
            tile = None
            for u in range(per_chunk):
                piece = turn(found[u], (u - i) * span)
                tile = piece if u == 0 else jnp.where(lane_block == u, piece, tile)
            every_ref[i * slot_rows : (i + 1) * slot_rows, chunk * LANES : (chunk + 1) * LANES] = tile
    every = every_ref[...]
    total = every.shape[1]
    row = every[ROW_FLAG : ROW_FLAG + 1].astype(jnp.int32) - 1
    mate = every[ROW_MATE : ROW_MATE + 1].astype(jnp.int32)
    column = div(div(iota((1, total), 1), span), groups) * scan_local + mate
    row_hot = iota((scan_local, total), 0) == row
    offset = lax.axis_index("scan") * scan_local - lax.axis_index("grp") * columns
    line = iota((columns, total), 0)
    mix = (line == row + offset).astype(jnp.float32) - (line == column).astype(jnp.float32)
    mix = mix.astype(jnp.bfloat16)
    rows = jnp.concatenate(list(block_rows(every, row_hot, MAT)), axis=1)
    cross = dot(rows, jnp.concatenate([mix, mix], axis=1), BOTH_LANES)
    sums = jnp.zeros((sum_rows, LANES), jnp.float32)
    for c in range(groups):
        part = back_ref[c * senders * block : c * senders * block + sum_rows, :]
        for d in range(c * senders + 1, (c + 1) * senders):
            part = part + back_ref[d * block : d * block + sum_rows, :]
        sums = sums + jnp.where(lax.axis_index("grp") != c, part, 0.0)
    near = back_ref[pl.ds(first + grad_row, 1), :]
    for u in range(1, senders):
        near = near + back_ref[pl.ds(first + u * block + grad_row, 1), :]
    line = iota((scan_local, LANES), 0)
    lane = iota((scan_local, LANES), 1)

    def by_row(q):
        i, r = divmod(q, sum_rows)
        return jnp.sum(jnp.where(lane == line + i * scan_local, sums[r : r + 1], 0.0), axis=1, keepdims=True)

    whole = part_refs[0][...]
    for part_ref in part_refs[1:]:
        whole = whole + part_ref[...]
    diagonal = iota((scan_local, columns), 1) == iota((scan_local, columns), 0) + offset
    shifted = pltpu.roll(sums, mod(offset + LANES * (devices // groups), LANES), 1)
    facing = [turn(shifted, -n * scan_local) for n in range(WIDTH // sum_rows)]
    for q in range(MAT):
        k, r = divmod(q, per_block)
        tile = whole[r * scan_local : (r + 1) * scan_local, k * columns : (k + 1) * columns]
        tile = tile + cross[q * scan_local : (q + 1) * scan_local]
        n, r = divmod(q, sum_rows)
        tile = tile + jnp.where(diagonal, facing[n][r : r + 1, 0:columns], 0.0)
        i, j = PAIRS[q]
        hess_ref[i * FIELDS + j] = tile
        if i != j:
            hess_ref[j * FIELDS + i] = tile
    k, r = divmod(MAT, per_block)
    grad = turn(whole[r * scan_local : (r + 1) * scan_local], -k * columns)
    for q in range(FIELDS):
        grad = grad + jnp.where(lane == q, by_row(HEAD + q), 0.0)
    hold_ref[...] = grad
    part = scan_local // groups
    own = jnp.zeros((part, LANES), jnp.float32)
    for q in range(FIELDS):
        spot = grad_lane + q * part + iota((part, LANES), 0) == iota((part, LANES), 1)
        value = jnp.sum(jnp.where(spot, near, 0.0), axis=1, keepdims=True)
        own = jnp.where(iota((part, LANES), 1) == q, value, own)
    hold = hold_ref[pl.ds(lax.axis_index("grp") * part, part), :] + own
    grad_ref[...] = hold[:, 0:FIELDS]


def call(kernel, out_shape, smem, vmem, scratch=(), out_specs=None):
    body = pl.pallas_call(
        kernel,
        out_shape=out_shape,
        in_specs=[pl.BlockSpec(memory_space=pltpu.SMEM)] * smem + [pl.BlockSpec(memory_space=pltpu.VMEM)] * vmem,
        scratch_shapes=list(scratch),
        **({} if out_specs is None else {"out_specs": out_specs}),
    )

    def run(*args):
        args = args[:smem] + tuple(pltpu.with_memory_space_constraint(x, pltpu.VMEM) for x in args[smem:])
        return body(*args)

    return run


def f32(*shape):
    return jax.ShapeDtypeStruct(shape, jnp.float32)


def near(*shape):
    return pltpu.VMEM(shape, jnp.float32)


def exchange(x, axes):
    count, width = x.shape
    moved = lax.all_to_all(x.reshape(count, 1, width), axes, split_axis=0, concat_axis=0, tiled=True)
    return moved.reshape(count, width)


def local(samples, point_count, corr_scan, corr_tile, corr_src):
    devices = lax.axis_size(AXES)
    groups = lax.axis_size("grp")
    samples = samples.transpose(0, 2, 1, 3)
    scan_local, tiles, per_scan, entries, cap, block = sizes(samples.shape, corr_scan.shape, devices)
    slots = devices * cap
    scan_total = scan_local * (devices // groups)
    columns, pack, per_block = layout(scan_local, groups, scan_total)
    back_rows = back_layout(scan_local, groups, cap)[-1]

    def bind(kernel, *args):
        return lambda *refs: kernel(*args, *refs)

    sent, samples, limits = pl.pallas_call(
        bind(send_kernel, devices, groups),
        out_shape=(
            near(devices * block, LANES),
            near(*samples.shape),
            pltpu.VMEM((scan_local, LANES), jnp.int32),
        ),
        in_specs=[pl.BlockSpec(memory_space=pl.ANY)] * 5,
        scratch_shapes=[
            pltpu.SMEM(point_count.shape, jnp.int32),
            pltpu.VMEM(corr_scan.shape, jnp.int32),
            pltpu.VMEM(corr_tile.shape, jnp.int32),
            pltpu.VMEM(corr_src.shape, jnp.int32),
            pltpu.VMEM((SENT, entries, LANES), jnp.float32),
            pltpu.SemaphoreType.DMA((6,)),
        ],
    )(point_count, samples, corr_scan, corr_tile, corr_src)
    received = exchange(sent, AXES)
    flat, back = call(
        bind(pair_kernel, devices, groups),
        (near(WIDTH, slots), f32(devices * back_rows, LANES)),
        0,
        3,
        [
            pltpu.VMEM((devices * back_rows, LANES), jnp.float32),
            pltpu.VMEM((SENT, LANES, slots), jnp.float32),
            pltpu.VMEM((FIELDS, LANES, slots), jnp.float32),
            pltpu.VMEM((devices, LANES), jnp.float32),
            pltpu.SemaphoreType.DMA((slots // LANES,)),
        ],
        (pl.BlockSpec(memory_space=pltpu.VMEM), pl.BlockSpec(memory_space=pl.ANY)),
    )(limits, samples, received)
    back = exchange(back, AXES)
    share = near(per_block * scan_local, LANES)
    shares = call(
        bind(held_kernel, devices, groups, scan_local),
        (share,) * groups,
        0,
        1,
        [pltpu.VMEM((groups,) + share.shape, jnp.float32)],
    )(flat)
    shares = [shares[0]] + [
        lax.ppermute(shares[k], "grp", [(g, partner(g, k, groups)) for g in range(groups)]) for k in range(1, groups)
    ]
    hess, grad = call(
        bind(close_kernel, devices, groups, cap),
        (f32(FIELDS * FIELDS, scan_local, columns), f32(scan_local // groups, FIELDS)),
        0,
        1 + groups,
        [
            pltpu.VMEM((HEAD, (devices // groups) * groups * cap), jnp.float32),
            pltpu.VMEM((scan_local, LANES), jnp.float32),
        ],
    )(back, *shares)
    return hess.reshape(FIELDS, FIELDS, scan_local, columns).transpose(2, 0, 1, 3), grad


def solution(mesh):
    placed = (
        P("scan", "grp", None, None),
        P("scan"),
        P("scan", "grp"),
        P("scan", "grp"),
        P("scan", "grp", None),
    )
    return jax.shard_map(
        local,
        mesh=mesh,
        in_specs=placed,
        out_specs=(P("scan", None, None, "grp"), P(AXES, None)),
        check_vma=False,
    )
```
